32 devices in a mesh: dp: 4 (over y, x), seq: 8 (over z, core).
Axes of the slice: x: 2, y: 2, z: 4, core: 2. Of those that a mesh axis runs over, the one named last changes fastest.
Arguments:
- tokens: bfloat16 [4, 2048, 1024], P('dp', 'seq'), may hold values from -6 to 6
- cotangent: bfloat16 [4, 2048, 1024], P('dp', 'seq'), may hold values from -6 to 6
- segments: int32 [4, 2048], P('dp'), may hold values from 0 to 3, never falling along the last dimension, each value on 1 to 1024 neighbouring positions
- qkv_weight: bfloat16 [2, 1024, 3072], P(None, ('dp', 'seq')), may hold values from -0.1875 to 0.1875
- out_weight: bfloat16 [2, 1024, 1024], P(None, ('dp', 'seq')), may hold values from -0.75 to 0.75
- fc_weight: bfloat16 [2, 1024, 4096], P(None, ('dp', 'seq')), may hold values from -0.1875 to 0.1875
- proj_weight: bfloat16 [2, 4096, 1024], P(None, ('dp', 'seq')), may hold values from -0.09375 to 0.09375
- biases: bfloat16 [2, 9, 1024], P(None, None, ('dp', 'seq')), may hold values from -2 to 2
- ln_gain: bfloat16 [2, 2, 1024], P(None, None, ('dp', 'seq')), may hold values from 0.099609375 to 1.8984375
- ln_shift: bfloat16 [2, 2, 1024], P(None, None, ('dp', 'seq')), may hold values from -2 to 2
Outputs:
- outputs: bfloat16 [4, 2048, 1024], P('dp', 'seq')
- grad_tokens: bfloat16 [4, 2048, 1024], P('dp', 'seq')
- grad_qkv_weight: float32 [2, 1024, 3072], P(None, ('dp', 'seq'))
- grad_out_weight: float32 [2, 1024, 1024], P(None, ('dp', 'seq'))
- grad_fc_weight: float32 [2, 1024, 4096], P(None, ('dp', 'seq'))
- grad_proj_weight: float32 [2, 4096, 1024], P(None, ('dp', 'seq'))
- grad_biases: float32 [2, 9, 1024], P(None, None, ('dp', 'seq'))
- grad_ln_gain: float32 [2, 2, 1024], P(None, None, ('dp', 'seq'))
- grad_ln_shift: float32 [2, 2, 1024], P(None, None, ('dp', 'seq'))
The draws below stay inside these ranges and needn't reach their ends.
Inputs may be any that keep to these rules, and one draw needn't show every extreme that they name: `segments`: segment numbers never fall along a sequence; each of the 4 documents of a sequence has 1 to 1024 tokens, and one has exactly 1024.
All inputs are finite; a program needn't handle non-finite values.
Results may differ from the reference program's by a relative error of at most 0.015.
Values may be sent and summed in bfloat16 or wider, within the bound.
A program may use at most 384 MiB of HBM per device.

```python
import math
import jax
import jax.numpy as jnp
import numpy as np
from jax import lax

D = 1024
HEADS = 16
HEAD_DIM = 64
ROT = 16
FF = 4096
LEN = 2048
DOCS = 4
LAYERS = 2
SEQS = 4


def level_of(key, shape, pieces, smallest, top_value):
    factor_of, own = 1.0, jax.random.fold_in(key, 6)
    for dim, shards_of in pieces:
        steps = jnp.exp(jax.random.uniform(jax.random.fold_in(own, dim), (shards_of,), jnp.float32, smallest / len(pieces), top_value / len(pieces)))
        factor_of = factor_of * jnp.repeat(steps, shape[dim] // shards_of).reshape([-1 if axis == dim else 1 for axis in range(len(shape))])
    return factor_of


def profile(number_of, total, most, slope):
    loads = [(1 << 20) // math.isqrt(standing ** slope) + 1 for standing in range(2, number_of + 1)]
    rest, counts = total - most - (number_of - 1), [1] * (number_of - 1)
    while rest > 0:
        free = [i for i in range(number_of - 1) if counts[i] < most]
        whole, remaining = sum([loads[i] for i in free]), rest
        for i in free:
            more = min(most - counts[i], max(1, remaining * loads[i] // whole), rest)
            counts[i] = counts[i] + more
            rest = rest - more
    return np.array([most] + counts)


def uneven_parts(own_key, count, total, reach, lean):
    if count == 2:
        one = jax.random.randint(own_key, (), max(1, total - reach), min(reach, total - 1) + 1)
        return jnp.stack([one, total - one])
    tallies = jnp.asarray(profile(count, total, reach, lean), jnp.int32)
    twos = (count - 1) // 2
    source_of, receiver = tallies[1:1 + 2 * twos:2], tallies[2:2 + 2 * twos:2]
    room = jnp.minimum(source_of - 1, reach - receiver)
    passed = jax.random.randint(jax.random.fold_in(own_key, 1), (twos,), 0, 1 << 20) % (room + 1)
    tallies = tallies.at[1:1 + 2 * twos:2].set(source_of - passed).at[2:2 + 2 * twos:2].set(receiver + passed)
    return tallies[jax.random.permutation(jax.random.fold_in(own_key, 2), count)]


def scatter_about(rng, dims, width, bound, split=(), kind=jnp.bfloat16):
    values = width * jax.random.normal(rng, dims, jnp.float32)
    if split:
        values = values * level_of(rng, dims, split, -0.22, 0.18)
    return jnp.clip(values, -bound, bound).astype(kind)


def setup_inputs(seed: int = 0) -> dict:
    streams_of = jax.random.split(jax.random.key(seed), 11)
    return {
        "tokens": scatter_about(streams_of[0], (SEQS, LEN, D), 1.0, 6.0, ((0, 4), (1, 8))),
        "cotangent": scatter_about(streams_of[1], (SEQS, LEN, D), 1.0, 6.0, ((0, 4), (1, 8))),
        "segments": jax.vmap(lambda own: jnp.searchsorted(jnp.cumsum(uneven_parts(own, DOCS, LEN, LEN // 2, 2)), jnp.arange(LEN), side="right"))(jax.random.split(streams_of[2], SEQS)).reshape((SEQS, LEN)).astype(jnp.int32),
        "qkv_weight": scatter_about(streams_of[3], (LAYERS, D, 3 * D), D ** -0.5, 0.1875, ((1, 32),)),
        "out_weight": scatter_about(streams_of[4], (LAYERS, D, D), (D // 16) ** -0.5, 0.75, ((1, 32),)),
        "fc_weight": scatter_about(streams_of[5], (LAYERS, D, FF), D ** -0.5, 0.1875, ((1, 32),)),
        "proj_weight": scatter_about(streams_of[6], (LAYERS, FF, D), FF ** -0.5, 0.09375, ((1, 32),)),
        "biases": scatter_about(streams_of[7], (LAYERS, 5 + FF // D, D), 0.3, 2.0, ((2, 32),)),
        "ln_gain": jnp.clip(1.0 + 0.18 * jax.random.normal(streams_of[8], (LAYERS, 2, D), jnp.float32), 0.099609375, 1.8984375).astype(jnp.bfloat16),
        "ln_shift": scatter_about(streams_of[9], (LAYERS, 2, D), 0.3, 2.0, ((2, 32),)),
    }


@jax.custom_vjp
def low(v):
    return lax.optimization_barrier(v.astype(jnp.bfloat16)).astype(jnp.float32)

@jax.custom_vjp
def low_back(v):
    return v

def low_keep(v):
    return (low(v), None)

def low_pass(kept, grad):
    return (grad,)

def back_keep(v):
    return (v, None)

def back_low(kept, grad):
    return (low(grad),)
low.defvjp(low_keep, low_pass)
low_back.defvjp(back_keep, back_low)
norm_eps = 1e-05
mask_fill = -1e+30
highest = lax.Precision.HIGHEST

def layer_norm(features, norm_gain, norm_shift):
    center = features - lax.optimization_barrier(jnp.mean(features, axis=-1, keepdims=True))
    spread = lax.optimization_barrier(jnp.mean(center * center, axis=-1, keepdims=True))
    return center * lax.rsqrt(spread + norm_eps) * norm_gain + norm_shift

def rotary_tables(seg_rows):
    key_index = jnp.arange(seg_rows.shape[-1], dtype=jnp.int32)
    run_start = jnp.concatenate([jnp.ones(seg_rows.shape[:-1] + (1,), dtype=bool), seg_rows[..., 1:] != seg_rows[..., :-1]], axis=-1)
    starts = lax.cummax(jnp.where(run_start, key_index, 0), axis=seg_rows.ndim - 1)
    position = (key_index - starts).astype(jnp.float32)
    half_rot = ROT // 2
    inverse = 10000.0 ** (-2.0 * jnp.arange(half_rot, dtype=jnp.float32) / ROT)
    angle_table = position[..., None] * inverse
    angle_table = jnp.concatenate([angle_table, angle_table], axis=-1)
    return (jnp.cos(angle_table), jnp.sin(angle_table))

def rotate(head_vals, cosine, sine_table):
    cosine = cosine[..., None, :]
    sine_table = sine_table[..., None, :]
    half_rot = ROT // 2
    turned = head_vals[..., :ROT]
    swapped = jnp.concatenate([-turned[..., half_rot:], turned[..., :half_rot]], axis=-1)
    return jnp.concatenate([turned * cosine + swapped * sine_table, head_vals[..., ROT:]], axis=-1)

def attend(queries, key_rows, value_rows, allowed):
    block_rows = min(512, LEN)
    score_scale = HEAD_DIM ** (-0.5)

    def one_block(start):
        part_query = lax.dynamic_slice_in_dim(queries, start, block_rows, 0)
        part_allow = lax.dynamic_slice_in_dim(allowed, start, block_rows, 0)
        scores = jnp.einsum('qhd,khd->hqk', part_query, key_rows, precision=highest) * score_scale
        scores = low_back(scores)
        scores = jnp.where(part_allow[None], scores, mask_fill)
        row_top = lax.optimization_barrier(jnp.max(scores, axis=-1, keepdims=True))
        row_expo = jnp.exp(scores - row_top)
        attn_probs = low(row_expo / lax.optimization_barrier(jnp.sum(row_expo, axis=-1, keepdims=True)))
        return jnp.einsum('hqk,khd->qhd', attn_probs, value_rows, precision=highest)
    starts = jnp.arange(LEN // block_rows, dtype=jnp.int32) * block_rows
    blocks_out = lax.map(jax.checkpoint(one_block), starts)
    return blocks_out.reshape(LEN, HEADS, HEAD_DIM)

def block(resid, mats, vectors, cosine, sine_table, allowed):
    qkv_w, out_w, fc_w, proj_w = mats
    bias_rows, gain_all, shift_all = vectors
    bias_all = bias_rows.reshape(-1)
    normed_one = low(layer_norm(resid, gain_all[0], shift_all[0]))
    normed_two = low(layer_norm(resid, gain_all[1], shift_all[1]))
    qkv_mixed = low_back(jnp.dot(normed_one, qkv_w, precision=highest) + bias_all[:3 * D])
    qkv_mixed = qkv_mixed.reshape(LEN, 3, HEADS, HEAD_DIM)
    queries = low(rotate(qkv_mixed[:, 0], cosine, sine_table))
    key_rows = low(rotate(qkv_mixed[:, 1], cosine, sine_table))
    value_rows = low(qkv_mixed[:, 2])
    context = attend(queries, key_rows, value_rows, allowed).reshape(LEN, D)
    context = low_back(low(context))
    attn_out = jnp.dot(context, out_w, precision=highest) + bias_all[3 * D:4 * D]
    hidden_pre = low_back(jnp.dot(normed_two, fc_w, precision=highest) + bias_all[4 * D:4 * D + FF])
    hidden = low(jax.nn.gelu(hidden_pre, approximate=False))
    mlp_out = jnp.dot(hidden, proj_w, precision=highest) + bias_all[4 * D + FF:]
    return low_back(resid + attn_out + mlp_out)

def reference(tokens, cotangent, segments, qkv_weight, out_weight, fc_weight, proj_weight, biases, ln_gain, ln_shift):
    params = tuple((weight_arr.astype(jnp.float32) for weight_arr in (qkv_weight, out_weight, fc_weight, proj_weight, biases, ln_gain, ln_shift)))
    key_index = jnp.arange(LEN, dtype=jnp.int32)

    def forward(resid, param_set, cosine, sine_table, allowed):
        for layer_at in range(LAYERS):
            mats = (param_set[0][layer_at], param_set[1][layer_at], param_set[2][layer_at], param_set[3][layer_at])
            vectors = (param_set[4][layer_at], param_set[5][layer_at], param_set[6][layer_at])
            resid = block(resid, mats, vectors, cosine, sine_table, allowed)
        return resid

    def one_seq(totals, inputs):
        seq_tokens, seq_cot, seq_seg = inputs
        cosine, sine_table = rotary_tables(seq_seg)
        allowed = (key_index[None, :] <= key_index[:, None]) & (seq_seg[None, :] == seq_seg[:, None])

        def run(resid, param_set):
            return forward(resid, param_set, cosine, sine_table, allowed)
        result, pull = jax.vjp(run, seq_tokens.astype(jnp.float32), params)
        grad_in, grad_params = pull(seq_cot.astype(jnp.float32))
        totals = tuple((left + right for left, right in zip(totals, grad_params)))
        return (totals, (result.astype(jnp.bfloat16), grad_in.astype(jnp.bfloat16)))
    zeros = tuple((jnp.zeros(weight_arr.shape, jnp.float32) for weight_arr in params))
    totals, (outputs, grad_tokens) = lax.scan(one_seq, zeros, (tokens, cotangent, segments))
    return (outputs, grad_tokens, totals[0], totals[1], totals[2], totals[3], totals[4], totals[5], totals[6])
```

```python
import functools

import jax
import jax.numpy as jnp
from jax import lax
from jax.experimental import pallas as pl
from jax.experimental.pallas import tpu as pltpu
from jax.sharding import PartitionSpec as P

HEAD_DIM = 64
ROT = 16
norm_eps = 1e-05
mask_fill = -1e30
BF = jnp.bfloat16
F32 = jnp.float32
AXES = ("dp", "seq")
BLOCK = 256


def nt(left, right):
    return lax.dot_general(left, right, (((1,), (1,)), ((), ())), preferred_element_type=F32)


def nn(left, right):
    return lax.dot_general(left, right, (((1,), (0,)), ((), ())), preferred_element_type=F32)


def tn(left, right):
    return lax.dot_general(left, right, (((0,), (0,)), ((), ())), preferred_element_type=F32)


def lane_in_head(shape):
    lane = lax.broadcasted_iota(jnp.int32, shape, len(shape) - 1)
    return lane, lane % HEAD_DIM


def rope(vals, cosine, sine):
    width = vals.shape[-1]
    half = ROT // 2
    _, entry = lane_in_head(vals.shape)
    up = pltpu.roll(vals, width - half, 1)
    down = pltpu.roll(vals, half, 1)
    swapped = jnp.where(entry < half, -up, down)
    return vals * cosine + swapped * sine


def rope_back(grads, cosine, sine):
    width = grads.shape[-1]
    half = ROT // 2
    _, entry = lane_in_head(grads.shape)
    scaled = grads * sine
    up = pltpu.roll(scaled, width - half, 1)
    down = pltpu.roll(scaled, half, 1)
    swapped = jnp.where(entry < half, up, jnp.where(entry < ROT, -down, 0.0))
    return grads * cosine + swapped


def head_only(vals, head):
    lane, _ = lane_in_head(vals.shape)
    keep = (lane >= head * HEAD_DIM) & (lane < (head + 1) * HEAD_DIM)
    return jnp.where(keep, vals, jnp.zeros_like(vals))


def attn_fwd_kernel(
    first_ref, mixed_ref, cos_ref, sin_ref, start_ref,
    query_ref, key_ref, value_ref, ctx_ref, ctx_low_ref, lse_ref,
    value_t_ref,
):
    at = pl.program_id(0)
    total, width = key_ref.shape
    heads = width // HEAD_DIM

    @pl.when(at == 0)
    def _():
        def one(i, carry):
            rows = pl.ds(pl.multiple_of(i * BLOCK, BLOCK), BLOCK)
            keys = mixed_ref[rows, width : 2 * width]
            key_ref[rows, :] = rope(keys, cos_ref[rows, :], sin_ref[rows, :]).astype(BF)
            vals = mixed_ref[rows, 2 * width : 3 * width]
            value_ref[rows, :] = vals.astype(BF)
            value_t_ref[:, rows] = vals.T.astype(BF)
            return carry

        lax.fori_loop(0, total // BLOCK, one, 0)

    rows = pl.ds(pl.multiple_of(at * BLOCK, BLOCK), BLOCK)
    quer = rope(mixed_ref[rows, 0:width], cos_ref[rows, :], sin_ref[rows, :]).astype(BF)
    quer = quer * jnp.asarray(HEAD_DIM**-0.5, BF)
    query_ref[...] = quer
    by_head = [head_only(quer, h) for h in range(heads)]
    key_iota = lax.broadcasted_iota(jnp.int32, (BLOCK, BLOCK), 0)
    query_pos = at * BLOCK + lax.broadcasted_iota(jnp.int32, (1, BLOCK), 1)
    starts = start_ref[...]

    def step(turn, carry):
        block = at - turn
        keys_at = pl.ds(pl.multiple_of(block * BLOCK, BLOCK), BLOCK)
        keys = key_ref[keys_at, :]
        vals_t = value_t_ref[:, keys_at]
        keep = (key_iota >= starts - block * BLOCK) & (key_iota <= query_pos - block * BLOCK)
        out = []
        for h in range(heads):
            top, total_h, acc = carry[h]
            scores = jnp.where(keep, nt(keys, by_head[h]), mask_fill)
            new_top = jnp.maximum(top, jnp.max(scores, axis=0, keepdims=True))
            fade = jnp.exp(top - new_top)
            probs = jnp.exp(scores - new_top)
            total_h = total_h * fade + jnp.sum(probs, axis=0, keepdims=True)
            acc = acc * fade + nn(vals_t, probs.astype(BF))
            out.append((new_top, total_h, acc))
        return tuple(out)

    init = tuple(
        (
            jnp.full((1, BLOCK), mask_fill, F32),
            jnp.zeros((1, BLOCK), F32),
            jnp.zeros((width, BLOCK), F32),
        )
        for h in range(heads)
    )
    done = lax.fori_loop(0, at - first_ref[at] + 1, step, init)
    parts = []
    for h in range(heads):
        top, total_h, acc = done[h]
        lse_ref[h : h + 1, :] = top + jnp.log(total_h)
        parts.append(acc[h * HEAD_DIM : (h + 1) * HEAD_DIM, :] / total_h)
    ctx = jnp.concatenate(parts, axis=0).T
    ctx_ref[...] = ctx
    ctx_low_ref[...] = ctx.astype(BF)


def attn_forward(mixed, cosine, sine, starts, first_block):
    total, width = cosine.shape
    heads = width // HEAD_DIM
    blocks = total // BLOCK
    full = lambda cols: pl.BlockSpec((total, cols), lambda i, f: (0, 0))
    rows = pl.BlockSpec((BLOCK, width), lambda i, f: (i, 0))
    lanes = lambda n: pl.BlockSpec((n, BLOCK), lambda i, f: (0, i))
    wide = jax.ShapeDtypeStruct((total, width), BF)
    return pl.pallas_call(
        attn_fwd_kernel,
        grid_spec=pltpu.PrefetchScalarGridSpec(
            num_scalar_prefetch=1,
            grid=(blocks,),
            in_specs=[full(3 * width), full(width), full(width), lanes(1)],
            out_specs=[rows, full(width), full(width), rows, rows, lanes(heads)],
            scratch_shapes=[pltpu.VMEM((width, total), BF)],
        ),
        out_shape=[
            wide, wide, wide,
            jax.ShapeDtypeStruct((total, width), F32),
            wide,
            jax.ShapeDtypeStruct((heads, total), F32),
        ],
        compiler_params=pltpu.CompilerParams(
            dimension_semantics=("arbitrary",), vmem_limit_bytes=40 << 20
        ),
        cost_estimate=pl.CostEstimate(
            flops=20 * 4 * BLOCK * BLOCK * width * heads,
            bytes_accessed=total * width * 40,
            transcendentals=20 * BLOCK * BLOCK * heads,
        ),
        name="attn_fwd",
    )(first_block, mixed, cosine, sine, starts)


def attn_bwd_kernel(
    first_ref, query_ref, key_ref, value_ref, ctx_ref, lse_ref, grad_ref, cos_ref, sin_ref, start_ref,
    out_ref,
    key_t_ref, grad_key_ref, grad_value_ref,
):
    at = pl.program_id(0)
    total, width = key_ref.shape
    heads = width // HEAD_DIM

    @pl.when(at == 0)
    def _():
        def one(i, carry):
            rows = pl.ds(pl.multiple_of(i * BLOCK, BLOCK), BLOCK)
            key_t_ref[:, rows] = key_ref[rows, :].T
            grad_key_ref[rows, :] = jnp.zeros((BLOCK, width), F32)
            grad_value_ref[rows, :] = jnp.zeros((BLOCK, width), F32)
            return carry

        lax.fori_loop(0, total // BLOCK, one, 0)

    quer = query_ref[...]
    grad = grad_ref[...]
    by_head = [head_only(quer, h) for h in range(heads)]
    grad_head = [head_only(grad, h) for h in range(heads)]
    inner_t = (grad.astype(F32) * ctx_ref[...]).T
    inner = [
        jnp.sum(inner_t[h * HEAD_DIM : (h + 1) * HEAD_DIM, :], axis=0, keepdims=True)
        for h in range(heads)
    ]
    logs = [lse_ref[h : h + 1, :] for h in range(heads)]
    key_iota = lax.broadcasted_iota(jnp.int32, (BLOCK, BLOCK), 0)
    query_pos = at * BLOCK + lax.broadcasted_iota(jnp.int32, (1, BLOCK), 1)
    starts = start_ref[...]

    def step(turn, carry):
        block = at - turn
        keys_at = pl.ds(pl.multiple_of(block * BLOCK, BLOCK), BLOCK)
        keys = key_ref[keys_at, :]
        vals = value_ref[keys_at, :]
        keys_t = key_t_ref[:, keys_at]
        keep = (key_iota >= starts - block * BLOCK) & (key_iota <= query_pos - block * BLOCK)
        out = []
        grad_key = jnp.zeros((BLOCK, width), F32)
        grad_value = jnp.zeros((BLOCK, width), F32)
        for h in range(heads):
            scores = nt(keys, by_head[h])
            probs = jnp.where(keep, jnp.exp(jnp.where(keep, scores, mask_fill) - logs[h]), 0.0)
            grad_probs = nt(vals, grad_head[h])
            grad_scores = (probs * (grad_probs - inner[h])).astype(BF)
            grad_value = grad_value + nn(probs.astype(BF), grad_head[h])
            grad_key = grad_key + nn(grad_scores, by_head[h])
            out.append(carry[h] + nn(keys_t, grad_scores))
        grad_key_ref[keys_at, :] += grad_key
        grad_value_ref[keys_at, :] += grad_value
        return tuple(out)

    init = tuple(jnp.zeros((width, BLOCK), F32) for h in range(heads))
    done = lax.fori_loop(0, at - first_ref[at] + 1, step, init)
    parts = [done[h][h * HEAD_DIM : (h + 1) * HEAD_DIM, :] for h in range(heads)]
    grad_query = jnp.concatenate(parts, axis=0).T * (HEAD_DIM**-0.5)
    rows = pl.ds(pl.multiple_of(at * BLOCK, BLOCK), BLOCK)
    out_ref[rows, 0:width] = rope_back(grad_query, cos_ref[rows, :], sin_ref[rows, :]).astype(BF)

    @pl.when(at == pl.num_programs(0) - 1)
    def _():
        def one(i, carry):
            rows = pl.ds(pl.multiple_of(i * BLOCK, BLOCK), BLOCK)
            grad_key = rope_back(grad_key_ref[rows, :], cos_ref[rows, :], sin_ref[rows, :])
            out_ref[rows, width : 2 * width] = grad_key.astype(BF)
            out_ref[rows, 2 * width : 3 * width] = grad_value_ref[rows, :].astype(BF)
            return carry

        lax.fori_loop(0, total // BLOCK, one, 0)


def attn_backward(query, key, value, ctx, lse, grad_ctx, cosine, sine, starts, first_block):
    total, width = cosine.shape
    heads = width // HEAD_DIM
    blocks = total // BLOCK
    full = lambda cols: pl.BlockSpec((total, cols), lambda i, f: (0, 0))
    rows = pl.BlockSpec((BLOCK, width), lambda i, f: (i, 0))
    lanes = lambda n: pl.BlockSpec((n, BLOCK), lambda i, f: (0, i))
    return pl.pallas_call(
        attn_bwd_kernel,
        grid_spec=pltpu.PrefetchScalarGridSpec(
            num_scalar_prefetch=1,
            grid=(blocks,),
            in_specs=[
                rows, full(width), full(width), rows, lanes(heads), rows,
                full(width), full(width), lanes(1),
            ],
            out_specs=full(3 * width),
            scratch_shapes=[
                pltpu.VMEM((width, total), BF),
                pltpu.VMEM((total, width), F32),
                pltpu.VMEM((total, width), F32),
            ],
        ),
        out_shape=jax.ShapeDtypeStruct((total, 3 * width), BF),
        compiler_params=pltpu.CompilerParams(
            dimension_semantics=("arbitrary",), vmem_limit_bytes=40 << 20
        ),
        cost_estimate=pl.CostEstimate(
            flops=20 * 10 * BLOCK * BLOCK * width * heads,
            bytes_accessed=total * width * 40,
            transcendentals=20 * BLOCK * BLOCK * heads,
        ),
        name="attn_bwd",
    )(first_block, query, key, value, ctx, lse, grad_ctx, cosine, sine, starts)


class Net:
    def __init__(self, mesh):
        self.planes = mesh.shape["seq"] // 2
        self.spots = mesh.shape["dp"]
        self.p = lax.axis_index("dp")
        self.z = lax.axis_index("seq") // 2
        self.c = lax.axis_index("seq") % 2

    def permute(self, x, to):
        pairs = []
        for p in range(self.spots):
            for z in range(self.planes):
                for c in range(2):
                    tp, tz, tc = to(p, z, c)
                    source = (p * self.planes + z) * 2 + c
                    pairs.append((source, (tp * self.planes + tz) * 2 + tc))
        return lax.ppermute(x, AXES, pairs)

    def sibling(self, x):
        return self.permute(x, lambda p, z, c: (p, z, 1 - c))

    def turned(self, x):
        return self.permute(x, lambda p, z, c: (z, p, c))

    def gather(self, x, axis):
        count = self.spots if axis == "p" else self.planes
        me = self.p if axis == "p" else self.z
        buf = jnp.zeros((count,) + x.shape, x.dtype)
        buf = lax.dynamic_update_index_in_dim(buf, x, me, 0)
        for k in range(1, count):
            if axis == "p":
                got = self.permute(x, lambda p, z, c: (p ^ k, z, c))
            else:
                got = self.permute(x, lambda p, z, c: (p, z ^ k, c))
            buf = lax.dynamic_update_index_in_dim(buf, got, me ^ k, 0)
        return buf

    def swap(self, x, axis):
        count = self.spots if axis == "p" else self.planes
        me = self.p if axis == "p" else self.z
        pieces = [lax.dynamic_index_in_dim(x, me, 0, keepdims=False)]
        for k in range(1, count):
            piece = lax.dynamic_index_in_dim(x, me ^ k, 0, keepdims=False)
            if axis == "p":
                pieces.append(self.permute(piece, lambda p, z, c: (p ^ k, z, c)))
            else:
                pieces.append(self.permute(piece, lambda p, z, c: (p, z ^ k, c)))
        return pieces

    def ordered(self, pieces, axis):
        me = self.p if axis == "p" else self.z
        buf = jnp.zeros((len(pieces),) + pieces[0].shape, pieces[0].dtype)
        for k, piece in enumerate(pieces):
            buf = lax.dynamic_update_index_in_dim(buf, piece, me ^ k, 0)
        return buf

    def both_cores(self, x):
        other = self.sibling(x)
        return jnp.where(self.c == 0, jnp.stack([x, other]), jnp.stack([other, x]))

    def core_part(self, x, core, axis):
        return lax.dynamic_index_in_dim(x, core, axis, keepdims=False)

    def core_swap(self, x, axis):
        own = self.core_part(x, self.c, axis)
        got = self.sibling(self.core_part(x, 1 - self.c, axis))
        first = jnp.where(self.c == 0, own, got)
        second = jnp.where(self.c == 0, got, own)
        return jnp.stack([first, second], axis=axis)

    def gather_tokens(self, x):
        own = self.gather(x, "p")
        other = self.sibling(own)
        first = jnp.where(self.c == 0, own, other)
        second = jnp.where(self.c == 0, other, own)
        return jnp.stack([first, second], axis=1).reshape(-1, x.shape[-1])

    def scatter_tokens(self, part):
        width = part.shape[-1]
        parts = part.reshape(self.spots, 2, -1, width)
        own = self.core_part(parts, self.c, 1)
        got = self.sibling(self.core_part(parts, 1 - self.c, 1))
        chip = own.astype(F32) + got.astype(F32)
        pieces = self.swap(chip.astype(BF), "p")
        total = pieces[0].astype(F32)
        for piece in pieces[1:]:
            total = total + piece.astype(F32)
        return total


def normalize(resid):
    mean = jnp.mean(resid, axis=-1, keepdims=True)
    center = resid - mean
    spread = jnp.mean(center * center, axis=-1, keepdims=True)
    inv = lax.rsqrt(spread + norm_eps)
    return center * inv, inv


def gelu_parts(pre):
    cdf = 0.5 * (1.0 + lax.erf(pre * (2.0**-0.5)))
    return cdf


def on_device(
    mesh, tokens, cotangent, segments, qkv_weight, out_weight, fc_weight, proj_weight,
    biases, ln_gain, ln_shift,
):
    net = Net(mesh)
    spots, planes = net.spots, net.planes
    team = spots * 2
    layers, rows, _ = qkv_weight.shape
    width = out_weight.shape[2]
    local = tokens.shape[1]
    head_cols = width // team
    hidden_all = fc_weight.shape[2]
    fc_piece = proj_weight.shape[1]
    owner = (net.p * planes + net.z) * 2 + net.c
    assert spots == planes

    tokens_own = net.turned(tokens.reshape(local, width))
    seg_row = net.turned(segments)
    full_len = seg_row.shape[1]
    index = lax.broadcasted_iota(jnp.int32, (1, full_len), 1)
    starts = jnp.zeros((1, full_len), jnp.int32)
    for doc in range(3):
        count = jnp.sum((seg_row == doc).astype(jnp.int32))
        starts = starts + jnp.where(seg_row > doc, count, 0)
    position = (index - starts).astype(F32)
    first_block = starts[0, ::BLOCK] // BLOCK
    half = ROT // 2
    entry = jnp.arange(head_cols, dtype=jnp.int32) % HEAD_DIM
    inverse = 10000.0 ** (-2.0 * (entry % half).astype(F32) / ROT)
    inverse = jnp.where(entry < ROT, inverse, 0.0)
    angle = position.reshape(full_len, 1) * inverse[None, :]
    cosine, sine = jnp.cos(angle), jnp.sin(angle)

    small = jnp.concatenate([biases, ln_gain, ln_shift], axis=1)
    small = net.both_cores(small)
    small = net.gather(small, "z")
    small = net.gather(small, "p")
    small = jnp.transpose(small, (3, 4, 0, 1, 2, 5)).reshape(layers, -1, width).astype(F32)
    bias_rows = biases.shape[1]
    bias_all, gain_all, shift_all = (
        small[:, :bias_rows], small[:, bias_rows : bias_rows + 2], small[:, bias_rows + 2 :],
    )
    t_at = net.p * 2 + net.c

    gain_own = ln_gain.astype(F32)
    shift_own = ln_shift.astype(F32)

    def in_weight(layer):
        qkv = qkv_weight[layer].astype(F32) * gain_own[layer, 0][:, None]
        qkv = qkv.astype(BF).reshape(rows, 3, spots, 2, head_cols)
        qkv = jnp.transpose(qkv, (2, 3, 0, 1, 4)).reshape(spots, 2, rows, 3 * head_cols)
        fc = fc_weight[layer].astype(F32) * gain_own[layer, 1][:, None]
        fc = fc.astype(BF).reshape(rows, spots, planes, 2, fc_piece)
        fc = jnp.transpose(fc, (1, 3, 0, 2, 4)).reshape(spots, 2, rows, planes * fc_piece)
        both = jnp.concatenate([qkv, fc], axis=-1)
        both = net.core_swap(both, 1)
        both = net.ordered(net.swap(both, "p"), "p")
        both = net.gather(both, "z")
        both = jnp.transpose(both, (1, 0, 2, 3, 4)).reshape(width, -1)
        return both[:, : 3 * head_cols], both[:, 3 * head_cols :]

    def out_weight_of(layer):
        mine = jnp.concatenate([out_weight[layer], proj_weight[layer]], axis=0)
        col = net.gather(mine, "z")
        heads = col[:, :rows].reshape(2, planes // 2, rows, width)
        heads = net.core_swap(heads, 0)
        heads = jnp.transpose(heads, (1, 0, 2, 3)).reshape(head_cols, width)
        return heads, col[:, rows:].reshape(planes * fc_piece, width)

    weights_in = [in_weight(layer) for layer in range(layers)]
    weights_out = [out_weight_of(layer) for layer in range(layers)]

    def bias_in(layer):
        qkv_b = bias_all[layer, :3].reshape(3, team, head_cols)
        qkv_b = lax.dynamic_index_in_dim(qkv_b, t_at, 1, keepdims=False).reshape(1, -1)
        fc_b = bias_all[layer, 4 : bias_rows - 1].reshape(spots, planes, 2, fc_piece)
        fc_b = lax.dynamic_index_in_dim(fc_b, net.p, 0, keepdims=False)
        fc_b = lax.dynamic_index_in_dim(fc_b, net.c, 1, keepdims=False).reshape(1, -1)
        ratio = shift_all[layer] / gain_all[layer]
        high = ratio.astype(BF)
        low = (ratio - high.astype(F32)).astype(BF)
        qkv_w, fc_w = weights_in[layer]
        qkv_b = qkv_b + nn(high[:1], qkv_w) + nn(low[:1], qkv_w)
        fc_b = fc_b + nn(high[1:], fc_w) + nn(low[1:], fc_w)
        return qkv_b, fc_b

    cot_own = net.turned(cotangent.reshape(local, width))

    resid = tokens_own.astype(F32)
    saved = []
    for layer in range(layers):
        normed, inv = normalize(resid)
        normed_all = net.gather_tokens(normed.astype(BF))
        qkv_w, fc_w = weights_in[layer]
        head_w, proj_w = weights_out[layer]
        qkv_b, fc_b = bias_in(layer)
        mixed = nn(normed_all, qkv_w) + qkv_b
        hidden_pre = nn(normed_all, fc_w) + fc_b
        query, key, value, ctx, ctx_low, lse = attn_forward(
            mixed, cosine, sine, starts, first_block
        )
        hidden = (hidden_pre * gelu_parts(hidden_pre)).astype(BF)
        part = (nn(hidden, proj_w) + nn(ctx_low, head_w)).astype(BF)
        saved.append((normed, inv, normed_all, query, key, value, ctx, ctx_low, lse, hidden_pre, hidden))
        end_bias = bias_all[layer, 3] + bias_all[layer, bias_rows - 1]
        resid = resid + net.scatter_tokens(part) + end_bias[None, :]
    outputs = net.turned(resid.astype(BF)).reshape(1, local, width)

    grads = [None] * layers
    grad_own = cot_own
    for layer in reversed(range(layers)):
        normed, inv, normed_all, query, key, value, ctx, ctx_low, lse, hidden_pre, hidden = saved[layer]
        qkv_w, fc_w = weights_in[layer]
        head_w, proj_w = weights_out[layer]
        grad_all = net.gather_tokens(grad_own)
        grad_ctx = nt(grad_all, head_w).astype(BF)
        grad_mixed = attn_backward(
            query, key, value, ctx, lse, grad_ctx, cosine, sine, starts, first_block
        )
        cdf = gelu_parts(hidden_pre)
        density = jnp.exp(-0.5 * hidden_pre * hidden_pre) * ((2.0 * jnp.pi) ** -0.5)
        grad_pre = (nt(grad_all, proj_w) * (cdf + hidden_pre * density)).astype(BF)
        part = (nt(grad_mixed, qkv_w) + nt(grad_pre, fc_w)).astype(BF)
        norm_grad = net.scatter_tokens(part)
        mean_grad = jnp.mean(norm_grad, axis=-1, keepdims=True)
        mean_dot = jnp.mean(norm_grad * normed, axis=-1, keepdims=True)
        grad_next = grad_own.astype(F32) + inv * (norm_grad - mean_grad - normed * mean_dot)

        grad_heads = tn(ctx_low, grad_all).astype(BF)
        grad_proj = tn(hidden, grad_all).astype(BF)
        grad_heads = grad_heads.reshape(planes // 2, 2, rows, width)
        own = net.core_part(grad_heads, net.c, 1)
        got = net.sibling(net.core_part(grad_heads, 1 - net.c, 1))
        first = jnp.where(net.c == 0, own, got)
        second = jnp.where(net.c == 0, got, own)
        grad_col = jnp.concatenate(
            [
                jnp.concatenate([first, second], axis=0),
                grad_proj.reshape(planes, fc_piece, width),
            ],
            axis=1,
        )
        pieces = net.swap(grad_col, "z")
        grad_out_rows = sum(piece.astype(F32) for piece in pieces)
        grad_in_w = jnp.concatenate(
            [tn(normed_all, grad_mixed).astype(BF), tn(normed_all, grad_pre).astype(BF)], axis=1
        )
        grad_in_w = jnp.moveaxis(grad_in_w.reshape(spots, planes, 2, rows, -1), 1, 0)
        pieces = net.swap(grad_in_w, "z")
        grad_in_w = sum(piece.astype(F32) for piece in pieces).astype(BF)
        grad_in_w = net.core_swap(grad_in_w, 1)
        grad_in_w = net.ordered(net.swap(grad_in_w, "p"), "p").astype(F32)

        sums = jnp.concatenate(
            [
                jnp.sum(grad_mixed.astype(F32), axis=0),
                jnp.sum(grad_pre.astype(F32), axis=0),
                jnp.sum(grad_own.astype(F32), axis=0),
            ]
        )
        in_cols = 3 * head_cols + planes * fc_piece
        sums = sum(net.swap(jnp.broadcast_to(sums, (planes,) + sums.shape), "z"))
        sums = net.gather(net.both_cores(sums), "p")
        end_sum = jnp.sum(sums[:, :, in_cols:], axis=(0, 1))
        qkv_sum = sums[:, :, : 3 * head_cols].reshape(team, 3, head_cols)
        qkv_sum = jnp.transpose(qkv_sum, (1, 0, 2)).reshape(-1)
        fc_sum = sums[:, :, 3 * head_cols : in_cols].reshape(spots, 2, planes, fc_piece)
        fc_sum = jnp.transpose(fc_sum, (0, 2, 1, 3)).reshape(-1)

        grad_qkv = grad_in_w[..., : 3 * head_cols].reshape(team, rows, 3, head_cols)
        grad_qkv = jnp.transpose(grad_qkv, (1, 2, 0, 3)).reshape(rows, -1)
        grad_fc = grad_in_w[..., 3 * head_cols :].reshape(spots, 2, rows, planes, fc_piece)
        grad_fc = jnp.transpose(grad_fc, (2, 0, 3, 1, 4)).reshape(rows, -1)
        qkv_own = qkv_weight[layer].astype(F32)
        fc_own = fc_weight[layer].astype(F32)
        gain_grad = jnp.stack(
            [jnp.sum(qkv_own * grad_qkv, axis=1), jnp.sum(fc_own * grad_fc, axis=1)]
        )
        shift_grad = jnp.stack(
            [jnp.sum(qkv_own * qkv_sum, axis=1), jnp.sum(fc_own * fc_sum, axis=1)]
        )
        gain_l, shift_l = gain_own[layer], shift_own[layer]
        bias_grad = jnp.concatenate([qkv_sum, end_sum, fc_sum, end_sum]).reshape(bias_rows, width)
        bias_grad = lax.dynamic_slice_in_dim(bias_grad, owner * rows, rows, 1)
        grads[layer] = (
            gain_l[0][:, None] * grad_qkv + shift_l[0][:, None] * qkv_sum[None, :],
            grad_out_rows[:rows],
            gain_l[1][:, None] * grad_fc + shift_l[1][:, None] * fc_sum[None, :],
            grad_out_rows[rows:],
            bias_grad,
            gain_grad,
            shift_grad,
        )
        grad_own = lax.optimization_barrier(grad_next.astype(BF))
    grad_tokens = net.turned(grad_own).reshape(1, local, width)
    stacked = [jnp.stack([grads[layer][slot] for layer in range(layers)]) for slot in range(7)]
    return (outputs, grad_tokens, *stacked)


def solution(mesh):
    return jax.shard_map(
        functools.partial(on_device, mesh),
        mesh=mesh,
        in_specs=(
            P("dp", "seq", None),
            P("dp", "seq", None),
            P("dp", None),
            P(None, ("dp", "seq"), None),
            P(None, ("dp", "seq"), None),
            P(None, ("dp", "seq"), None),
            P(None, ("dp", "seq"), None),
            P(None, None, ("dp", "seq")),
            P(None, None, ("dp", "seq")),
            P(None, None, ("dp", "seq")),
        ),
        out_specs=(
            P("dp", "seq", None),
            P("dp", "seq", None),
            P(None, ("dp", "seq"), None),
            P(None, ("dp", "seq"), None),
            P(None, ("dp", "seq"), None),
            P(None, ("dp", "seq"), None),
            P(None, None, ("dp", "seq")),
            P(None, None, ("dp", "seq")),
            P(None, None, ("dp", "seq")),
        ),
        check_vma=False,
    )
```

```python
import functools

import jax
import jax.numpy as jnp
from jax import lax
from jax.experimental import pallas as pl
from jax.experimental.pallas import tpu as pltpu
from jax.sharding import PartitionSpec as P

HEAD_DIM = 64
ROT = 16
norm_eps = 1e-05
mask_fill = -1e30
BF = jnp.bfloat16
F32 = jnp.float32
AXES = ("dp", "seq")
BLOCK = 256


def nt(left, right):
    return lax.dot_general(left, right, (((1,), (1,)), ((), ())), preferred_element_type=F32)


def nn(left, right):
    return lax.dot_general(left, right, (((1,), (0,)), ((), ())), preferred_element_type=F32)


def tn(left, right):
    return lax.dot_general(left, right, (((0,), (0,)), ((), ())), preferred_element_type=F32)


def lane_in_head(shape):
    lane = lax.broadcasted_iota(jnp.int32, shape, len(shape) - 1)
    return lane, lane % HEAD_DIM


def rope(vals, cosine, sine):
    width = vals.shape[-1]
    half = ROT // 2
    _, entry = lane_in_head(vals.shape)
    up = pltpu.roll(vals, width - half, 1)
    down = pltpu.roll(vals, half, 1)
    swapped = jnp.where(entry < half, -up, down)
    return vals * cosine + swapped * sine


def rope_back(grads, cosine, sine):
    width = grads.shape[-1]
    half = ROT // 2
    _, entry = lane_in_head(grads.shape)
    scaled = grads * sine
    up = pltpu.roll(scaled, width - half, 1)
    down = pltpu.roll(scaled, half, 1)
    swapped = jnp.where(entry < half, up, jnp.where(entry < ROT, -down, 0.0))
    return grads * cosine + swapped


def head_only(vals, head):
    lane, _ = lane_in_head(vals.shape)
    keep = (lane >= head * HEAD_DIM) & (lane < (head + 1) * HEAD_DIM)
    return jnp.where(keep, vals, jnp.zeros_like(vals))


def attn_fwd_kernel(
    first_ref, mixed_ref, cos_ref, sin_ref, start_ref,
    query_ref, key_ref, value_ref, ctx_ref, ctx_low_ref, lse_ref,
    value_t_ref,
):
    at = pl.program_id(0)
    total, width = key_ref.shape
    heads = width // HEAD_DIM

    @pl.when(at == 0)
    def _():
        def one(i, carry):
            rows = pl.ds(pl.multiple_of(i * BLOCK, BLOCK), BLOCK)
            keys = mixed_ref[rows, width : 2 * width]
            key_ref[rows, :] = rope(keys, cos_ref[rows, :], sin_ref[rows, :]).astype(BF)
            vals = mixed_ref[rows, 2 * width : 3 * width]
            value_ref[rows, :] = vals.astype(BF)
            value_t_ref[:, rows] = vals.T.astype(BF)
            return carry

        lax.fori_loop(0, total // BLOCK, one, 0)

    rows = pl.ds(pl.multiple_of(at * BLOCK, BLOCK), BLOCK)
    quer = rope(mixed_ref[rows, 0:width], cos_ref[rows, :], sin_ref[rows, :]).astype(BF)
    quer = quer * jnp.asarray(HEAD_DIM**-0.5, BF)
    query_ref[...] = quer
    by_head = [head_only(quer, h) for h in range(heads)]
    key_iota = lax.broadcasted_iota(jnp.int32, (BLOCK, BLOCK), 0)
    query_pos = at * BLOCK + lax.broadcasted_iota(jnp.int32, (1, BLOCK), 1)
    starts = start_ref[...]

    def step(turn, carry):
        block = at - turn
        keys_at = pl.ds(pl.multiple_of(block * BLOCK, BLOCK), BLOCK)
        keys = key_ref[keys_at, :]
        vals_t = value_t_ref[:, keys_at]
        keep = (key_iota >= starts - block * BLOCK) & (key_iota <= query_pos - block * BLOCK)
        out = []
        for h in range(heads):
            top, total_h, acc = carry[h]
            scores = jnp.where(keep, nt(keys, by_head[h]), mask_fill)
            new_top = jnp.maximum(top, jnp.max(scores, axis=0, keepdims=True))
            fade = jnp.exp(top - new_top)
            probs = jnp.exp(scores - new_top)
            total_h = total_h * fade + jnp.sum(probs, axis=0, keepdims=True)
            acc = acc * fade + nn(vals_t, probs.astype(BF))
            out.append((new_top, total_h, acc))
        return tuple(out)

    init = tuple(
        (
            jnp.full((1, BLOCK), mask_fill, F32),
            jnp.zeros((1, BLOCK), F32),
            jnp.zeros((width, BLOCK), F32),
        )
        for h in range(heads)
    )
    done = lax.fori_loop(0, at - first_ref[at] + 1, step, init)
    parts = []
    for h in range(heads):
        top, total_h, acc = done[h]
        lse_ref[h : h + 1, :] = top + jnp.log(total_h)
        parts.append(acc[h * HEAD_DIM : (h + 1) * HEAD_DIM, :] / total_h)
    ctx = jnp.concatenate(parts, axis=0).T
    ctx_ref[...] = ctx
    ctx_low_ref[...] = ctx.astype(BF)


def attn_forward(mixed, cosine, sine, starts, first_block):
    total, width = cosine.shape
    heads = width // HEAD_DIM
    blocks = total // BLOCK
    full = lambda cols: pl.BlockSpec((total, cols), lambda i, f: (0, 0))
    rows = pl.BlockSpec((BLOCK, width), lambda i, f: (i, 0))
    lanes = lambda n: pl.BlockSpec((n, BLOCK), lambda i, f: (0, i))
    wide = jax.ShapeDtypeStruct((total, width), BF)
    return pl.pallas_call(
        attn_fwd_kernel,
        grid_spec=pltpu.PrefetchScalarGridSpec(
            num_scalar_prefetch=1,
            grid=(blocks,),
            in_specs=[full(3 * width), full(width), full(width), lanes(1)],
            out_specs=[rows, full(width), full(width), rows, rows, lanes(heads)],
            scratch_shapes=[pltpu.VMEM((width, total), BF)],
        ),
        out_shape=[
            wide, wide, wide,
            jax.ShapeDtypeStruct((total, width), F32),
            wide,
            jax.ShapeDtypeStruct((heads, total), F32),
        ],
        compiler_params=pltpu.CompilerParams(
            dimension_semantics=("arbitrary",), vmem_limit_bytes=40 << 20
        ),
        cost_estimate=pl.CostEstimate(
            flops=20 * 4 * BLOCK * BLOCK * width * heads,
            bytes_accessed=total * width * 40,
            transcendentals=20 * BLOCK * BLOCK * heads,
        ),
        name="attn_fwd",
    )(first_block, mixed, cosine, sine, starts)


def attn_bwd_kernel(
    first_ref, query_ref, key_ref, value_ref, ctx_ref, lse_ref, grad_ref, cos_ref, sin_ref, start_ref,
    out_ref,
    key_t_ref, grad_key_ref, grad_value_ref,
):
    at = pl.program_id(0)
    total, width = key_ref.shape
    heads = width // HEAD_DIM

    @pl.when(at == 0)
    def _():
        def one(i, carry):
            rows = pl.ds(pl.multiple_of(i * BLOCK, BLOCK), BLOCK)
            key_t_ref[:, rows] = key_ref[rows, :].T
            grad_key_ref[rows, :] = jnp.zeros((BLOCK, width), F32)
            grad_value_ref[rows, :] = jnp.zeros((BLOCK, width), F32)
            return carry

        lax.fori_loop(0, total // BLOCK, one, 0)

    quer = query_ref[...]
    grad = grad_ref[...]
    by_head = [head_only(quer, h) for h in range(heads)]
    grad_head = [head_only(grad, h) for h in range(heads)]
    inner_t = (grad.astype(F32) * ctx_ref[...]).T
    inner = [
        jnp.sum(inner_t[h * HEAD_DIM : (h + 1) * HEAD_DIM, :], axis=0, keepdims=True)
        for h in range(heads)
    ]
    logs = [lse_ref[h : h + 1, :] for h in range(heads)]
    key_iota = lax.broadcasted_iota(jnp.int32, (BLOCK, BLOCK), 0)
    query_pos = at * BLOCK + lax.broadcasted_iota(jnp.int32, (1, BLOCK), 1)
    starts = start_ref[...]

    def step(turn, carry):
        block = at - turn
        keys_at = pl.ds(pl.multiple_of(block * BLOCK, BLOCK), BLOCK)
        keys = key_ref[keys_at, :]
        vals = value_ref[keys_at, :]
        keys_t = key_t_ref[:, keys_at]
        keep = (key_iota >= starts - block * BLOCK) & (key_iota <= query_pos - block * BLOCK)
        out = []
        grad_key = jnp.zeros((BLOCK, width), F32)
        grad_value = jnp.zeros((BLOCK, width), F32)
        for h in range(heads):
            scores = nt(keys, by_head[h])
            probs = jnp.where(keep, jnp.exp(jnp.where(keep, scores, mask_fill) - logs[h]), 0.0)
            grad_probs = nt(vals, grad_head[h])
            grad_scores = (probs * (grad_probs - inner[h])).astype(BF)
            grad_value = grad_value + nn(probs.astype(BF), grad_head[h])
            grad_key = grad_key + nn(grad_scores, by_head[h])
            out.append(carry[h] + nn(keys_t, grad_scores))
        grad_key_ref[keys_at, :] += grad_key
        grad_value_ref[keys_at, :] += grad_value
        return tuple(out)

    init = tuple(jnp.zeros((width, BLOCK), F32) for h in range(heads))
    done = lax.fori_loop(0, at - first_ref[at] + 1, step, init)
    parts = [done[h][h * HEAD_DIM : (h + 1) * HEAD_DIM, :] for h in range(heads)]
    grad_query = jnp.concatenate(parts, axis=0).T * (HEAD_DIM**-0.5)
    rows = pl.ds(pl.multiple_of(at * BLOCK, BLOCK), BLOCK)
    out_ref[rows, 0:width] = rope_back(grad_query, cos_ref[rows, :], sin_ref[rows, :]).astype(BF)

    @pl.when(at == pl.num_programs(0) - 1)
    def _():
        def one(i, carry):
            rows = pl.ds(pl.multiple_of(i * BLOCK, BLOCK), BLOCK)
            grad_key = rope_back(grad_key_ref[rows, :], cos_ref[rows, :], sin_ref[rows, :])
            out_ref[rows, width : 2 * width] = grad_key.astype(BF)
            out_ref[rows, 2 * width : 3 * width] = grad_value_ref[rows, :].astype(BF)
            return carry

        lax.fori_loop(0, total // BLOCK, one, 0)


def attn_backward(query, key, value, ctx, lse, grad_ctx, cosine, sine, starts, first_block):
    total, width = cosine.shape
    heads = width // HEAD_DIM
    blocks = total // BLOCK
    full = lambda cols: pl.BlockSpec((total, cols), lambda i, f: (0, 0))
    rows = pl.BlockSpec((BLOCK, width), lambda i, f: (i, 0))
    lanes = lambda n: pl.BlockSpec((n, BLOCK), lambda i, f: (0, i))
    return pl.pallas_call(
        attn_bwd_kernel,
        grid_spec=pltpu.PrefetchScalarGridSpec(
            num_scalar_prefetch=1,
            grid=(blocks,),
            in_specs=[
                rows, full(width), full(width), rows, lanes(heads), rows,
                full(width), full(width), lanes(1),
            ],
            out_specs=full(3 * width),
            scratch_shapes=[
                pltpu.VMEM((width, total), BF),
                pltpu.VMEM((total, width), F32),
                pltpu.VMEM((total, width), F32),
            ],
        ),
        out_shape=jax.ShapeDtypeStruct((total, 3 * width), BF),
        compiler_params=pltpu.CompilerParams(
            dimension_semantics=("arbitrary",), vmem_limit_bytes=40 << 20
        ),
        cost_estimate=pl.CostEstimate(
            flops=20 * 10 * BLOCK * BLOCK * width * heads,
            bytes_accessed=total * width * 40,
            transcendentals=20 * BLOCK * BLOCK * heads,
        ),
        name="attn_bwd",
    )(first_block, query, key, value, ctx, lse, grad_ctx, cosine, sine, starts)


MESH = pl.DeviceIdType.MESH


def partners(p, spots):
    if spots == 4:
        return [p + 1 - 2 * (p % 2), p + 2 - 4 * (p // 2)]
    return [(p + k) % spots for k in range(1, spots)]


def greet(p, s, near, others):
    barrier = pltpu.get_barrier_semaphore()
    for q in others:
        pl.semaphore_signal(barrier, inc=1, device_id=(q, s), device_id_type=MESH)
    pl.semaphore_signal(barrier, inc=1, device_id=(p, near), device_id_type=MESH)
    pl.semaphore_wait(barrier, len(others) + 1)


def gather_kernel(spots, own_ref, all_ref, copy_sem, send_sem, recv_sem, near_send, near_recv):
    p, s = lax.axis_index("dp"), lax.axis_index("seq")
    c = s % 2
    near = s + 1 - 2 * c
    others = partners(p, spots)
    groups = own_ref.shape[0]
    half = groups // 2
    halves = [pl.ds(0, half), pl.ds(half, half)]
    whole = pl.ds(0, groups)
    greet(p, s, near, others)

    def far(source, part, spot, dest, at):
        return pltpu.make_async_remote_copy(
            src_ref=source, dst_ref=all_ref.at[part, c, spot],
            send_sem=send_sem.at[at], recv_sem=recv_sem.at[at],
            device_id=(dest, s), device_id_type=MESH,
        )

    def close(source, part, spot, at):
        return pltpu.make_async_remote_copy(
            src_ref=source, dst_ref=all_ref.at[part, c, spot],
            send_sem=near_send.at[at], recv_sem=near_recv.at[at],
            device_id=(p, near), device_id_type=MESH,
        )

    keep = pltpu.make_async_copy(own_ref, all_ref.at[whole, c, p], copy_sem)
    if spots == 4:
        x, y = others
        first, last = own_ref.at[halves[0]], own_ref.at[halves[1]]
        sent = [
            far(first, halves[0], p, x, 0),
            far(last, halves[1], p, y, 1),
            far(last, halves[1], p, x, 2),
            far(first, halves[0], p, y, 3),
        ]
        for copy in sent:
            copy.start()
        relays = {
            0: far(all_ref.at[halves[0], c, x], halves[0], x, y, 4),
            1: far(all_ref.at[halves[1], c, y], halves[1], y, x, 5),
        }
        sent += [relays[0], relays[1]]
        diagonal = 3 - p
        arrivals = [
            (halves[0], x), (halves[1], y), (halves[1], x),
            (halves[0], y), (halves[0], diagonal), (halves[1], diagonal),
        ]
    else:
        sent = [far(own_ref, whole, p, q, at) for at, q in enumerate(others)]
        for copy in sent:
            copy.start()
        relays = {}
        arrivals = [(whole, (p + spots - k) % spots) for k in range(1, spots)]
    count = len(arrivals)
    passed = [close(own_ref, whole, p, count)]
    passed[0].start()
    keep.start()
    for at, (part, spot) in enumerate(arrivals):
        sent[at].wait_recv()
        if at in relays:
            relays[at].start()
        copy = close(all_ref.at[part, c, spot], part, spot, at)
        copy.start()
        passed.append(copy)
    keep.wait()
    for copy in passed:
        copy.wait_recv()
    for copy in sent + passed:
        copy.wait_send()


def gather_tokens(own, spots):
    groups, rows, width = own.shape
    count = 6 if spots == 4 else spots - 1
    whole = pl.pallas_call(
        functools.partial(gather_kernel, spots),
        out_shape=jax.ShapeDtypeStruct((groups, 2, spots, rows, width), own.dtype),
        in_specs=[pl.BlockSpec(memory_space=pltpu.VMEM)],
        out_specs=pl.BlockSpec(memory_space=pl.ANY),
        scratch_shapes=[
            pltpu.SemaphoreType.DMA,
            pltpu.SemaphoreType.DMA((count,)),
            pltpu.SemaphoreType.DMA((count,)),
            pltpu.SemaphoreType.DMA((count + 1,)),
            pltpu.SemaphoreType.DMA((count + 1,)),
        ],
        compiler_params=pltpu.CompilerParams(collective_id=1, has_side_effects=True),
        name="gather_tokens",
    )(own)
    return whole.reshape(-1, width)


def scatter_kernel(
    spots, part_ref, out_ref, near_buf, mine, relay, inbox,
    copy_sem, near_send, near_recv, send_sem, recv_sem,
):
    p, s = lax.axis_index("dp"), lax.axis_index("seq")
    c = s % 2
    near = s + 1 - 2 * c
    others = partners(p, spots)
    _, groups, rows, width = mine.shape
    half = groups // 2
    halves = [pl.ds(0, half), pl.ds(half, half)]
    whole = pl.ds(0, groups)
    step = min(rows, 16)
    greet(p, s, near, others)
    if spots == 4:
        x, y = others
        spot_of = [p, x, y, 3 - p]
        order = [3, 1, 2, 0]
    else:
        spot_of = [p] + others
        order = list(range(1, spots)) + [0]
    handed, kept = {}, {}
    for m in order:
        handed[m] = pltpu.make_async_remote_copy(
            src_ref=part_ref.at[whole, 1 - c, spot_of[m]], dst_ref=near_buf.at[m],
            send_sem=near_send.at[m], recv_sem=near_recv.at[m],
            device_id=(p, near), device_id_type=MESH,
        )
        kept[m] = pltpu.make_async_copy(
            part_ref.at[whole, c, spot_of[m]], mine.at[m], copy_sem.at[m]
        )
        handed[m].start()
        kept[m].start()

    def add(first, count, into, left, right):
        per = rows // step

        def one(i, carry):
            g = first + i // per
            at = pl.ds(pl.multiple_of((i % per) * step, step), step)
            into[g, at, :] = (left(g, at) + right(g, at)).astype(into.dtype)
            return carry

        lax.fori_loop(0, count * per, one, 0)

    def far(m, part, slot, dest, at):
        return pltpu.make_async_remote_copy(
            src_ref=mine.at[m, part], dst_ref=slot,
            send_sem=send_sem.at[at], recv_sem=recv_sem.at[at],
            device_id=(dest, s), device_id_type=MESH,
        )

    sent = {}
    for m in order:
        handed[m].wait_recv()
        kept[m].wait()
        into = out_ref if m == 0 else mine.at[m]
        add(
            0, groups, into,
            lambda g, at: mine[m, g, at, :].astype(F32),
            lambda g, at: near_buf[m, g, at, :].astype(F32),
        )
        if spots == 4:
            if m == 3:
                sent[0] = far(3, halves[0], relay.at[0], x, 0)
                sent[1] = far(3, halves[1], relay.at[1], y, 1)
                sent[0].start()
                sent[1].start()
            elif m == 1:
                sent[2] = far(1, halves[0], inbox.at[0, halves[0]], x, 2)
                sent[2].start()
            elif m == 2:
                sent[3] = far(2, halves[1], inbox.at[1, halves[1]], y, 3)
                sent[3].start()
        elif m > 0:
            sent[m - 1] = far(m, whole, inbox.at[m - 1], others[m - 1], m - 1)
            sent[m - 1].start()
    if spots == 4:
        sent[0].wait_recv()
        add(
            0, half, mine.at[2],
            lambda g, at: mine[2, g, at, :].astype(F32),
            lambda g, at: relay[0, g, at, :].astype(F32),
        )
        sent[4] = far(2, halves[0], inbox.at[1, halves[0]], y, 4)
        sent[4].start()
        sent[1].wait_recv()
        add(
            half, half, mine.at[1],
            lambda g, at: mine[1, g, at, :].astype(F32),
            lambda g, at: relay[1, g - half, at, :].astype(F32),
        )
        sent[5] = far(1, halves[1], inbox.at[0, halves[1]], x, 5)
        sent[5].start()
        for at in (2, 3, 4, 5):
            sent[at].wait_recv()
    else:
        for at in sent:
            sent[at].wait_recv()

    def received(g, at):
        total = inbox[0, g, at, :].astype(F32)
        for slot in range(1, inbox.shape[0]):
            total = total + inbox[slot, g, at, :].astype(F32)
        return total

    add(0, groups, out_ref, lambda g, at: out_ref[g, at, :], received)
    for m in order:
        handed[m].wait_send()
    for at in sent:
        sent[at].wait_send()


def scatter_tokens(part, groups, spots):
    total, width = part.shape
    rows = total // (groups * 2 * spots)
    far = 6 if spots == 4 else spots - 1
    slots = 2 if spots == 4 else spots - 1
    return pl.pallas_call(
        functools.partial(scatter_kernel, spots),
        out_shape=jax.ShapeDtypeStruct((groups, rows, width), F32),
        in_specs=[pl.BlockSpec(memory_space=pl.ANY)],
        out_specs=pl.BlockSpec(memory_space=pltpu.VMEM),
        scratch_shapes=[
            pltpu.VMEM((spots, groups, rows, width), BF),
            pltpu.VMEM((spots, groups, rows, width), BF),
            pltpu.VMEM((2, groups // 2, rows, width), BF),
            pltpu.VMEM((slots, groups, rows, width), BF),
            pltpu.SemaphoreType.DMA((spots,)),
            pltpu.SemaphoreType.DMA((spots,)),
            pltpu.SemaphoreType.DMA((spots,)),
            pltpu.SemaphoreType.DMA((far,)),
            pltpu.SemaphoreType.DMA((far,)),
        ],
        compiler_params=pltpu.CompilerParams(
            collective_id=2, has_side_effects=True, vmem_limit_bytes=32 << 20
        ),
        name="scatter_tokens",
    )(part.reshape(groups, 2, spots, rows, width))


class Net:
    def __init__(self, mesh):
        self.planes = mesh.shape["seq"] // 2
        self.spots = mesh.shape["dp"]
        self.p = lax.axis_index("dp")
        self.z = lax.axis_index("seq") // 2
        self.c = lax.axis_index("seq") % 2

    def permute(self, x, to):
        pairs = []
        for p in range(self.spots):
            for z in range(self.planes):
                for c in range(2):
                    tp, tz, tc = to(p, z, c)
                    source = (p * self.planes + z) * 2 + c
                    pairs.append((source, (tp * self.planes + tz) * 2 + tc))
        return lax.ppermute(x, AXES, pairs)

    def sibling(self, x):
        return self.permute(x, lambda p, z, c: (p, z, 1 - c))

    def turned(self, x):
        return self.permute(x, lambda p, z, c: (z, p, c))

    def gather(self, x, axis):
        count = self.spots if axis == "p" else self.planes
        me = self.p if axis == "p" else self.z
        buf = jnp.zeros((count,) + x.shape, x.dtype)
        buf = lax.dynamic_update_index_in_dim(buf, x, me, 0)
        for k in range(1, count):
            if axis == "p":
                got = self.permute(x, lambda p, z, c: (p ^ k, z, c))
            else:
                got = self.permute(x, lambda p, z, c: (p, z ^ k, c))
            buf = lax.dynamic_update_index_in_dim(buf, got, me ^ k, 0)
        return buf

    def swap(self, x, axis):
        count = self.spots if axis == "p" else self.planes
        me = self.p if axis == "p" else self.z
        pieces = [lax.dynamic_index_in_dim(x, me, 0, keepdims=False)]
        for k in range(1, count):
            piece = lax.dynamic_index_in_dim(x, me ^ k, 0, keepdims=False)
            if axis == "p":
                pieces.append(self.permute(piece, lambda p, z, c: (p ^ k, z, c)))
            else:
                pieces.append(self.permute(piece, lambda p, z, c: (p, z ^ k, c)))
        return pieces

    def ordered(self, pieces, axis):
        me = self.p if axis == "p" else self.z
        buf = jnp.zeros((len(pieces),) + pieces[0].shape, pieces[0].dtype)
        for k, piece in enumerate(pieces):
            buf = lax.dynamic_update_index_in_dim(buf, piece, me ^ k, 0)
        return buf

    def both_cores(self, x):
        other = self.sibling(x)
        return jnp.where(self.c == 0, jnp.stack([x, other]), jnp.stack([other, x]))

    def core_part(self, x, core, axis):
        return lax.dynamic_index_in_dim(x, core, axis, keepdims=False)

    def core_swap(self, x, axis):
        own = self.core_part(x, self.c, axis)
        got = self.sibling(self.core_part(x, 1 - self.c, axis))
        first = jnp.where(self.c == 0, own, got)
        second = jnp.where(self.c == 0, got, own)
        return jnp.stack([first, second], axis=axis)

    def to_plane(self, x):
        local, width = x.shape
        x = x.reshape(self.spots, local // self.spots, width)
        x = self.ordered(self.swap(x, "p"), "p")
        return self.ordered(self.swap(x, "z"), "z")

    def from_plane(self, x):
        x = self.ordered(self.swap(x, "z"), "z")
        x = self.ordered(self.swap(x, "p"), "p")
        return x.reshape(1, -1, x.shape[-1])


def normalize(resid):
    mean = jnp.mean(resid, axis=-1, keepdims=True)
    center = resid - mean
    spread = jnp.mean(center * center, axis=-1, keepdims=True)
    inv = lax.rsqrt(spread + norm_eps)
    return center * inv, inv


def gelu_parts(pre):
    cdf = 0.5 * (1.0 + lax.erf(pre * (2.0**-0.5)))
    return cdf


def on_device(
    mesh, tokens, cotangent, segments, qkv_weight, out_weight, fc_weight, proj_weight,
    biases, ln_gain, ln_shift,
):
    net = Net(mesh)
    spots, planes = net.spots, net.planes
    team = spots * 2
    layers, rows, _ = qkv_weight.shape
    width = out_weight.shape[2]
    local = tokens.shape[1]
    head_cols = width // team
    hidden_all = fc_weight.shape[2]
    fc_piece = proj_weight.shape[1]
    owner = (net.p * planes + net.z) * 2 + net.c
    assert spots == planes

    tokens_own = net.to_plane(tokens.reshape(local, width))
    seg_row = net.turned(segments)
    full_len = seg_row.shape[1]
    index = lax.broadcasted_iota(jnp.int32, (1, full_len), 1)
    starts = jnp.zeros((1, full_len), jnp.int32)
    for doc in range(3):
        count = jnp.sum((seg_row == doc).astype(jnp.int32))
        starts = starts + jnp.where(seg_row > doc, count, 0)
    position = (index - starts).astype(F32)
    first_block = starts[0, ::BLOCK] // BLOCK
    half = ROT // 2
    entry = jnp.arange(head_cols, dtype=jnp.int32) % HEAD_DIM
    inverse = 10000.0 ** (-2.0 * (entry % half).astype(F32) / ROT)
    inverse = jnp.where(entry < ROT, inverse, 0.0)
    angle = position.reshape(full_len, 1) * inverse[None, :]
    cosine, sine = jnp.cos(angle), jnp.sin(angle)

    small = jnp.concatenate([biases, ln_gain, ln_shift], axis=1)
    small = net.both_cores(small)
    small = net.gather(small, "z")
    small = net.gather(small, "p")
    small = jnp.transpose(small, (3, 4, 0, 1, 2, 5)).reshape(layers, -1, width).astype(F32)
    bias_rows = biases.shape[1]
    bias_all, gain_all, shift_all = (
        small[:, :bias_rows], small[:, bias_rows : bias_rows + 2], small[:, bias_rows + 2 :],
    )
    t_at = net.p * 2 + net.c

    gain_own = ln_gain.astype(F32)
    shift_own = ln_shift.astype(F32)

    def in_weight(layer):
        qkv = qkv_weight[layer].astype(F32) * gain_own[layer, 0][:, None]
        qkv = qkv.astype(BF).reshape(rows, 3, spots, 2, head_cols)
        qkv = jnp.transpose(qkv, (2, 3, 0, 1, 4)).reshape(spots, 2, rows, 3 * head_cols)
        fc = fc_weight[layer].astype(F32) * gain_own[layer, 1][:, None]
        fc = fc.astype(BF).reshape(rows, spots, planes, 2, fc_piece)
        fc = jnp.transpose(fc, (1, 3, 0, 2, 4)).reshape(spots, 2, rows, planes * fc_piece)
        both = jnp.concatenate([qkv, fc], axis=-1)
        both = net.core_swap(both, 1)
        both = net.ordered(net.swap(both, "p"), "p")
        both = net.gather(both, "z")
        both = jnp.transpose(both, (1, 0, 2, 3, 4)).reshape(width, -1)
        return both[:, : 3 * head_cols], both[:, 3 * head_cols :]

    def out_weight_of(layer):
        mine = jnp.concatenate([out_weight[layer], proj_weight[layer]], axis=0)
        col = net.gather(mine, "z")
        heads = col[:, :rows].reshape(2, planes // 2, rows, width)
        heads = net.core_swap(heads, 0)
        heads = jnp.transpose(heads, (1, 0, 2, 3)).reshape(head_cols, width)
        return heads, col[:, rows:].reshape(planes * fc_piece, width)

    weights_in = [in_weight(layer) for layer in range(layers)]
    weights_out = [out_weight_of(layer) for layer in range(layers)]

    def bias_in(layer):
        qkv_b = bias_all[layer, :3].reshape(3, team, head_cols)
        qkv_b = lax.dynamic_index_in_dim(qkv_b, t_at, 1, keepdims=False).reshape(1, -1)
        fc_b = bias_all[layer, 4 : bias_rows - 1].reshape(spots, planes, 2, fc_piece)
        fc_b = lax.dynamic_index_in_dim(fc_b, net.p, 0, keepdims=False)
        fc_b = lax.dynamic_index_in_dim(fc_b, net.c, 1, keepdims=False).reshape(1, -1)
        ratio = shift_all[layer] / gain_all[layer]
        high = ratio.astype(BF)
        low = (ratio - high.astype(F32)).astype(BF)
        qkv_w, fc_w = weights_in[layer]
        qkv_b = qkv_b + nn(high[:1], qkv_w) + nn(low[:1], qkv_w)
        fc_b = fc_b + nn(high[1:], fc_w) + nn(low[1:], fc_w)
        return qkv_b, fc_b

    cot_own = net.to_plane(cotangent.reshape(local, width))

    resid = tokens_own.astype(F32)
    saved = []
    for layer in range(layers):
        normed, inv = normalize(resid)
        normed_all = gather_tokens(normed.astype(BF), spots)
        qkv_w, fc_w = weights_in[layer]
        head_w, proj_w = weights_out[layer]
        qkv_b, fc_b = bias_in(layer)
        mixed = nn(normed_all, qkv_w) + qkv_b
        hidden_pre = nn(normed_all, fc_w) + fc_b
        query, key, value, ctx, ctx_low, lse = attn_forward(
            mixed, cosine, sine, starts, first_block
        )
        hidden = (hidden_pre * gelu_parts(hidden_pre)).astype(BF)
        part = (nn(hidden, proj_w) + nn(ctx_low, head_w)).astype(BF)
        saved.append((normed, inv, normed_all, query, key, value, ctx, ctx_low, lse, hidden_pre, hidden))
        end_bias = bias_all[layer, 3] + bias_all[layer, bias_rows - 1]
        resid = resid + scatter_tokens(part, planes, spots) + end_bias
    outputs = net.from_plane(resid.astype(BF))

    grads = [None] * layers
    grad_own = cot_own
    for layer in reversed(range(layers)):
        normed, inv, normed_all, query, key, value, ctx, ctx_low, lse, hidden_pre, hidden = saved[layer]
        qkv_w, fc_w = weights_in[layer]
        head_w, proj_w = weights_out[layer]
        grad_all = gather_tokens(grad_own, spots)
        grad_ctx = nt(grad_all, head_w).astype(BF)
        grad_mixed = attn_backward(
            query, key, value, ctx, lse, grad_ctx, cosine, sine, starts, first_block
        )
        cdf = gelu_parts(hidden_pre)
        density = jnp.exp(-0.5 * hidden_pre * hidden_pre) * ((2.0 * jnp.pi) ** -0.5)
        grad_pre = (nt(grad_all, proj_w) * (cdf + hidden_pre * density)).astype(BF)
        part = (nt(grad_mixed, qkv_w) + nt(grad_pre, fc_w)).astype(BF)
        norm_grad = scatter_tokens(part, planes, spots)
        mean_grad = jnp.mean(norm_grad, axis=-1, keepdims=True)
        mean_dot = jnp.mean(norm_grad * normed, axis=-1, keepdims=True)
        grad_next = grad_own.astype(F32) + inv * (norm_grad - mean_grad - normed * mean_dot)

        grad_heads = tn(ctx_low, grad_all).astype(BF)
        grad_proj = tn(hidden, grad_all).astype(BF)
        grad_heads = grad_heads.reshape(planes // 2, 2, rows, width)
        own = net.core_part(grad_heads, net.c, 1)
        got = net.sibling(net.core_part(grad_heads, 1 - net.c, 1))
        first = jnp.where(net.c == 0, own, got)
        second = jnp.where(net.c == 0, got, own)
        grad_col = jnp.concatenate(
            [
                jnp.concatenate([first, second], axis=0),
                grad_proj.reshape(planes, fc_piece, width),
            ],
            axis=1,
        )
        pieces = net.swap(grad_col, "z")
        grad_out_rows = sum(piece.astype(F32) for piece in pieces)
        grad_in_w = jnp.concatenate(
            [tn(normed_all, grad_mixed).astype(BF), tn(normed_all, grad_pre).astype(BF)], axis=1
        )
        grad_in_w = jnp.moveaxis(grad_in_w.reshape(spots, planes, 2, rows, -1), 1, 0)
        pieces = net.swap(grad_in_w, "z")
        grad_in_w = sum(piece.astype(F32) for piece in pieces).astype(BF)
        grad_in_w = net.core_swap(grad_in_w, 1)
        grad_in_w = net.ordered(net.swap(grad_in_w, "p"), "p").astype(F32)

        sums = jnp.concatenate(
            [
                jnp.sum(grad_mixed.astype(F32), axis=0),
                jnp.sum(grad_pre.astype(F32), axis=0),
                jnp.sum(grad_own.astype(F32), axis=(0, 1)),
            ]
        )
        in_cols = 3 * head_cols + planes * fc_piece
        sums = sum(net.swap(jnp.broadcast_to(sums, (planes,) + sums.shape), "z"))
        sums = net.gather(net.both_cores(sums), "p")
        end_sum = jnp.sum(sums[:, :, in_cols:], axis=(0, 1))
        qkv_sum = sums[:, :, : 3 * head_cols].reshape(team, 3, head_cols)
        qkv_sum = jnp.transpose(qkv_sum, (1, 0, 2)).reshape(-1)
        fc_sum = sums[:, :, 3 * head_cols : in_cols].reshape(spots, 2, planes, fc_piece)
        fc_sum = jnp.transpose(fc_sum, (0, 2, 1, 3)).reshape(-1)

        grad_qkv = grad_in_w[..., : 3 * head_cols].reshape(team, rows, 3, head_cols)
        grad_qkv = jnp.transpose(grad_qkv, (1, 2, 0, 3)).reshape(rows, -1)
        grad_fc = grad_in_w[..., 3 * head_cols :].reshape(spots, 2, rows, planes, fc_piece)
        grad_fc = jnp.transpose(grad_fc, (2, 0, 3, 1, 4)).reshape(rows, -1)
        qkv_own = qkv_weight[layer].astype(F32)
        fc_own = fc_weight[layer].astype(F32)
        gain_grad = jnp.stack(
            [jnp.sum(qkv_own * grad_qkv, axis=1), jnp.sum(fc_own * grad_fc, axis=1)]
        )
        shift_grad = jnp.stack(
            [jnp.sum(qkv_own * qkv_sum, axis=1), jnp.sum(fc_own * fc_sum, axis=1)]
        )
        gain_l, shift_l = gain_own[layer], shift_own[layer]
        bias_grad = jnp.concatenate([qkv_sum, end_sum, fc_sum, end_sum]).reshape(bias_rows, width)
        bias_grad = lax.dynamic_slice_in_dim(bias_grad, owner * rows, rows, 1)
        grads[layer] = (
            gain_l[0][:, None] * grad_qkv + shift_l[0][:, None] * qkv_sum[None, :],
            grad_out_rows[:rows],
            gain_l[1][:, None] * grad_fc + shift_l[1][:, None] * fc_sum[None, :],
            grad_out_rows[rows:],
            bias_grad,
            gain_grad,
            shift_grad,
        )
        grad_own = lax.optimization_barrier(grad_next.astype(BF))
    grad_tokens = net.from_plane(grad_own)
    stacked = [jnp.stack([grads[layer][slot] for layer in range(layers)]) for slot in range(7)]
    return (outputs, grad_tokens, *stacked)


def solution(mesh):
    return jax.shard_map(
        functools.partial(on_device, mesh),
        mesh=mesh,
        in_specs=(
            P("dp", "seq", None),
            P("dp", "seq", None),
            P("dp", None),
            P(None, ("dp", "seq"), None),
            P(None, ("dp", "seq"), None),
            P(None, ("dp", "seq"), None),
            P(None, ("dp", "seq"), None),
            P(None, None, ("dp", "seq")),
            P(None, None, ("dp", "seq")),
            P(None, None, ("dp", "seq")),
        ),
        out_specs=(
            P("dp", "seq", None),
            P("dp", "seq", None),
            P(None, ("dp", "seq"), None),
            P(None, ("dp", "seq"), None),
            P(None, ("dp", "seq"), None),
            P(None, ("dp", "seq"), None),
            P(None, None, ("dp", "seq")),
            P(None, None, ("dp", "seq")),
            P(None, None, ("dp", "seq")),
        ),
        check_vma=False,
    )
```

```python
import functools

import jax
import jax.numpy as jnp
from jax import lax
from jax.experimental import pallas as pl
from jax.experimental.pallas import tpu as pltpu
from jax.sharding import PartitionSpec as P

HEAD_DIM = 64
ROT = 16
norm_eps = 1e-05
mask_fill = -1e30
BF = jnp.bfloat16
F32 = jnp.float32
AXES = ("dp", "seq")
BLOCK = 256


def nt(left, right):
    return lax.dot_general(left, right, (((1,), (1,)), ((), ())), preferred_element_type=F32)


def nn(left, right):
    return lax.dot_general(left, right, (((1,), (0,)), ((), ())), preferred_element_type=F32)


def tn(left, right):
    return lax.dot_general(left, right, (((0,), (0,)), ((), ())), preferred_element_type=F32)


def lane_in_head(shape):
    lane = lax.broadcasted_iota(jnp.int32, shape, len(shape) - 1)
    return lane, lane % HEAD_DIM


def rope(vals, cosine, sine):
    width = vals.shape[-1]
    half = ROT // 2
    _, entry = lane_in_head(vals.shape)
    up = pltpu.roll(vals, width - half, 1)
    down = pltpu.roll(vals, half, 1)
    swapped = jnp.where(entry < half, -up, down)
    return vals * cosine + swapped * sine


def rope_back(grads, cosine, sine):
    width = grads.shape[-1]
    half = ROT // 2
    _, entry = lane_in_head(grads.shape)
    scaled = grads * sine
    up = pltpu.roll(scaled, width - half, 1)
    down = pltpu.roll(scaled, half, 1)
    swapped = jnp.where(entry < half, up, jnp.where(entry < ROT, -down, 0.0))
    return grads * cosine + swapped


def head_only(vals, head):
    lane, _ = lane_in_head(vals.shape)
    keep = (lane >= head * HEAD_DIM) & (lane < (head + 1) * HEAD_DIM)
    return jnp.where(keep, vals, jnp.zeros_like(vals))


def attn_fwd_kernel(
    first_ref, mixed_ref, cos_ref, sin_ref, start_ref,
    query_ref, key_ref, value_ref, ctx_ref, ctx_low_ref, lse_ref,
    value_t_ref,
):
    at = pl.program_id(0)
    total, width = key_ref.shape
    heads = width // HEAD_DIM

    @pl.when(at == 0)
    def _():
        def one(i, carry):
            rows = pl.ds(pl.multiple_of(i * BLOCK, BLOCK), BLOCK)
            keys = mixed_ref[rows, width : 2 * width]
            key_ref[rows, :] = rope(keys, cos_ref[rows, :], sin_ref[rows, :]).astype(BF)
            vals = mixed_ref[rows, 2 * width : 3 * width]
            value_ref[rows, :] = vals.astype(BF)
            value_t_ref[:, rows] = vals.T.astype(BF)
            return carry

        lax.fori_loop(0, total // BLOCK, one, 0)

    rows = pl.ds(pl.multiple_of(at * BLOCK, BLOCK), BLOCK)
    quer = rope(mixed_ref[rows, 0:width], cos_ref[rows, :], sin_ref[rows, :]).astype(BF)
    quer = quer * jnp.asarray(HEAD_DIM**-0.5, BF)
    query_ref[...] = quer
    by_head = [head_only(quer, h) for h in range(heads)]
    key_iota = lax.broadcasted_iota(jnp.int32, (BLOCK, BLOCK), 0)
    query_pos = at * BLOCK + lax.broadcasted_iota(jnp.int32, (1, BLOCK), 1)
    starts = start_ref[...]

    def step(turn, carry):
        block = at - turn
        keys_at = pl.ds(pl.multiple_of(block * BLOCK, BLOCK), BLOCK)
        keys = key_ref[keys_at, :]
        vals_t = value_t_ref[:, keys_at]
        keep = (key_iota >= starts - block * BLOCK) & (key_iota <= query_pos - block * BLOCK)
        out = []
        for h in range(heads):
            top, total_h, acc = carry[h]
            scores = jnp.where(keep, nt(keys, by_head[h]), mask_fill)
            new_top = jnp.maximum(top, jnp.max(scores, axis=0, keepdims=True))
            fade = jnp.exp(top - new_top)
            probs = jnp.exp(scores - new_top)
            total_h = total_h * fade + jnp.sum(probs, axis=0, keepdims=True)
            acc = acc * fade + nn(vals_t, probs.astype(BF))
            out.append((new_top, total_h, acc))
        return tuple(out)

    init = tuple(
        (
            jnp.full((1, BLOCK), mask_fill, F32),
            jnp.zeros((1, BLOCK), F32),
            jnp.zeros((width, BLOCK), F32),
        )
        for h in range(heads)
    )
    done = lax.fori_loop(0, at - first_ref[at] + 1, step, init)
    parts = []
    for h in range(heads):
        top, total_h, acc = done[h]
        lse_ref[h : h + 1, :] = top + jnp.log(total_h)
        parts.append(acc[h * HEAD_DIM : (h + 1) * HEAD_DIM, :] / total_h)
    ctx = jnp.concatenate(parts, axis=0).T
    ctx_ref[...] = ctx
    ctx_low_ref[...] = ctx.astype(BF)


def attn_forward(mixed, cosine, sine, starts, first_block):
    total, width = cosine.shape
    heads = width // HEAD_DIM
    blocks = total // BLOCK
    full = lambda cols: pl.BlockSpec((total, cols), lambda i, f: (0, 0))
    rows = pl.BlockSpec((BLOCK, width), lambda i, f: (i, 0))
    lanes = lambda n: pl.BlockSpec((n, BLOCK), lambda i, f: (0, i))
    wide = jax.ShapeDtypeStruct((total, width), BF)
    return pl.pallas_call(
        attn_fwd_kernel,
        grid_spec=pltpu.PrefetchScalarGridSpec(
            num_scalar_prefetch=1,
            grid=(blocks,),
            in_specs=[full(3 * width), full(width), full(width), lanes(1)],
            out_specs=[rows, full(width), full(width), rows, rows, lanes(heads)],
            scratch_shapes=[pltpu.VMEM((width, total), BF)],
        ),
        out_shape=[
            wide, wide, wide,
            jax.ShapeDtypeStruct((total, width), F32),
            wide,
            jax.ShapeDtypeStruct((heads, total), F32),
        ],
        compiler_params=pltpu.CompilerParams(
            dimension_semantics=("arbitrary",), vmem_limit_bytes=40 << 20
        ),
        cost_estimate=pl.CostEstimate(
            flops=20 * 4 * BLOCK * BLOCK * width * heads,
            bytes_accessed=total * width * 40,
            transcendentals=20 * BLOCK * BLOCK * heads,
        ),
        name="attn_fwd",
    )(first_block, mixed, cosine, sine, starts)


def attn_bwd_kernel(
    first_ref, query_ref, key_ref, value_ref, ctx_ref, lse_ref, grad_ref, cos_ref, sin_ref, start_ref,
    out_ref,
    key_t_ref, grad_key_ref, grad_value_ref,
):
    at = pl.program_id(0)
    total, width = key_ref.shape
    heads = width // HEAD_DIM

    @pl.when(at == 0)
    def _():
        def one(i, carry):
            rows = pl.ds(pl.multiple_of(i * BLOCK, BLOCK), BLOCK)
            key_t_ref[:, rows] = key_ref[rows, :].T
            grad_key_ref[rows, :] = jnp.zeros((BLOCK, width), F32)
            grad_value_ref[rows, :] = jnp.zeros((BLOCK, width), F32)
            return carry

        lax.fori_loop(0, total // BLOCK, one, 0)

    quer = query_ref[...]
    grad = grad_ref[...]
    by_head = [head_only(quer, h) for h in range(heads)]
    grad_head = [head_only(grad, h) for h in range(heads)]
    inner_t = (grad.astype(F32) * ctx_ref[...]).T
    inner = [
        jnp.sum(inner_t[h * HEAD_DIM : (h + 1) * HEAD_DIM, :], axis=0, keepdims=True)
        for h in range(heads)
    ]
    logs = [lse_ref[h : h + 1, :] for h in range(heads)]
    key_iota = lax.broadcasted_iota(jnp.int32, (BLOCK, BLOCK), 0)
    query_pos = at * BLOCK + lax.broadcasted_iota(jnp.int32, (1, BLOCK), 1)
    starts = start_ref[...]

    def step(turn, carry):
        block = at - turn
        keys_at = pl.ds(pl.multiple_of(block * BLOCK, BLOCK), BLOCK)
        keys = key_ref[keys_at, :]
        vals = value_ref[keys_at, :]
        keys_t = key_t_ref[:, keys_at]
        keep = (key_iota >= starts - block * BLOCK) & (key_iota <= query_pos - block * BLOCK)
        out = []
        grad_key = jnp.zeros((BLOCK, width), F32)
        grad_value = jnp.zeros((BLOCK, width), F32)
        for h in range(heads):
            scores = nt(keys, by_head[h])
            probs = jnp.where(keep, jnp.exp(jnp.where(keep, scores, mask_fill) - logs[h]), 0.0)
            grad_probs = nt(vals, grad_head[h])
            grad_scores = (probs * (grad_probs - inner[h])).astype(BF)
            grad_value = grad_value + nn(probs.astype(BF), grad_head[h])
            grad_key = grad_key + nn(grad_scores, by_head[h])
            out.append(carry[h] + nn(keys_t, grad_scores))
        grad_key_ref[keys_at, :] += grad_key
        grad_value_ref[keys_at, :] += grad_value
        return tuple(out)

    init = tuple(jnp.zeros((width, BLOCK), F32) for h in range(heads))
    done = lax.fori_loop(0, at - first_ref[at] + 1, step, init)
    parts = [done[h][h * HEAD_DIM : (h + 1) * HEAD_DIM, :] for h in range(heads)]
    grad_query = jnp.concatenate(parts, axis=0).T * (HEAD_DIM**-0.5)
    rows = pl.ds(pl.multiple_of(at * BLOCK, BLOCK), BLOCK)
    out_ref[rows, 0:width] = rope_back(grad_query, cos_ref[rows, :], sin_ref[rows, :]).astype(BF)

    @pl.when(at == pl.num_programs(0) - 1)
    def _():
        def one(i, carry):
            rows = pl.ds(pl.multiple_of(i * BLOCK, BLOCK), BLOCK)
            grad_key = rope_back(grad_key_ref[rows, :], cos_ref[rows, :], sin_ref[rows, :])
            out_ref[rows, width : 2 * width] = grad_key.astype(BF)
            out_ref[rows, 2 * width : 3 * width] = grad_value_ref[rows, :].astype(BF)
            return carry

        lax.fori_loop(0, total // BLOCK, one, 0)


def attn_backward(query, key, value, ctx, lse, grad_ctx, cosine, sine, starts, first_block):
    total, width = cosine.shape
    heads = width // HEAD_DIM
    blocks = total // BLOCK
    full = lambda cols: pl.BlockSpec((total, cols), lambda i, f: (0, 0))
    rows = pl.BlockSpec((BLOCK, width), lambda i, f: (i, 0))
    lanes = lambda n: pl.BlockSpec((n, BLOCK), lambda i, f: (0, i))
    return pl.pallas_call(
        attn_bwd_kernel,
        grid_spec=pltpu.PrefetchScalarGridSpec(
            num_scalar_prefetch=1,
            grid=(blocks,),
            in_specs=[
                rows, full(width), full(width), rows, lanes(heads), rows,
                full(width), full(width), lanes(1),
            ],
            out_specs=full(3 * width),
            scratch_shapes=[
                pltpu.VMEM((width, total), BF),
                pltpu.VMEM((total, width), F32),
                pltpu.VMEM((total, width), F32),
            ],
        ),
        out_shape=jax.ShapeDtypeStruct((total, 3 * width), BF),
        compiler_params=pltpu.CompilerParams(
            dimension_semantics=("arbitrary",), vmem_limit_bytes=40 << 20
        ),
        cost_estimate=pl.CostEstimate(
            flops=20 * 10 * BLOCK * BLOCK * width * heads,
            bytes_accessed=total * width * 40,
            transcendentals=20 * BLOCK * BLOCK * heads,
        ),
        name="attn_bwd",
    )(first_block, query, key, value, ctx, lse, grad_ctx, cosine, sine, starts)


MESH = pl.DeviceIdType.MESH


class Place:
    def __init__(self, spots, planes, send_sem, recv_sem, copy_sem):
        self.spots, self.planes = spots, planes
        self.p, self.s = lax.axis_index("dp"), lax.axis_index("seq")
        self.z, self.c = self.s // 2, self.s % 2
        self.near = self.s + 1 - 2 * self.c
        self.send_sem, self.recv_sem, self.copy_sem = send_sem, recv_sem, copy_sem
        self.used, self.kept = 0, 0

    def take(self, count=1):
        self.used += count
        return self.used - count

    def far(self, src, dst, at, dest, recv_at=None):
        return pltpu.make_async_remote_copy(
            src_ref=src, dst_ref=dst,
            send_sem=self.send_sem.at[at],
            recv_sem=self.recv_sem.at[at if recv_at is None else recv_at],
            device_id=dest, device_id_type=MESH,
        )

    def keep(self, src, dst):
        self.kept += 1
        return pltpu.make_async_copy(src, dst, self.copy_sem.at[self.kept - 1])

    def at_z(self, z):
        return (self.p, z * 2 + self.c)

    def plane_partners(self):
        p = self.p
        if self.spots == 4:
            return [p + 1 - 2 * (p % 2), p + 2 - 4 * (p // 2)]
        return [(p + k) % self.spots for k in range(1, self.spots)]


class Relay:
    def __init__(self, place, own, slot):
        self.place, self.own, self.slot = place, own, slot
        self.up = place.take(place.planes)
        self.down = place.take(place.planes)

    def copy(self, src, z, at, step):
        place = self.place
        return place.far(src, self.slot(z), at, place.at_z(place.z + step))

    def start(self):
        z, last = self.place.z, self.place.planes - 1

        @pl.when(z < last)
        def _():
            self.copy(self.own, z, self.up, 1).start()

        @pl.when(z > 0)
        def _():
            self.copy(self.own, z, self.down, -1).start()

    def stage(self, k):
        z, last = self.place.z, self.place.planes - 1

        @pl.when(z >= k)
        def _():
            self.copy(self.slot(z - k), z - k, self.up + k - 1, 1).wait_recv()

            @pl.when(z < last)
            def _():
                self.copy(self.slot(z - k), z - k, self.up + k, 1).start()

        @pl.when(z + k <= last)
        def _():
            self.copy(self.slot(z + k), z + k, self.down + k - 1, -1).wait_recv()

            @pl.when(z > 0)
            def _():
                self.copy(self.slot(z + k), z + k, self.down + k, -1).start()

    def finish(self):
        z, last = self.place.z, self.place.planes - 1
        for k in range(last + 1):
            if k < last:

                @pl.when((z < last) & (z >= k))
                def _():
                    self.copy(self.slot(z), z, self.up + k, 1).wait_send()

                @pl.when((z > 0) & (z + k <= last))
                def _():
                    self.copy(self.slot(z), z, self.down + k, -1).wait_send()


class PlaneGather:
    def __init__(self, place, all_ref, parts):
        self.place, self.all_ref = place, all_ref
        self.parts = parts
        self.sent, self.passed = [], []
        relayed = place.spots == 4
        self.others = place.plane_partners()
        self.ways = len(self.others)
        count = len(parts)
        self.base = [place.take(self.ways) for _ in parts]
        self.relay = [place.take() if relayed else None for _ in parts]
        self.close = [place.take(place.spots) for _ in parts]

    def view(self, part, spot):
        return self.all_ref.at[part, self.place.c, spot]

    def near(self, i, src, spot, m):
        place = self.place
        copy = place.far(src, self.view(self.parts[i], spot), self.close[i] + m, (place.p, place.near))
        copy.start()
        self.passed.append(copy)

    def start(self, i, src=None):
        place = self.place
        src = self.view(self.parts[i], place.p) if src is None else src
        for w, q in enumerate(self.others):
            copy = place.far(
                src, self.view(self.parts[i], place.p), self.base[i] + w, (q, place.s)
            )
            copy.start()
            self.sent.append(copy)
        self.near(i, src, place.p, 0)

    def arrive(self, i):
        place = self.place
        relayed = place.spots == 4
        for w, q in enumerate(self.others):
            spot = q if relayed else (place.p + place.spots - 1 - w) % place.spots
            got = self.view(self.parts[i], spot)
            place.far(got, got, self.base[i] + w, (q, place.s)).wait_recv()
            if relayed and w == (0 if i < len(self.parts) // 2 else 1):
                copy = place.far(got, got, self.relay[i], (self.others[1 - w], place.s))
                copy.start()
                self.sent.append(copy)
            self.near(i, got, spot, 1 + w)

    def arrive_diagonal(self, i):
        place = self.place
        if place.spots == 4:
            got = self.view(self.parts[i], 3 - place.p)
            place.far(got, got, self.relay[i], (self.others[0], place.s)).wait_recv()
            self.near(i, got, 3 - place.p, 3)

    def finish(self):
        for copy in self.passed:
            copy.wait_recv()
        for copy in self.sent + self.passed:
            copy.wait_send()


def greet(place, plane, line):
    barrier = pltpu.get_barrier_semaphore()
    for dest in plane:
        pl.semaphore_signal(barrier, inc=1, device_id=dest, device_id_type=MESH)
    count = len(plane)
    if line:
        z, last = place.z, place.planes - 1

        @pl.when(z < last)
        def _():
            pl.semaphore_signal(barrier, inc=1, device_id=place.at_z(z + 1), device_id_type=MESH)

        @pl.when(z > 0)
        def _():
            pl.semaphore_signal(barrier, inc=1, device_id=place.at_z(z - 1), device_id_type=MESH)

        count = count + jnp.where(z < last, 1, 0) + jnp.where(z > 0, 1, 0)
    pl.semaphore_wait(barrier, count)


def heads_home(place, col, heads_ref, half):
    c = place.c
    at = place.take()
    keep = place.keep(col.at[pl.ds(c * half, half)], heads_ref.at[pl.ds(0, half), c])
    keep.start()
    over = place.far(
        col.at[pl.ds((1 - c) * half, half)], heads_ref.at[pl.ds(0, half), c], at, (place.p, place.near)
    )
    over.start()
    return keep, over


def sems(remote, local):
    return [
        pltpu.SemaphoreType.DMA((remote,)),
        pltpu.SemaphoreType.DMA((remote,)),
        pltpu.SemaphoreType.DMA((local,)),
    ]


def gather_sems(spots, pieces):
    ways = 2 if spots == 4 else spots - 1
    return pieces * (ways + spots + (1 if spots == 4 else 0))


def start_kernel(
    spots, planes,
    tok_ref, cot_ref, first_in_ref, next_in_ref, out_ref, proj_ref,
    tok_all, cot_all, first_all, next_slot, heads_all, proj_all,
    tok_buf, cot_buf, col, send_sem, recv_sem, copy_sem,
):
    place = Place(spots, planes, send_sem, recv_sem, copy_sem)
    p, s, z, c = place.p, place.s, place.z, place.c
    half = planes // 2
    crowd = [
        ((p + k) % spots, s if e == 0 else place.near)
        for k in range(spots) for e in range(2) if k or e
    ]
    rest = [place.at_z((z + k) % planes) for k in range(1, planes)]
    greet(place, crowd + rest, False)

    streams = [(tok_ref, tok_buf, tok_all), (cot_ref, cot_buf, cot_all)]
    spread = []
    for own, buf, _ in streams:
        row = []
        for k in range(1, spots):
            q = (p + k) % spots
            copy = place.far(own.at[q], buf.at[p], place.take(), (q, s))
            copy.start()
            row.append(copy)
        spread.append(row)
    proj_line = Relay(place, proj_ref, lambda at: proj_all.at[at])
    head_line = Relay(place, out_ref, lambda at: col.at[at])
    proj_line.start()
    head_line.start()
    kept = [place.keep(proj_ref, proj_all.at[z]), place.keep(out_ref, col.at[z])]
    mailed = []
    for own, slot in (
        (first_in_ref, lambda q, core: first_all.at[q, z, core]),
        (next_in_ref, lambda q, core: next_slot.at[q, core]),
    ):
        for k in range(spots):
            for e in range(2):
                q = (p + k) % spots
                core = c if e == 0 else 1 - c
                if k or e:
                    copy = place.far(
                        own.at[q, core], slot(p, c), place.take(),
                        (q, s if e == 0 else place.near),
                    )
                    copy.start()
                    mailed.append(copy)
        kept.append(place.keep(own.at[p, c], slot(p, c)))
    for copy in kept:
        copy.start()
    moved = []
    for (own, buf, whole), row in zip(streams, spread):
        send_at, recv_at = place.take(spots), place.take(planes)
        place.kept += 1
        local = place.kept - 1
        for k in range(spots):
            j = (p + spots - k) % spots
            if k:
                row[k - 1].wait_recv()
            data = own.at[p] if k == 0 else buf.at[j]

            @pl.when(j != z)
            def _():
                place.far(data, whole.at[z, c, p], send_at + k, place.at_z(j), recv_at + z).start()

            @pl.when(j == z)
            def _():
                pltpu.make_async_copy(data, whole.at[z, c, p], copy_sem.at[local]).start()

        moved.append((send_at, recv_at, local))
    for copy in kept:
        copy.wait()
    count = len(mailed) // 2
    for copy in mailed[:count]:
        copy.wait_recv()
    all_spots = pl.ds(0, spots)
    in_line = Relay(place, first_all.at[all_spots, z], lambda at: first_all.at[all_spots, at])
    in_line.start()
    head_line.stage(1)
    proj_line.stage(1)
    gathers = []
    for (own, buf, whole), (send_at, recv_at, local) in zip(streams, moved):
        gather = PlaneGather(place, whole, [(z + i) % planes for i in range(planes)])
        for i in range(planes):
            at = (z + i) % planes
            piece = whole.at[at, c, p]
            if i == 0:
                pltpu.make_async_copy(tok_ref.at[0], piece, copy_sem.at[local]).wait()
            else:
                place.far(piece, piece, send_at, place.at_z(at), recv_at + at).wait_recv()
            gather.start(i)
        gathers.append(gather)
        if len(gathers) == 1:
            in_line.stage(1)
            head_line.stage(2)
            proj_line.stage(2)
    for i in range(planes):
        gathers[0].arrive(i)
    for k in range(2, planes):
        in_line.stage(k)
        if k + 1 < planes:
            head_line.stage(k + 1)
            proj_line.stage(k + 1)
        if k == 2:
            for i in range(planes):
                gathers[0].arrive_diagonal(i)
            for i in range(planes):
                gathers[1].arrive(i)
            for i in range(planes):
                gathers[1].arrive_diagonal(i)
    keep, over = heads_home(place, col, heads_all, half)
    for copy in mailed[count:]:
        copy.wait_recv()
    for gather in gathers:
        gather.finish()
    keep.wait()
    over.wait()
    for line in (in_line, head_line, proj_line):
        line.finish()
    for row in spread:
        for copy in row:
            copy.wait_send()
    for copy in mailed:
        copy.wait_send()
    for (own, buf, whole), (send_at, recv_at, local) in zip(streams, moved):
        for k in range(spots):
            j = (p + spots - k) % spots

            @pl.when(j != z)
            def _():
                place.far(own.at[p], whole.at[z, c, p], send_at + k, place.at_z(j)).wait_send()


def bring_all(tok, cot, first_in, next_in, out_w, proj_w, spots, planes):
    _, rows, width = tok.shape
    vmem = pl.BlockSpec(memory_space=pltpu.VMEM)
    hbm = pl.BlockSpec(memory_space=pl.ANY)
    whole = jax.ShapeDtypeStruct((planes, 2, spots, rows, width), BF)
    owned, cols = first_in.shape[2:]
    return pl.pallas_call(
        functools.partial(start_kernel, spots, planes),
        out_shape=[
            whole, whole,
            jax.ShapeDtypeStruct((spots, planes, 2, owned, cols), BF),
            jax.ShapeDtypeStruct(next_in.shape, BF),
            jax.ShapeDtypeStruct((planes // 2, 2) + out_w.shape, BF),
            jax.ShapeDtypeStruct((planes,) + proj_w.shape, BF),
        ],
        in_specs=[vmem] * 6,
        out_specs=[hbm] * 6,
        scratch_shapes=[
            pltpu.VMEM((spots, rows, width), BF),
            pltpu.VMEM((spots, rows, width), BF),
            pltpu.VMEM((planes,) + out_w.shape, BF),
        ] + sems(
            2 * (spots - 1) + 2 * (2 * spots - 1) + 6 * planes + 2 * (spots + planes)
            + 2 * gather_sems(spots, planes) + 1,
            7,
        ),
        compiler_params=pltpu.CompilerParams(
            collective_id=3, has_side_effects=True, vmem_limit_bytes=32 << 20
        ),
        name="bring_all",
    )(tok, cot, first_in, next_in, out_w, proj_w)


def gather_kernel(spots, planes, lined, own_ref, *refs):
    if lined:
        out_ref, proj_ref, all_ref, heads_all, proj_all, col, send_sem, recv_sem, copy_sem = refs
    else:
        all_ref, send_sem, recv_sem, copy_sem = refs
    place = Place(spots, planes, send_sem, recv_sem, copy_sem)
    groups = own_ref.shape[0]
    half = groups // 2
    parts = [pl.ds(0, half), pl.ds(half, half)]
    whole = pl.ds(0, groups)
    plane = [(q, place.s) for q in place.plane_partners()] + [(place.p, place.near)]
    greet(place, plane, lined)
    gather = PlaneGather(place, all_ref, parts)
    lines = []
    for i in range(2):
        gather.start(i, own_ref.at[parts[i]])
    kept = [place.keep(own_ref, all_ref.at[whole, place.c, place.p])]
    if lined:
        lines = [
            Relay(place, out_ref, lambda at: col.at[at]),
            Relay(place, proj_ref, lambda at: proj_all.at[at]),
        ]
        for line in lines:
            line.start()
        kept += [
            place.keep(out_ref, col.at[place.z]), place.keep(proj_ref, proj_all.at[place.z]),
        ]
    for copy in kept:
        copy.start()
    for i in range(2):
        gather.arrive(i)
    for line in lines:
        line.stage(1)
    for i in range(2):
        gather.arrive_diagonal(i)
    for k in range(2, planes):
        for line in lines:
            line.stage(k)
    for copy in kept:
        copy.wait()
    if lined:
        keep, over = heads_home(place, col, heads_all, planes // 2)
        keep.wait()
        over.wait()
    gather.finish()
    for line in lines:
        line.finish()


def gather_tokens(own, spots, planes, out_w=None, proj_w=None):
    groups, rows, width = own.shape
    lined = out_w is not None
    vmem = pl.BlockSpec(memory_space=pltpu.VMEM)
    hbm = pl.BlockSpec(memory_space=pl.ANY)
    shapes = [jax.ShapeDtypeStruct((groups, 2, spots, rows, width), own.dtype)]
    scratch, args = [], [own]
    if lined:
        shapes += [
            jax.ShapeDtypeStruct((planes // 2, 2) + out_w.shape, BF),
            jax.ShapeDtypeStruct((planes,) + proj_w.shape, BF),
        ]
        scratch = [pltpu.VMEM((planes,) + out_w.shape, BF)]
        args += [out_w, proj_w]
    out = pl.pallas_call(
        functools.partial(gather_kernel, spots, planes, lined),
        out_shape=shapes,
        in_specs=[vmem] * len(args),
        out_specs=[hbm] * len(shapes),
        scratch_shapes=scratch + sems(
            gather_sems(spots, 2) + (4 * planes + 1 if lined else 0), 4 if lined else 1
        ),
        compiler_params=pltpu.CompilerParams(
            collective_id=4 if lined else 1, has_side_effects=True, vmem_limit_bytes=32 << 20
        ),
        name="gather_weights" if lined else "gather_tokens",
    )(*args)
    return [out[0].reshape(-1, width)] + list(out[1:])


def scatter_kernel(spots, planes, lined, part_ref, *refs):
    if lined:
        slot_ref, out_ref, in_all, near_buf, mine, relay, inbox, send_sem, recv_sem, copy_sem = refs
    else:
        out_ref, near_buf, mine, relay, inbox, send_sem, recv_sem, copy_sem = refs
    place = Place(spots, planes, send_sem, recv_sem, copy_sem)
    p, s, c = place.p, place.s, place.c
    others = place.plane_partners()
    _, groups, rows, width = mine.shape
    half = groups // 2
    halves = [pl.ds(0, half), pl.ds(half, half)]
    whole = pl.ds(0, groups)
    step = min(rows, 16)
    greet(place, [(q, s) for q in others] + [(p, place.near)], lined)
    if spots == 4:
        x, y = others
        spot_of = [p, x, y, 3 - p]
        order = [3, 1, 2, 0]
    else:
        spot_of = [p] + others
        order = list(range(1, spots)) + [0]
    handed, kept = {}, {}
    for m in order:
        handed[m] = place.far(
            part_ref.at[whole, 1 - c, spot_of[m]], near_buf.at[m], place.take(), (p, place.near)
        )
        kept[m] = place.keep(part_ref.at[whole, c, spot_of[m]], mine.at[m])
        handed[m].start()
        kept[m].start()
    lines = []
    if lined:
        all_spots = pl.ds(0, spots)
        lines = [Relay(place, slot_ref, lambda at: in_all.at[all_spots, at])]
        lines[0].start()
        in_kept = place.keep(slot_ref, in_all.at[all_spots, place.z])
        in_kept.start()

    def add(first, count, into, left, right):
        per = rows // step

        def one(i, carry):
            g = first + i // per
            at = pl.ds(pl.multiple_of((i % per) * step, step), step)
            into[g, at, :] = (left(g, at) + right(g, at)).astype(into.dtype)
            return carry

        lax.fori_loop(0, count * per, one, 0)

    def far(m, part, slot, dest):
        copy = place.far(mine.at[m, part], slot, place.take(), (dest, s))
        copy.start()
        return copy

    sent = {}
    for m in order:
        handed[m].wait_recv()
        kept[m].wait()
        into = out_ref if m == 0 else mine.at[m]
        add(
            0, groups, into,
            lambda g, at: mine[m, g, at, :].astype(F32),
            lambda g, at: near_buf[m, g, at, :].astype(F32),
        )
        if spots == 4:
            if m == 3:
                sent[0] = far(3, halves[0], relay.at[0], x)
                sent[1] = far(3, halves[1], relay.at[1], y)
            elif m == 1:
                sent[2] = far(1, halves[0], inbox.at[0, halves[0]], x)
            elif m == 2:
                sent[3] = far(2, halves[1], inbox.at[1, halves[1]], y)
        elif m > 0:
            sent[m - 1] = far(m, whole, inbox.at[m - 1], others[m - 1])
    if spots == 4:
        sent[0].wait_recv()
        add(
            0, half, mine.at[2],
            lambda g, at: mine[2, g, at, :].astype(F32),
            lambda g, at: relay[0, g, at, :].astype(F32),
        )
        sent[4] = far(2, halves[0], inbox.at[1, halves[0]], y)
        sent[1].wait_recv()
        add(
            half, half, mine.at[1],
            lambda g, at: mine[1, g, at, :].astype(F32),
            lambda g, at: relay[1, g - half, at, :].astype(F32),
        )
        sent[5] = far(1, halves[1], inbox.at[0, halves[1]], x)
        for line in lines:
            line.stage(1)
        for at in (2, 3, 4, 5):
            sent[at].wait_recv()
    else:
        for line in lines:
            line.stage(1)
        for at in sent:
            sent[at].wait_recv()

    def received(g, at):
        total = inbox[0, g, at, :].astype(F32)
        for slot in range(1, inbox.shape[0]):
            total = total + inbox[slot, g, at, :].astype(F32)
        return total

    for line in lines:
        line.stage(2)
    add(0, groups, out_ref, lambda g, at: out_ref[g, at, :], received)
    for k in range(3, planes):
        for line in lines:
            line.stage(k)
    for m in order:
        handed[m].wait_send()
    for at in sent:
        sent[at].wait_send()
    for line in lines:
        line.finish()
        in_kept.wait()


def scatter_tokens(part, spots, planes, slot=None):
    total, width = part.shape
    groups = planes
    rows = total // (groups * 2 * spots)
    slots = 2 if spots == 4 else spots - 1
    lined = slot is not None
    vmem = pl.BlockSpec(memory_space=pltpu.VMEM)
    hbm = pl.BlockSpec(memory_space=pl.ANY)
    shapes, args = [jax.ShapeDtypeStruct((groups, rows, width), F32)], []
    if lined:
        owned, cols = slot.shape[2:]
        shapes.append(jax.ShapeDtypeStruct((spots, planes, 2, owned, cols), BF))
        args.append(slot)
    return pl.pallas_call(
        functools.partial(scatter_kernel, spots, planes, lined),
        out_shape=shapes,
        in_specs=[hbm] + [vmem] * len(args),
        out_specs=[vmem] + [hbm] * len(args),
        scratch_shapes=[
            pltpu.VMEM((spots, groups, rows, width), BF),
            pltpu.VMEM((spots, groups, rows, width), BF),
            pltpu.VMEM((2, groups // 2, rows, width), BF),
            pltpu.VMEM((slots, groups, rows, width), BF),
        ] + sems(
            spots + (6 if spots == 4 else spots - 1) + (2 * planes if lined else 0), spots + 1
        ),
        compiler_params=pltpu.CompilerParams(
            collective_id=5 if lined else 2, has_side_effects=True, vmem_limit_bytes=32 << 20
        ),
        name="scatter_weights" if lined else "scatter_tokens",
    )(part.reshape(groups, 2, spots, rows, width), *args)


class Net:
    def __init__(self, mesh):
        self.planes = mesh.shape["seq"] // 2
        self.spots = mesh.shape["dp"]
        self.p = lax.axis_index("dp")
        self.z = lax.axis_index("seq") // 2
        self.c = lax.axis_index("seq") % 2

    def permute(self, x, to):
        pairs = []
        for p in range(self.spots):
            for z in range(self.planes):
                for c in range(2):
                    tp, tz, tc = to(p, z, c)
                    source = (p * self.planes + z) * 2 + c
                    pairs.append((source, (tp * self.planes + tz) * 2 + tc))
        return lax.ppermute(x, AXES, pairs)

    def sibling(self, x):
        return self.permute(x, lambda p, z, c: (p, z, 1 - c))

    def turned(self, x):
        return self.permute(x, lambda p, z, c: (z, p, c))

    def gather(self, x, axis):
        count = self.spots if axis == "p" else self.planes
        me = self.p if axis == "p" else self.z
        buf = jnp.zeros((count,) + x.shape, x.dtype)
        buf = lax.dynamic_update_index_in_dim(buf, x, me, 0)
        for k in range(1, count):
            if axis == "p":
                got = self.permute(x, lambda p, z, c: (p ^ k, z, c))
            else:
                got = self.permute(x, lambda p, z, c: (p, z ^ k, c))
            buf = lax.dynamic_update_index_in_dim(buf, got, me ^ k, 0)
        return buf

    def swap(self, x, axis):
        count = self.spots if axis == "p" else self.planes
        me = self.p if axis == "p" else self.z
        pieces = [lax.dynamic_index_in_dim(x, me, 0, keepdims=False)]
        for k in range(1, count):
            piece = lax.dynamic_index_in_dim(x, me ^ k, 0, keepdims=False)
            if axis == "p":
                pieces.append(self.permute(piece, lambda p, z, c: (p ^ k, z, c)))
            else:
                pieces.append(self.permute(piece, lambda p, z, c: (p, z ^ k, c)))
        return pieces

    def ordered(self, pieces, axis):
        me = self.p if axis == "p" else self.z
        buf = jnp.zeros((len(pieces),) + pieces[0].shape, pieces[0].dtype)
        for k, piece in enumerate(pieces):
            buf = lax.dynamic_update_index_in_dim(buf, piece, me ^ k, 0)
        return buf

    def both_cores(self, x):
        other = self.sibling(x)
        return jnp.where(self.c == 0, jnp.stack([x, other]), jnp.stack([other, x]))

    def core_part(self, x, core, axis):
        return lax.dynamic_index_in_dim(x, core, axis, keepdims=False)

    def core_swap(self, x, axis):
        own = self.core_part(x, self.c, axis)
        got = self.sibling(self.core_part(x, 1 - self.c, axis))
        first = jnp.where(self.c == 0, own, got)
        second = jnp.where(self.c == 0, got, own)
        return jnp.stack([first, second], axis=axis)

    def from_plane(self, x):
        x = self.ordered(self.swap(x, "z"), "z")
        x = self.ordered(self.swap(x, "p"), "p")
        return x.reshape(1, -1, x.shape[-1])


def normalize(resid):
    mean = jnp.mean(resid, axis=-1, keepdims=True)
    center = resid - mean
    spread = jnp.mean(center * center, axis=-1, keepdims=True)
    inv = lax.rsqrt(spread + norm_eps)
    return center * inv, inv


def gelu_parts(pre):
    cdf = 0.5 * (1.0 + lax.erf(pre * (2.0**-0.5)))
    return cdf


def on_device(
    mesh, tokens, cotangent, segments, qkv_weight, out_weight, fc_weight, proj_weight,
    biases, ln_gain, ln_shift,
):
    net = Net(mesh)
    spots, planes = net.spots, net.planes
    team = spots * 2
    layers, rows, _ = qkv_weight.shape
    width = out_weight.shape[2]
    local = tokens.shape[1]
    head_cols = width // team
    hidden_all = fc_weight.shape[2]
    fc_piece = proj_weight.shape[1]
    owner = (net.p * planes + net.z) * 2 + net.c
    assert spots == planes

    seg_row = net.turned(segments)
    full_len = seg_row.shape[1]
    index = lax.broadcasted_iota(jnp.int32, (1, full_len), 1)
    starts = jnp.zeros((1, full_len), jnp.int32)
    for doc in range(3):
        count = jnp.sum((seg_row == doc).astype(jnp.int32))
        starts = starts + jnp.where(seg_row > doc, count, 0)
    position = (index - starts).astype(F32)
    first_block = starts[0, ::BLOCK] // BLOCK
    half = ROT // 2
    entry = jnp.arange(head_cols, dtype=jnp.int32) % HEAD_DIM
    inverse = 10000.0 ** (-2.0 * (entry % half).astype(F32) / ROT)
    inverse = jnp.where(entry < ROT, inverse, 0.0)
    angle = position.reshape(full_len, 1) * inverse[None, :]
    cosine, sine = jnp.cos(angle), jnp.sin(angle)

    gain_own = ln_gain.astype(F32)
    shift_own = ln_shift.astype(F32)
    t_at = net.p * 2 + net.c
    qkv_cols, fc_cols = 3 * head_cols, planes * fc_piece
    in_cols = qkv_cols + fc_cols
    bias_rows = biases.shape[1]

    def in_weight(layer):
        qkv = qkv_weight[layer].astype(F32) * gain_own[layer, 0][:, None]
        qkv = qkv.astype(BF).reshape(rows, 3, spots, 2, head_cols)
        qkv = jnp.transpose(qkv, (2, 3, 0, 1, 4)).reshape(spots, 2, rows, qkv_cols)
        fc = fc_weight[layer].astype(F32) * gain_own[layer, 1][:, None]
        fc = fc.astype(BF).reshape(rows, spots, planes, 2, fc_piece)
        fc = jnp.transpose(fc, (1, 3, 0, 2, 4)).reshape(spots, 2, rows, fc_cols)
        return [qkv, fc]

    small = jnp.concatenate([biases, ln_gain, ln_shift], axis=1).reshape(-1, rows).T
    small_cols = small.shape[1]
    small = jnp.pad(small, ((0, 0), (0, 128 - small_cols)))
    small = jnp.broadcast_to(small, (spots, 2, rows, 128))
    first_in = jnp.concatenate(in_weight(0) + [small], axis=-1)
    next_in = jnp.concatenate(in_weight(1), axis=-1)

    per_spot = (spots, local // spots, width)
    tok_all, cot_all, first_all, next_slot, heads_w0, proj_w0 = bring_all(
        tokens.reshape(per_spot), cotangent.reshape(per_spot), first_in, next_in,
        out_weight[0], proj_weight[0], spots, planes,
    )
    first_all = first_all.reshape(width, -1)
    small = first_all[:, in_cols : in_cols + small_cols].T.astype(F32).reshape(layers, -1, width)
    bias_all, gain_all, shift_all = (
        small[:, :bias_rows], small[:, bias_rows : bias_rows + 2], small[:, bias_rows + 2 :],
    )
    weights_in = [(first_all[:, :qkv_cols], first_all[:, qkv_cols:in_cols]), None]
    weights_out = [(heads_w0.reshape(head_cols, width), proj_w0.reshape(fc_cols, width)), None]

    def bias_in(layer):
        qkv_b = bias_all[layer, :3].reshape(3, team, head_cols)
        qkv_b = lax.dynamic_index_in_dim(qkv_b, t_at, 1, keepdims=False).reshape(1, -1)
        fc_b = bias_all[layer, 4 : bias_rows - 1].reshape(spots, planes, 2, fc_piece)
        fc_b = lax.dynamic_index_in_dim(fc_b, net.p, 0, keepdims=False)
        fc_b = lax.dynamic_index_in_dim(fc_b, net.c, 1, keepdims=False).reshape(1, -1)
        ratio = shift_all[layer] / gain_all[layer]
        high = ratio.astype(BF)
        low = (ratio - high.astype(F32)).astype(BF)
        qkv_w, fc_w = weights_in[layer]
        qkv_b = qkv_b + nn(high[:1], qkv_w) + nn(low[:1], qkv_w)
        fc_b = fc_b + nn(high[1:], fc_w) + nn(low[1:], fc_w)
        return qkv_b, fc_b

    def own_part(whole):
        part = lax.dynamic_index_in_dim(whole, net.c, 1, keepdims=False)
        return lax.dynamic_index_in_dim(part, net.p, 1, keepdims=False)

    cot_own = own_part(cot_all)
    cot_all = cot_all.reshape(full_len, width)

    resid = own_part(tok_all).astype(F32)
    saved = []
    for layer in range(layers):
        normed, inv = normalize(resid)
        if layer == 0:
            normed_all = normalize(tok_all.reshape(full_len, width).astype(F32))[0].astype(BF)
        else:
            normed_all, heads_w, proj_w = gather_tokens(
                normed.astype(BF), spots, planes, out_weight[layer], proj_weight[layer]
            )
            weights_out[layer] = (
                heads_w.reshape(head_cols, width), proj_w.reshape(fc_cols, width)
            )
        qkv_w, fc_w = weights_in[layer]
        head_w, proj_w = weights_out[layer]
        qkv_b, fc_b = bias_in(layer)
        mixed = nn(normed_all, qkv_w) + qkv_b
        hidden_pre = nn(normed_all, fc_w) + fc_b
        query, key, value, ctx, ctx_low, lse = attn_forward(
            mixed, cosine, sine, starts, first_block
        )
        hidden = (hidden_pre * gelu_parts(hidden_pre)).astype(BF)
        part = (nn(hidden, proj_w) + nn(ctx_low, head_w)).astype(BF)
        saved.append((normed, inv, normed_all, query, key, value, ctx, ctx_low, lse, hidden_pre, hidden))
        end_bias = bias_all[layer, 3] + bias_all[layer, bias_rows - 1]
        if layer == 0:
            summed, next_all = scatter_tokens(part, spots, planes, next_slot)
            next_all = next_all.reshape(width, -1)
            weights_in[1] = (next_all[:, :qkv_cols], next_all[:, qkv_cols:])
        else:
            (summed,) = scatter_tokens(part, spots, planes)
        resid = resid + summed + end_bias
    outputs = net.from_plane(resid.astype(BF))

    grads = [None] * layers
    grad_own = cot_own
    for layer in reversed(range(layers)):
        normed, inv, normed_all, query, key, value, ctx, ctx_low, lse, hidden_pre, hidden = saved[layer]
        qkv_w, fc_w = weights_in[layer]
        head_w, proj_w = weights_out[layer]
        grad_all = cot_all if layer == layers - 1 else gather_tokens(grad_own, spots, planes)[0]
        grad_ctx = nt(grad_all, head_w).astype(BF)
        grad_mixed = attn_backward(
            query, key, value, ctx, lse, grad_ctx, cosine, sine, starts, first_block
        )
        cdf = gelu_parts(hidden_pre)
        density = jnp.exp(-0.5 * hidden_pre * hidden_pre) * ((2.0 * jnp.pi) ** -0.5)
        grad_pre = (nt(grad_all, proj_w) * (cdf + hidden_pre * density)).astype(BF)
        part = (nt(grad_mixed, qkv_w) + nt(grad_pre, fc_w)).astype(BF)
        (norm_grad,) = scatter_tokens(part, spots, planes)
        mean_grad = jnp.mean(norm_grad, axis=-1, keepdims=True)
        mean_dot = jnp.mean(norm_grad * normed, axis=-1, keepdims=True)
        grad_next = grad_own.astype(F32) + inv * (norm_grad - mean_grad - normed * mean_dot)

        grad_heads = tn(ctx_low, grad_all).astype(BF)
        grad_proj = tn(hidden, grad_all).astype(BF)
        grad_heads = grad_heads.reshape(planes // 2, 2, rows, width)
        own = net.core_part(grad_heads, net.c, 1)
        got = net.sibling(net.core_part(grad_heads, 1 - net.c, 1))
        first = jnp.where(net.c == 0, own, got)
        second = jnp.where(net.c == 0, got, own)
        grad_col = jnp.concatenate(
            [
                jnp.concatenate([first, second], axis=0),
                grad_proj.reshape(planes, fc_piece, width),
            ],
            axis=1,
        )
        pieces = net.swap(grad_col, "z")
        grad_out_rows = sum(piece.astype(F32) for piece in pieces)
        grad_in_w = jnp.concatenate(
            [tn(normed_all, grad_mixed).astype(BF), tn(normed_all, grad_pre).astype(BF)], axis=1
        )
        grad_in_w = jnp.moveaxis(grad_in_w.reshape(spots, planes, 2, rows, -1), 1, 0)
        pieces = net.swap(grad_in_w, "z")
        grad_in_w = sum(piece.astype(F32) for piece in pieces).astype(BF)
        grad_in_w = net.core_swap(grad_in_w, 1)
        grad_in_w = net.ordered(net.swap(grad_in_w, "p"), "p").astype(F32)

        sums = jnp.concatenate(
            [
                jnp.sum(grad_mixed.astype(F32), axis=0),
                jnp.sum(grad_pre.astype(F32), axis=0),
                jnp.sum(grad_own.astype(F32), axis=(0, 1)),
            ]
        )
        sums = sum(net.swap(jnp.broadcast_to(sums, (planes,) + sums.shape), "z"))
        sums = net.gather(net.both_cores(sums), "p")
        end_sum = jnp.sum(sums[:, :, in_cols:], axis=(0, 1))
        qkv_sum = sums[:, :, : 3 * head_cols].reshape(team, 3, head_cols)
        qkv_sum = jnp.transpose(qkv_sum, (1, 0, 2)).reshape(-1)
        fc_sum = sums[:, :, 3 * head_cols : in_cols].reshape(spots, 2, planes, fc_piece)
        fc_sum = jnp.transpose(fc_sum, (0, 2, 1, 3)).reshape(-1)

        grad_qkv = grad_in_w[..., : 3 * head_cols].reshape(team, rows, 3, head_cols)
        grad_qkv = jnp.transpose(grad_qkv, (1, 2, 0, 3)).reshape(rows, -1)
        grad_fc = grad_in_w[..., 3 * head_cols :].reshape(spots, 2, rows, planes, fc_piece)
        grad_fc = jnp.transpose(grad_fc, (2, 0, 3, 1, 4)).reshape(rows, -1)
        qkv_own = qkv_weight[layer].astype(F32)
        fc_own = fc_weight[layer].astype(F32)
        gain_grad = jnp.stack(
            [jnp.sum(qkv_own * grad_qkv, axis=1), jnp.sum(fc_own * grad_fc, axis=1)]
        )
        shift_grad = jnp.stack(
            [jnp.sum(qkv_own * qkv_sum, axis=1), jnp.sum(fc_own * fc_sum, axis=1)]
        )
        gain_l, shift_l = gain_own[layer], shift_own[layer]
        bias_grad = jnp.concatenate([qkv_sum, end_sum, fc_sum, end_sum]).reshape(bias_rows, width)
        bias_grad = lax.dynamic_slice_in_dim(bias_grad, owner * rows, rows, 1)
        grads[layer] = (
            gain_l[0][:, None] * grad_qkv + shift_l[0][:, None] * qkv_sum[None, :],
            grad_out_rows[:rows],
            gain_l[1][:, None] * grad_fc + shift_l[1][:, None] * fc_sum[None, :],
            grad_out_rows[rows:],
            bias_grad,
            gain_grad,
            shift_grad,
        )
        grad_own = lax.optimization_barrier(grad_next.astype(BF))
    grad_tokens = net.from_plane(grad_own)
    stacked = [jnp.stack([grads[layer][slot] for layer in range(layers)]) for slot in range(7)]
    return (outputs, grad_tokens, *stacked)


def solution(mesh):
    return jax.shard_map(
        functools.partial(on_device, mesh),
        mesh=mesh,
        in_specs=(
            P("dp", "seq", None),
            P("dp", "seq", None),
            P("dp", None),
            P(None, ("dp", "seq"), None),
            P(None, ("dp", "seq"), None),
            P(None, ("dp", "seq"), None),
            P(None, ("dp", "seq"), None),
            P(None, None, ("dp", "seq")),
            P(None, None, ("dp", "seq")),
            P(None, None, ("dp", "seq")),
        ),
        out_specs=(
            P("dp", "seq", None),
            P("dp", "seq", None),
            P(None, ("dp", "seq"), None),
            P(None, ("dp", "seq"), None),
            P(None, ("dp", "seq"), None),
            P(None, ("dp", "seq"), None),
            P(None, None, ("dp", "seq")),
            P(None, None, ("dp", "seq")),
            P(None, None, ("dp", "seq")),
        ),
        check_vma=False,
    )
```

```python
import functools

import jax
import jax.numpy as jnp
from jax import lax
from jax.experimental import pallas as pl
from jax.experimental.pallas import tpu as pltpu
from jax.sharding import PartitionSpec as P

HEAD_DIM = 64
ROT = 16
norm_eps = 1e-05
mask_fill = -1e30
BF = jnp.bfloat16
F32 = jnp.float32
AXES = ("dp", "seq")
BLOCK = 256


def nt(left, right):
    return lax.dot_general(left, right, (((1,), (1,)), ((), ())), preferred_element_type=F32)


def nn(left, right):
    return lax.dot_general(left, right, (((1,), (0,)), ((), ())), preferred_element_type=F32)


def tn(left, right):
    return lax.dot_general(left, right, (((0,), (0,)), ((), ())), preferred_element_type=F32)


def lane_in_head(shape):
    lane = lax.broadcasted_iota(jnp.int32, shape, len(shape) - 1)
    return lane, lane % HEAD_DIM


def rope(vals, cosine, sine):
    width = vals.shape[-1]
    half = ROT // 2
    _, entry = lane_in_head(vals.shape)
    up = pltpu.roll(vals, width - half, 1)
    down = pltpu.roll(vals, half, 1)
    swapped = jnp.where(entry < half, -up, down)
    return vals * cosine + swapped * sine


def rope_back(grads, cosine, sine):
    width = grads.shape[-1]
    half = ROT // 2
    _, entry = lane_in_head(grads.shape)
    scaled = grads * sine
    up = pltpu.roll(scaled, width - half, 1)
    down = pltpu.roll(scaled, half, 1)
    swapped = jnp.where(entry < half, up, jnp.where(entry < ROT, -down, 0.0))
    return grads * cosine + swapped


def head_only(vals, head):
    lane, _ = lane_in_head(vals.shape)
    keep = (lane >= head * HEAD_DIM) & (lane < (head + 1) * HEAD_DIM)
    return jnp.where(keep, vals, jnp.zeros_like(vals))


def attn_fwd_kernel(
    first_ref, mixed_ref, cos_ref, sin_ref, start_ref,
    query_ref, key_ref, value_ref, ctx_ref, ctx_low_ref, lse_ref,
    value_t_ref,
):
    at = pl.program_id(0)
    total, width = key_ref.shape
    heads = width // HEAD_DIM

    @pl.when(at == 0)
    def _():
        def one(i, carry):
            rows = pl.ds(pl.multiple_of(i * BLOCK, BLOCK), BLOCK)
            keys = mixed_ref[rows, width : 2 * width]
            key_ref[rows, :] = rope(keys, cos_ref[rows, :], sin_ref[rows, :]).astype(BF)
            vals = mixed_ref[rows, 2 * width : 3 * width]
            value_ref[rows, :] = vals.astype(BF)
            value_t_ref[:, rows] = vals.T.astype(BF)
            return carry

        lax.fori_loop(0, total // BLOCK, one, 0)

    rows = pl.ds(pl.multiple_of(at * BLOCK, BLOCK), BLOCK)
    quer = rope(mixed_ref[rows, 0:width], cos_ref[rows, :], sin_ref[rows, :]).astype(BF)
    quer = quer * jnp.asarray(HEAD_DIM**-0.5, BF)
    query_ref[...] = quer
    by_head = [head_only(quer, h) for h in range(heads)]
    key_iota = lax.broadcasted_iota(jnp.int32, (BLOCK, BLOCK), 0)
    query_pos = at * BLOCK + lax.broadcasted_iota(jnp.int32, (1, BLOCK), 1)
    starts = start_ref[...]

    def step(turn, carry):
        block = at - turn
        keys_at = pl.ds(pl.multiple_of(block * BLOCK, BLOCK), BLOCK)
        keys = key_ref[keys_at, :]
        vals_t = value_t_ref[:, keys_at]
        keep = (key_iota >= starts - block * BLOCK) & (key_iota <= query_pos - block * BLOCK)
        out = []
        for h in range(heads):
            top, total_h, acc = carry[h]
            scores = jnp.where(keep, nt(keys, by_head[h]), mask_fill)
            new_top = jnp.maximum(top, jnp.max(scores, axis=0, keepdims=True))
            fade = jnp.exp(top - new_top)
            probs = jnp.exp(scores - new_top)
            total_h = total_h * fade + jnp.sum(probs, axis=0, keepdims=True)
            acc = acc * fade + nn(vals_t, probs.astype(BF))
            out.append((new_top, total_h, acc))
        return tuple(out)

    init = tuple(
        (
            jnp.full((1, BLOCK), mask_fill, F32),
            jnp.zeros((1, BLOCK), F32),
            jnp.zeros((width, BLOCK), F32),
        )
        for h in range(heads)
    )
    done = lax.fori_loop(0, at - first_ref[at] + 1, step, init)
    parts = []
    for h in range(heads):
        top, total_h, acc = done[h]
        lse_ref[h : h + 1, :] = top + jnp.log(total_h)
        parts.append(acc[h * HEAD_DIM : (h + 1) * HEAD_DIM, :] / total_h)
    ctx = jnp.concatenate(parts, axis=0).T
    ctx_ref[...] = ctx
    ctx_low_ref[...] = ctx.astype(BF)


def attn_forward(mixed, cosine, sine, starts, first_block):
    total, width = cosine.shape
    heads = width // HEAD_DIM
    blocks = total // BLOCK
    full = lambda cols: pl.BlockSpec((total, cols), lambda i, f: (0, 0))
    rows = pl.BlockSpec((BLOCK, width), lambda i, f: (i, 0))
    lanes = lambda n: pl.BlockSpec((n, BLOCK), lambda i, f: (0, i))
    wide = jax.ShapeDtypeStruct((total, width), BF)
    return pl.pallas_call(
        attn_fwd_kernel,
        grid_spec=pltpu.PrefetchScalarGridSpec(
            num_scalar_prefetch=1,
            grid=(blocks,),
            in_specs=[full(3 * width), full(width), full(width), lanes(1)],
            out_specs=[rows, full(width), full(width), rows, rows, lanes(heads)],
            scratch_shapes=[pltpu.VMEM((width, total), BF)],
        ),
        out_shape=[
            wide, wide, wide,
            jax.ShapeDtypeStruct((total, width), F32),
            wide,
            jax.ShapeDtypeStruct((heads, total), F32),
        ],
        compiler_params=pltpu.CompilerParams(
            dimension_semantics=("arbitrary",), vmem_limit_bytes=40 << 20
        ),
        cost_estimate=pl.CostEstimate(
            flops=20 * 4 * BLOCK * BLOCK * width * heads,
            bytes_accessed=total * width * 40,
            transcendentals=20 * BLOCK * BLOCK * heads,
        ),
        name="attn_fwd",
    )(first_block, mixed, cosine, sine, starts)


def attn_bwd_kernel(
    first_ref, query_ref, key_ref, value_ref, ctx_ref, lse_ref, grad_ref, cos_ref, sin_ref, start_ref,
    out_ref,
    key_t_ref, grad_key_ref, grad_value_ref,
):
    at = pl.program_id(0)
    total, width = key_ref.shape
    heads = width // HEAD_DIM

    @pl.when(at == 0)
    def _():
        def one(i, carry):
            rows = pl.ds(pl.multiple_of(i * BLOCK, BLOCK), BLOCK)
            key_t_ref[:, rows] = key_ref[rows, :].T
            grad_key_ref[rows, :] = jnp.zeros((BLOCK, width), F32)
            grad_value_ref[rows, :] = jnp.zeros((BLOCK, width), F32)
            return carry

        lax.fori_loop(0, total // BLOCK, one, 0)

    quer = query_ref[...]
    grad = grad_ref[...]
    by_head = [head_only(quer, h) for h in range(heads)]
    grad_head = [head_only(grad, h) for h in range(heads)]
    inner_t = (grad.astype(F32) * ctx_ref[...]).T
    inner = [
        jnp.sum(inner_t[h * HEAD_DIM : (h + 1) * HEAD_DIM, :], axis=0, keepdims=True)
        for h in range(heads)
    ]
    logs = [lse_ref[h : h + 1, :] for h in range(heads)]
    key_iota = lax.broadcasted_iota(jnp.int32, (BLOCK, BLOCK), 0)
    query_pos = at * BLOCK + lax.broadcasted_iota(jnp.int32, (1, BLOCK), 1)
    starts = start_ref[...]

    def step(turn, carry):
        block = at - turn
        keys_at = pl.ds(pl.multiple_of(block * BLOCK, BLOCK), BLOCK)
        keys = key_ref[keys_at, :]
        vals = value_ref[keys_at, :]
        keys_t = key_t_ref[:, keys_at]
        keep = (key_iota >= starts - block * BLOCK) & (key_iota <= query_pos - block * BLOCK)
        out = []
        grad_key = jnp.zeros((BLOCK, width), F32)
        grad_value = jnp.zeros((BLOCK, width), F32)
        for h in range(heads):
            scores = nt(keys, by_head[h])
            probs = jnp.where(keep, jnp.exp(jnp.where(keep, scores, mask_fill) - logs[h]), 0.0)
            grad_probs = nt(vals, grad_head[h])
            grad_scores = (probs * (grad_probs - inner[h])).astype(BF)
            grad_value = grad_value + nn(probs.astype(BF), grad_head[h])
            grad_key = grad_key + nn(grad_scores, by_head[h])
            out.append(carry[h] + nn(keys_t, grad_scores))
        grad_key_ref[keys_at, :] += grad_key
        grad_value_ref[keys_at, :] += grad_value
        return tuple(out)

    init = tuple(jnp.zeros((width, BLOCK), F32) for h in range(heads))
    done = lax.fori_loop(0, at - first_ref[at] + 1, step, init)
    parts = [done[h][h * HEAD_DIM : (h + 1) * HEAD_DIM, :] for h in range(heads)]
    grad_query = jnp.concatenate(parts, axis=0).T * (HEAD_DIM**-0.5)
    rows = pl.ds(pl.multiple_of(at * BLOCK, BLOCK), BLOCK)
    out_ref[rows, 0:width] = rope_back(grad_query, cos_ref[rows, :], sin_ref[rows, :]).astype(BF)

    @pl.when(at == pl.num_programs(0) - 1)
    def _():
        def one(i, carry):
            rows = pl.ds(pl.multiple_of(i * BLOCK, BLOCK), BLOCK)
            grad_key = rope_back(grad_key_ref[rows, :], cos_ref[rows, :], sin_ref[rows, :])
            out_ref[rows, width : 2 * width] = grad_key.astype(BF)
            out_ref[rows, 2 * width : 3 * width] = grad_value_ref[rows, :].astype(BF)
            return carry

        lax.fori_loop(0, total // BLOCK, one, 0)


def attn_backward(query, key, value, ctx, lse, grad_ctx, cosine, sine, starts, first_block):
    total, width = cosine.shape
    heads = width // HEAD_DIM
    blocks = total // BLOCK
    full = lambda cols: pl.BlockSpec((total, cols), lambda i, f: (0, 0))
    rows = pl.BlockSpec((BLOCK, width), lambda i, f: (i, 0))
    lanes = lambda n: pl.BlockSpec((n, BLOCK), lambda i, f: (0, i))
    return pl.pallas_call(
        attn_bwd_kernel,
        grid_spec=pltpu.PrefetchScalarGridSpec(
            num_scalar_prefetch=1,
            grid=(blocks,),
            in_specs=[
                rows, full(width), full(width), rows, lanes(heads), rows,
                full(width), full(width), lanes(1),
            ],
            out_specs=full(3 * width),
            scratch_shapes=[
                pltpu.VMEM((width, total), BF),
                pltpu.VMEM((total, width), F32),
                pltpu.VMEM((total, width), F32),
            ],
        ),
        out_shape=jax.ShapeDtypeStruct((total, 3 * width), BF),
        compiler_params=pltpu.CompilerParams(
            dimension_semantics=("arbitrary",), vmem_limit_bytes=40 << 20
        ),
        cost_estimate=pl.CostEstimate(
            flops=20 * 10 * BLOCK * BLOCK * width * heads,
            bytes_accessed=total * width * 40,
            transcendentals=20 * BLOCK * BLOCK * heads,
        ),
        name="attn_bwd",
    )(first_block, query, key, value, ctx, lse, grad_ctx, cosine, sine, starts)


def pair_kernel(turned, cols, left_ref, right_ref, *refs):
    *weights, out_ref = refs
    if turned:
        whole = weights[0]
        split = left_ref.shape[1]
        total = nt(left_ref[...], whole[:, 0:split]) + nt(right_ref[...], whole[:, split:cols])
    else:
        total = nn(left_ref[...], weights[0][...]) + nn(right_ref[...], weights[1][...])
    out_ref[...] = total.astype(BF)


def pair_product(left, right, weights, turned):
    total = left.shape[0]
    cols = left.shape[1] + right.shape[1]
    width = weights[0].shape[0] if turned else weights[0].shape[1]
    rows = lambda x: pl.BlockSpec((BLOCK, x.shape[1]), lambda i: (i, 0))
    full = lambda x: pl.BlockSpec(x.shape, lambda i: (0, 0))
    return pl.pallas_call(
        functools.partial(pair_kernel, turned, cols),
        grid=(total // BLOCK,),
        out_shape=jax.ShapeDtypeStruct((total, width), BF),
        in_specs=[rows(left), rows(right)] + [full(w) for w in weights],
        out_specs=pl.BlockSpec((BLOCK, width), lambda i: (i, 0)),
        compiler_params=pltpu.CompilerParams(
            dimension_semantics=("arbitrary",), vmem_limit_bytes=32 << 20
        ),
        cost_estimate=pl.CostEstimate(
            flops=2 * total * cols * width, bytes_accessed=2 * total * (cols + width),
            transcendentals=0,
        ),
        name="pair_product",
    )(left, right, *weights)


def owner_kernel(
    spots, planes, head_cols, fc_piece,
    first_ref, next_ref, sums_ref, qkv_ref, fc_ref, scale_ref, qkv_out, fc_out, stat_out,
):
    layers, rows, wide = qkv_ref.shape
    width = wide // 3
    stats = []
    for layer, grad_ref in enumerate((first_ref, next_ref)):
        groups = [[], []]
        for p in range(spots):
            for core in range(2):
                t = p * 2 + core
                for j in range(3):
                    groups[0].append((p, core, j * head_cols, head_cols, j * width + t * head_cols))
                for z in range(planes):
                    groups[1].append(
                        (p, core, 3 * head_cols + z * fc_piece, fc_piece,
                         ((p * planes + z) * 2 + core) * fc_piece)
                    )
        for norm, (weight_ref, out_ref) in enumerate(((qkv_ref, qkv_out), (fc_ref, fc_out))):
            at = 4 * layer + norm
            gain, shift = scale_ref[:, at : at + 1], scale_ref[:, at + 2 : at + 3]
            gain_sum = shift_sum = 0.0
            for p, core, source, count, target in groups[norm]:
                grad = grad_ref[p, core, :, source : source + count].astype(F32)
                sums = sums_ref[p * 2 + core, layer : layer + 1, source : source + count]
                weight = weight_ref[layer, :, target : target + count].astype(F32)
                out_ref[layer, :, target : target + count] = gain * grad + shift * sums
                gain_sum = gain_sum + weight * grad
                shift_sum = shift_sum + weight * sums
            stats.append(jnp.sum(gain_sum, axis=1, keepdims=True))
            stats.append(jnp.sum(shift_sum, axis=1, keepdims=True))
    for i, stat in enumerate(stats):
        stat_out[:, i : i + 1] = stat


def owner_grads(first, following, sums, qkv_weight, fc_weight, scale, head_cols, fc_piece, planes):
    layers, rows, _ = qkv_weight.shape
    vmem = pl.BlockSpec(memory_space=pltpu.VMEM)
    return pl.pallas_call(
        functools.partial(owner_kernel, first.shape[0], planes, head_cols, fc_piece),
        out_shape=[
            jax.ShapeDtypeStruct(qkv_weight.shape, F32),
            jax.ShapeDtypeStruct(fc_weight.shape, F32),
            jax.ShapeDtypeStruct((rows, 4 * layers), F32),
        ],
        in_specs=[vmem] * 6,
        out_specs=[vmem] * 3,
        compiler_params=pltpu.CompilerParams(vmem_limit_bytes=32 << 20),
        name="owner_grads",
    )(first, following, sums, qkv_weight, fc_weight, scale)


MESH = pl.DeviceIdType.MESH


class Place:
    def __init__(self, spots, planes, send_sem, recv_sem, copy_sem):
        self.spots, self.planes = spots, planes
        self.p, self.s = lax.axis_index("dp"), lax.axis_index("seq")
        self.z, self.c = self.s // 2, self.s % 2
        self.near = self.s + 1 - 2 * self.c
        self.send_sem, self.recv_sem, self.copy_sem = send_sem, recv_sem, copy_sem
        self.used, self.kept = 0, 0

    def take(self, count=1):
        self.used += count
        return self.used - count

    def far(self, src, dst, at, dest, recv_at=None):
        return pltpu.make_async_remote_copy(
            src_ref=src, dst_ref=dst,
            send_sem=self.send_sem.at[at],
            recv_sem=self.recv_sem.at[at if recv_at is None else recv_at],
            device_id=dest, device_id_type=MESH,
        )

    def keep(self, src, dst):
        self.kept += 1
        return pltpu.make_async_copy(src, dst, self.copy_sem.at[self.kept - 1])

    def at_z(self, z):
        return (self.p, z * 2 + self.c)

    def plane_partners(self):
        p = self.p
        if self.spots == 4:
            return [p + 1 - 2 * (p % 2), p + 2 - 4 * (p // 2)]
        return [(p + k) % self.spots for k in range(1, self.spots)]


class Relay:
    def __init__(self, place, own, slot):
        self.place, self.own, self.slot = place, own, slot
        self.up = place.take(place.planes)
        self.down = place.take(place.planes)

    def copy(self, src, z, at, step):
        place = self.place
        return place.far(src, self.slot(z), at, place.at_z(place.z + step))

    def start(self):
        z, last = self.place.z, self.place.planes - 1

        @pl.when(z < last)
        def _():
            self.copy(self.own, z, self.up, 1).start()

        @pl.when(z > 0)
        def _():
            self.copy(self.own, z, self.down, -1).start()

    def stage(self, k):
        z, last = self.place.z, self.place.planes - 1

        @pl.when(z >= k)
        def _():
            self.copy(self.slot(z - k), z - k, self.up + k - 1, 1).wait_recv()

            @pl.when(z < last)
            def _():
                self.copy(self.slot(z - k), z - k, self.up + k, 1).start()

        @pl.when(z + k <= last)
        def _():
            self.copy(self.slot(z + k), z + k, self.down + k - 1, -1).wait_recv()

            @pl.when(z > 0)
            def _():
                self.copy(self.slot(z + k), z + k, self.down + k, -1).start()

    def finish(self):
        z, last = self.place.z, self.place.planes - 1
        for k in range(last + 1):
            if k < last:

                @pl.when((z < last) & (z >= k))
                def _():
                    self.copy(self.slot(z), z, self.up + k, 1).wait_send()

                @pl.when((z > 0) & (z + k <= last))
                def _():
                    self.copy(self.slot(z), z, self.down + k, -1).wait_send()


class PlaneGather:
    def __init__(self, place, all_ref, parts):
        self.place, self.all_ref = place, all_ref
        self.parts = parts
        self.sent, self.passed = [], []
        relayed = place.spots == 4
        self.others = place.plane_partners()
        self.ways = len(self.others)
        count = len(parts)
        self.base = [place.take(self.ways) for _ in parts]
        self.relay = [place.take() if relayed else None for _ in parts]
        self.close = [place.take(place.spots) for _ in parts]

    def view(self, part, spot):
        return self.all_ref.at[part, self.place.c, spot]

    def near(self, i, src, spot, m):
        place = self.place
        copy = place.far(src, self.view(self.parts[i], spot), self.close[i] + m, (place.p, place.near))
        copy.start()
        self.passed.append(copy)

    def start(self, i, src=None):
        place = self.place
        src = self.view(self.parts[i], place.p) if src is None else src
        for w, q in enumerate(self.others):
            copy = place.far(
                src, self.view(self.parts[i], place.p), self.base[i] + w, (q, place.s)
            )
            copy.start()
            self.sent.append(copy)
        self.near(i, src, place.p, 0)

    def arrive(self, i):
        place = self.place
        relayed = place.spots == 4
        for w, q in enumerate(self.others):
            spot = q if relayed else (place.p + place.spots - 1 - w) % place.spots
            got = self.view(self.parts[i], spot)
            place.far(got, got, self.base[i] + w, (q, place.s)).wait_recv()
            if relayed and w == (0 if i < len(self.parts) // 2 else 1):
                copy = place.far(got, got, self.relay[i], (self.others[1 - w], place.s))
                copy.start()
                self.sent.append(copy)
            self.near(i, got, spot, 1 + w)

    def arrive_diagonal(self, i):
        place = self.place
        if place.spots == 4:
            got = self.view(self.parts[i], 3 - place.p)
            place.far(got, got, self.relay[i], (self.others[0], place.s)).wait_recv()
            self.near(i, got, 3 - place.p, 3)

    def finish(self):
        for copy in self.passed:
            copy.wait_recv()
        for copy in self.sent + self.passed:
            copy.wait_send()


def greet(place, plane, column):
    barrier = pltpu.get_barrier_semaphore()
    dests = list(plane)
    if column:
        dests += [place.at_z((place.z + k) % place.planes) for k in range(1, place.planes)]
    for dest in dests:
        pl.semaphore_signal(barrier, inc=1, device_id=dest, device_id_type=MESH)
    pl.semaphore_wait(barrier, len(dests))


def heads_home(place, col, heads_ref, half):
    c = place.c
    at = place.take()
    keep = place.keep(col.at[pl.ds(c * half, half)], heads_ref.at[pl.ds(0, half), c])
    keep.start()
    over = place.far(
        col.at[pl.ds((1 - c) * half, half)], heads_ref.at[pl.ds(0, half), c], at, (place.p, place.near)
    )
    over.start()
    return keep, over


class LineSum:
    def __init__(self, place, below, above, own_value, piece, count):
        self.place, self.below, self.above = place, below, above
        self.own_value, self.piece, self.count = own_value, piece, count
        self.up = place.take(place.planes)
        self.down = place.take(place.planes)

    def copy(self, into, d, step):
        place = self.place
        at = (self.up if step > 0 else self.down) + d
        return place.far(into.at[d], into.at[d], at, place.at_z(place.z + step))

    def fill(self, into, d, add):
        def one(i, carry):
            at = self.piece(into, d, i)
            total = self.own_value(d, i)
            if add:
                total = (at[...].astype(F32) + total.astype(F32)).astype(BF)
            at[...] = total
            return carry

        lax.fori_loop(0, self.count, one, 0)

    def send(self, d, step):
        into = self.below if step > 0 else self.above
        self.fill(into, d, False)
        self.copy(into, d, step).start()

    def start(self):
        z, last = self.place.z, self.place.planes - 1
        pl.when(z == 0)(lambda: self.send(last, 1))
        pl.when(z == last)(lambda: self.send(0, -1))

    def stage(self, i):
        z, last = self.place.z, self.place.planes - 1
        high, low = last - i, i

        @pl.when((z > 0) & (z < high))
        def _():
            self.copy(self.below, high, 1).wait_recv()
            self.fill(self.below, high, True)
            self.copy(self.below, high, 1).start()

        @pl.when((z < last) & (z > low))
        def _():
            self.copy(self.above, low, -1).wait_recv()
            self.fill(self.above, low, True)
            self.copy(self.above, low, -1).start()

        if high > 1:

            @pl.when(z == 0)
            def _():
                self.copy(self.below, high, 1).wait_send()
                self.send(high - 1, 1)

            @pl.when(z == last)
            def _():
                self.copy(self.above, low, -1).wait_send()
                self.send(low + 1, -1)

    def finish(self, out_piece):
        z, last = self.place.z, self.place.planes - 1

        @pl.when(z > 0)
        def _():
            self.copy(self.below, z, 1).wait_recv()

        @pl.when(z < last)
        def _():
            self.copy(self.above, z, -1).wait_recv()

        def store(sources):
            def one(i, carry):
                total = self.own_value(z, i).astype(F32)
                for source in sources:
                    total = total + self.piece(source, z, i)[...].astype(F32)
                at = out_piece(i)
                at[...] = total.astype(at.dtype)
                return carry

            lax.fori_loop(0, self.count, one, 0)

        pl.when(z == 0)(lambda: store([self.above]))
        pl.when(z == last)(lambda: store([self.below]))
        pl.when((z > 0) & (z < last))(lambda: store([self.below, self.above]))
        for d in range(last + 1):
            if d > 0:

                @pl.when((z < d) & ((z > 0) | (d == 1)))
                def _():
                    self.copy(self.below, d, 1).wait_send()

            if d < last:

                @pl.when((z > d) & ((z < last) | (d == last - 1)))
                def _():
                    self.copy(self.above, d, -1).wait_send()


class InWeightGather:
    def __init__(self, place, ins, outs, scratch):
        (slot_ref,), (in_all,) = ins, outs
        every = pl.ds(0, place.spots)
        self.planes = place.planes
        self.line = Relay(place, slot_ref, lambda at: in_all.at[every, at])
        self.kept = place.keep(slot_ref, in_all.at[every, place.z])

    def start(self):
        self.line.start()
        self.kept.start()

    def stage(self, i):
        self.line.stage(i + 1)

    def finish(self):
        self.kept.wait()
        self.line.finish()


class OutWeightGather:
    def __init__(self, place, ins, outs, scratch):
        (out_ref, proj_ref), (self.heads, proj_all), (self.col,) = ins, outs, scratch
        col = self.col
        self.place = place
        self.lines = [
            Relay(place, out_ref, lambda at: col.at[at]),
            Relay(place, proj_ref, lambda at: proj_all.at[at]),
        ]
        self.kept = [
            place.keep(out_ref, col.at[place.z]), place.keep(proj_ref, proj_all.at[place.z]),
        ]

    def start(self):
        for line in self.lines:
            line.start()
        for copy in self.kept:
            copy.start()

    def stage(self, i):
        for line in self.lines:
            line.stage(i + 1)

    def finish(self):
        for copy in self.kept:
            copy.wait()
        keep, over = heads_home(self.place, self.col, self.heads, self.place.planes // 2)
        keep.wait()
        over.wait()
        for line in self.lines:
            line.finish()


class InGradSum:
    def __init__(self, place, ins, outs, scratch):
        (qkv_ref, fc_ref, self.sums), (self.out, self.sums_out) = ins, outs
        below, above, self.sums_buf = scratch
        self.place = place
        self.line = LineSum(
            place, below, above,
            lambda d, i: jnp.concatenate(
                [qkv_ref[i // 2, d, i % 2], fc_ref[i // 2, d, i % 2]], axis=-1
            ),
            lambda ref, d, i: ref.at[d, i // 2, i % 2],
            2 * place.spots,
        )
        self.at = place.take(place.planes)
        self.sent = []

    def start(self):
        place = self.place
        self.line.start()
        for k in range(1, place.planes):
            copy = place.far(
                self.sums, self.sums_buf.at[k], self.at + k,
                place.at_z((place.z + k) % place.planes),
            )
            copy.start()
            self.sent.append(copy)

    def stage(self, i):
        self.line.stage(i)

    def finish(self):
        total = self.sums[...]
        for k, copy in enumerate(self.sent):
            copy.wait_recv()
            total = total + self.sums_buf[k + 1]
        self.sums_out[...] = total
        self.line.finish(lambda i: self.out.at[i // 2, i % 2])
        for copy in self.sent:
            copy.wait_send()


class OutGradSum:
    def __init__(self, place, ins, outs, scratch):
        heads_ref, proj_ref = ins
        self.heads_out, self.proj_out = outs
        col, col_below, col_above, below, above = scratch
        c, half = place.c, place.planes // 2
        few = pl.ds(0, half)
        self.place = place
        mine = pl.ds(c * half, half)
        self.keep = place.keep(heads_ref.at[few, c], col.at[mine])
        self.over = place.far(heads_ref.at[few, 1 - c], col.at[mine], place.take(), (place.p, place.near))
        rows = col.shape[1]

        def line(own, below, above, count):
            step = own.shape[1] // count
            some = lambda i: pl.ds(pl.multiple_of(i * step, step), step)
            return LineSum(
                place, below, above,
                lambda d, i: own[d, some(i)], lambda ref, d, i: ref.at[d, some(i)], count,
            )

        self.count = proj_ref.shape[1] // rows
        self.rows = rows
        self.head_line = line(col, col_below, col_above, 1)
        self.proj_line = line(proj_ref, below, above, self.count)

    def start(self):
        self.keep.start()
        self.over.start()
        self.proj_line.start()
        self.keep.wait()
        self.over.wait_recv()
        self.head_line.start()

    def stage(self, i):
        self.proj_line.stage(i)
        self.head_line.stage(i)

    def finish(self):
        rows = self.rows
        self.head_line.finish(lambda i: self.heads_out.at[pl.ds(0, rows)])
        self.proj_line.finish(
            lambda i: self.proj_out.at[pl.ds(pl.multiple_of(i * rows, rows), rows)]
        )
        self.over.wait_send()


VM = pltpu.VMEM


def in_weight_gather(slot, spots, planes):
    owned, cols = slot.shape[2:]
    shape = jax.ShapeDtypeStruct((spots, planes, 2, owned, cols), BF)
    return (InWeightGather, [slot], [(shape, pl.ANY)], [], 2 * planes, 1)


def out_weight_gather(out_w, proj_w, spots, planes):
    heads = jax.ShapeDtypeStruct((planes // 2, 2) + out_w.shape, BF)
    proj = jax.ShapeDtypeStruct((planes,) + proj_w.shape, BF)
    return (
        OutWeightGather, [out_w, proj_w], [(heads, pl.ANY), (proj, pl.ANY)],
        [VM((planes,) + out_w.shape, BF)], 4 * planes + 1, 3,
    )


def in_grad_sum(grad_qkv, grad_fc, sums, spots, planes):
    owned = grad_qkv.shape[3]
    slot = (spots, 2, owned, grad_qkv.shape[4] + grad_fc.shape[4])
    return (
        InGradSum, [grad_qkv, grad_fc, sums],
        [(jax.ShapeDtypeStruct(slot, BF), VM), (jax.ShapeDtypeStruct(sums.shape, F32), VM)],
        [VM((planes,) + slot, BF), VM((planes,) + slot, BF), VM((planes,) + sums.shape, F32)],
        3 * planes, 0,
    )


def out_grad_sum(heads, proj, spots, planes):
    _, _, owned, width = heads.shape
    wide = proj.shape[1]
    return (
        OutGradSum, [heads, proj],
        [
            (jax.ShapeDtypeStruct((owned, width), F32), VM),
            (jax.ShapeDtypeStruct((wide, width), F32), VM),
        ],
        [VM((planes, owned, width), BF)] * 3 + [VM((planes, wide, width), BF)] * 2,
        4 * planes + 1, 1,
    )


def unpack(jobs, place, refs, lead_in, lead_out, lead_scratch):
    refs = list(refs)
    ins = [refs.pop(0) for _ in range(lead_in)]
    job_ins = [[refs.pop(0) for _ in job[1]] for job in jobs]
    outs = [refs.pop(0) for _ in range(lead_out)]
    job_outs = [[refs.pop(0) for _ in job[2]] for job in jobs]
    scratch = [refs.pop(0) for _ in range(lead_scratch)]
    job_scratch = [[refs.pop(0) for _ in job[3]] for job in jobs]
    place.send_sem, place.recv_sem, place.copy_sem = refs
    made = [
        job[0](place, *three) for job, three in zip(jobs, zip(job_ins, job_outs, job_scratch))
    ]
    return ins, outs, scratch, made


def job_call(kernel, name, number, spots, planes, jobs, args, in_spaces, outs, scratch, remote, local):
    spec = lambda space: pl.BlockSpec(memory_space=space)
    count = 0
    for job in jobs:
        args = args + job[1]
        in_spaces = in_spaces + [VM] * len(job[1])
        outs = outs + job[2]
        scratch = scratch + job[3]
        remote, local = remote + job[4], local + job[5]
    plain = [(job[0], [0] * len(job[1]), [0] * len(job[2]), [0] * len(job[3])) for job in jobs]
    return pl.pallas_call(
        functools.partial(kernel, spots, planes, plain),
        out_shape=[shape for shape, _ in outs],
        in_specs=[spec(space) for space in in_spaces],
        out_specs=[spec(space) for _, space in outs],
        scratch_shapes=scratch + sems(remote, local),
        compiler_params=pltpu.CompilerParams(
            collective_id=number, has_side_effects=True, vmem_limit_bytes=48 << 20
        ),
        name=name,
    )(*args)


def sems(remote, local):
    return [
        pltpu.SemaphoreType.DMA((remote,)),
        pltpu.SemaphoreType.DMA((remote,)),
        pltpu.SemaphoreType.DMA((local,)),
    ]


def gather_sems(spots, pieces):
    ways = 2 if spots == 4 else spots - 1
    return pieces * (ways + spots + (1 if spots == 4 else 0))


def start_kernel(
    spots, planes,
    tok_ref, cot_ref, first_in_ref, next_in_ref, out_ref, proj_ref,
    tok_all, cot_all, first_all, next_slot, heads_all, proj_all,
    tok_buf, cot_buf, col, send_sem, recv_sem, copy_sem,
):
    place = Place(spots, planes, send_sem, recv_sem, copy_sem)
    p, s, z, c = place.p, place.s, place.z, place.c
    half = planes // 2
    crowd = [
        ((p + k) % spots, s if e == 0 else place.near)
        for k in range(spots) for e in range(2) if k or e
    ]
    greet(place, crowd, True)

    streams = [(tok_ref, tok_buf, tok_all), (cot_ref, cot_buf, cot_all)]
    spread = []
    for own, buf, _ in streams:
        row = []
        for k in range(1, spots):
            q = (p + k) % spots
            copy = place.far(own.at[q], buf.at[p], place.take(), (q, s))
            copy.start()
            row.append(copy)
        spread.append(row)
    proj_line = Relay(place, proj_ref, lambda at: proj_all.at[at])
    head_line = Relay(place, out_ref, lambda at: col.at[at])
    proj_line.start()
    head_line.start()
    kept = [place.keep(proj_ref, proj_all.at[z]), place.keep(out_ref, col.at[z])]
    mailed = []
    for own, slot in (
        (first_in_ref, lambda q, core: first_all.at[q, z, core]),
        (next_in_ref, lambda q, core: next_slot.at[q, core]),
    ):
        for k in range(spots):
            for e in range(2):
                q = (p + k) % spots
                core = c if e == 0 else 1 - c
                if k or e:
                    copy = place.far(
                        own.at[q, core], slot(p, c), place.take(),
                        (q, s if e == 0 else place.near),
                    )
                    copy.start()
                    mailed.append(copy)
        kept.append(place.keep(own.at[p, c], slot(p, c)))
    for copy in kept:
        copy.start()
    moved = []
    for (own, buf, whole), row in zip(streams, spread):
        send_at, recv_at = place.take(spots), place.take(planes)
        place.kept += 1
        local = place.kept - 1
        for k in range(spots):
            j = (p + spots - k) % spots
            if k:
                row[k - 1].wait_recv()
            data = own.at[p] if k == 0 else buf.at[j]

            @pl.when(j != z)
            def _():
                place.far(data, whole.at[z, c, p], send_at + k, place.at_z(j), recv_at + z).start()

            @pl.when(j == z)
            def _():
                pltpu.make_async_copy(data, whole.at[z, c, p], copy_sem.at[local]).start()

        moved.append((send_at, recv_at, local))
    for copy in kept:
        copy.wait()
    count = len(mailed) // 2
    for copy in mailed[:count]:
        copy.wait_recv()
    all_spots = pl.ds(0, spots)
    in_line = Relay(place, first_all.at[all_spots, z], lambda at: first_all.at[all_spots, at])
    in_line.start()
    head_line.stage(1)
    proj_line.stage(1)
    gathers = []
    for (own, buf, whole), (send_at, recv_at, local) in zip(streams, moved):
        gather = PlaneGather(place, whole, [(z + i) % planes for i in range(planes)])
        for i in range(planes):
            at = (z + i) % planes
            piece = whole.at[at, c, p]
            if i == 0:
                pltpu.make_async_copy(tok_ref.at[0], piece, copy_sem.at[local]).wait()
            else:
                place.far(piece, piece, send_at, place.at_z(at), recv_at + at).wait_recv()
            gather.start(i)
        gathers.append(gather)
        if len(gathers) == 1:
            in_line.stage(1)
            head_line.stage(2)
            proj_line.stage(2)
    for i in range(planes):
        gathers[0].arrive(i)
    for k in range(2, planes):
        in_line.stage(k)
        if k + 1 < planes:
            head_line.stage(k + 1)
            proj_line.stage(k + 1)
        if k == 2:
            for i in range(planes):
                gathers[0].arrive_diagonal(i)
            for i in range(planes):
                gathers[1].arrive(i)
            for i in range(planes):
                gathers[1].arrive_diagonal(i)
    keep, over = heads_home(place, col, heads_all, half)
    for copy in mailed[count:]:
        copy.wait_recv()
    for gather in gathers:
        gather.finish()
    keep.wait()
    over.wait()
    for line in (in_line, head_line, proj_line):
        line.finish()
    for row in spread:
        for copy in row:
            copy.wait_send()
    for copy in mailed:
        copy.wait_send()
    for (own, buf, whole), (send_at, recv_at, local) in zip(streams, moved):
        for k in range(spots):
            j = (p + spots - k) % spots

            @pl.when(j != z)
            def _():
                place.far(own.at[p], whole.at[z, c, p], send_at + k, place.at_z(j)).wait_send()


def bring_all(tok, cot, first_in, next_in, out_w, proj_w, spots, planes):
    _, rows, width = tok.shape
    vmem = pl.BlockSpec(memory_space=pltpu.VMEM)
    hbm = pl.BlockSpec(memory_space=pl.ANY)
    whole = jax.ShapeDtypeStruct((planes, 2, spots, rows, width), BF)
    owned, cols = first_in.shape[2:]
    return pl.pallas_call(
        functools.partial(start_kernel, spots, planes),
        out_shape=[
            whole, whole,
            jax.ShapeDtypeStruct((spots, planes, 2, owned, cols), BF),
            jax.ShapeDtypeStruct(next_in.shape, BF),
            jax.ShapeDtypeStruct((planes // 2, 2) + out_w.shape, BF),
            jax.ShapeDtypeStruct((planes,) + proj_w.shape, BF),
        ],
        in_specs=[vmem] * 6,
        out_specs=[hbm] * 6,
        scratch_shapes=[
            pltpu.VMEM((spots, rows, width), BF),
            pltpu.VMEM((spots, rows, width), BF),
            pltpu.VMEM((planes,) + out_w.shape, BF),
        ] + sems(
            2 * (spots - 1) + 2 * (2 * spots - 1) + 6 * planes + 2 * (spots + planes)
            + 2 * gather_sems(spots, planes) + 1,
            7,
        ),
        compiler_params=pltpu.CompilerParams(
            collective_id=3, has_side_effects=True, vmem_limit_bytes=32 << 20
        ),
        name="bring_all",
    )(tok, cot, first_in, next_in, out_w, proj_w)


def gather_kernel(spots, planes, jobs, *refs):
    place = Place(spots, planes, None, None, None)
    (own_ref,), (all_ref,), _, made = unpack(jobs, place, refs, 1, 1, 0)
    groups = own_ref.shape[0]
    half = groups // 2
    parts = [pl.ds(0, half), pl.ds(half, half)]
    plane = [(q, place.s) for q in place.plane_partners()] + [(place.p, place.near)]
    greet(place, plane, bool(made))
    gather = PlaneGather(place, all_ref, parts)
    for i in range(2):
        gather.start(i, own_ref.at[parts[i]])
    keep = place.keep(own_ref, all_ref.at[pl.ds(0, groups), place.c, place.p])
    keep.start()
    for job in made:
        job.start()
    for i in range(2):
        gather.arrive(i)
    for job in made:
        job.stage(0)
    for i in range(2):
        gather.arrive_diagonal(i)
    for i in range(1, planes - 1):
        for job in made:
            job.stage(i)
    for job in made:
        job.finish()
    keep.wait()
    gather.finish()


def gather_tokens(own, spots, planes, number, jobs):
    groups, rows, width = own.shape
    whole = jax.ShapeDtypeStruct((groups, 2, spots, rows, width), own.dtype)
    out = job_call(
        gather_kernel, "gather_tokens", number, spots, planes, jobs, [own], [VM],
        [(whole, pl.ANY)], [], gather_sems(spots, 2), 1,
    )
    return [out[0].reshape(-1, width)] + list(out[1:])


class PlaneScatter:
    def __init__(self, place, part_ref, out_ref, near_buf, mine, relay, inbox):
        self.place, self.out = place, out_ref
        self.near_buf, self.mine, self.relay, self.inbox = near_buf, mine, relay, inbox
        spots, p, c = place.spots, place.p, place.c
        self.others = place.plane_partners()
        _, self.groups, self.rows, _ = mine.shape
        half = self.groups // 2
        self.halves = [pl.ds(0, half), pl.ds(half, half)]
        self.whole = pl.ds(0, self.groups)
        if spots == 4:
            spot_of = [p] + self.others + [3 - p]
            self.order = [3, 1, 2, 0]
        else:
            spot_of = [p] + self.others
            self.order = list(range(1, spots)) + [0]
        self.handed, self.kept, self.sent = {}, {}, {}
        for m in self.order:
            self.handed[m] = place.far(
                part_ref.at[self.whole, 1 - c, spot_of[m]], near_buf.at[m],
                place.take(), (p, place.near),
            )
            self.kept[m] = place.keep(part_ref.at[self.whole, c, spot_of[m]], mine.at[m])

    def start(self):
        for m in self.order:
            self.handed[m].start()
            self.kept[m].start()

    def add(self, first, count, into, left, right):
        step = min(self.rows, 16)
        per = self.rows // step

        def one(i, carry):
            g = first + i // per
            at = pl.ds(pl.multiple_of((i % per) * step, step), step)
            into[g, at, :] = (left(g, at) + right(g, at)).astype(into.dtype)
            return carry

        lax.fori_loop(0, count * per, one, 0)

    def far(self, name, m, part, slot, dest):
        copy = self.place.far(self.mine.at[m, part], slot, self.place.take(), (dest, self.place.s))
        copy.start()
        self.sent[name] = copy

    def combine(self, m):
        mine, near_buf = self.mine, self.near_buf
        self.handed[m].wait_recv()
        self.kept[m].wait()
        self.add(
            0, self.groups, self.out if m == 0 else mine.at[m],
            lambda g, at: mine[m, g, at, :].astype(F32),
            lambda g, at: near_buf[m, g, at, :].astype(F32),
        )
        if self.place.spots == 4:
            x, y = self.others
            first, last = self.halves
            if m == 3:
                self.far(0, 3, first, self.relay.at[0], x)
                self.far(1, 3, last, self.relay.at[1], y)
            elif m == 1:
                self.far(2, 1, first, self.inbox.at[0, first], x)
            elif m == 2:
                self.far(3, 2, last, self.inbox.at[1, last], y)
        elif m > 0:
            self.far(m + 1, m, self.whole, self.inbox.at[m - 1], self.others[m - 1])

    def pass_on(self):
        if self.place.spots != 4:
            return
        mine, relay = self.mine, self.relay
        x, y = self.others
        first, last = self.halves
        half = self.groups // 2
        self.sent[0].wait_recv()
        self.add(
            0, half, mine.at[2],
            lambda g, at: mine[2, g, at, :].astype(F32),
            lambda g, at: relay[0, g, at, :].astype(F32),
        )
        self.far(4, 2, first, self.inbox.at[1, first], y)
        self.sent[1].wait_recv()
        self.add(
            half, half, mine.at[1],
            lambda g, at: mine[1, g, at, :].astype(F32),
            lambda g, at: relay[1, g - half, at, :].astype(F32),
        )
        self.far(5, 1, last, self.inbox.at[0, last], x)

    def total(self):
        for name in self.sent:
            if name >= 2:
                self.sent[name].wait_recv()
        out, inbox = self.out, self.inbox

        def received(g, at):
            total = inbox[0, g, at, :].astype(F32)
            for slot in range(1, inbox.shape[0]):
                total = total + inbox[slot, g, at, :].astype(F32)
            return total

        self.add(0, self.groups, out, lambda g, at: out[g, at, :], received)

    def finish(self):
        for m in self.order:
            self.handed[m].wait_send()
        for name in self.sent:
            self.sent[name].wait_send()


def scatter_kernel(count, spots, planes, jobs, *refs):
    place = Place(spots, planes, None, None, None)
    ins, outs, scratch, made = unpack(jobs, place, refs, count, count, 4 * count)
    streams = [
        PlaneScatter(place, ins[i], outs[i], *scratch[4 * i : 4 * i + 4]) for i in range(count)
    ]
    plane = [(q, place.s) for q in place.plane_partners()] + [(place.p, place.near)]
    greet(place, plane, bool(made))
    for stream in streams:
        stream.start()
    for job in made:
        job.start()
    for stream in streams:
        for m in stream.order:
            stream.combine(m)
    for job in made:
        job.stage(0)
    for stream in streams:
        stream.pass_on()
    for job in made:
        job.stage(1)
    for stream in streams:
        stream.total()
    for i in range(2, planes - 1):
        for job in made:
            job.stage(i)
    for job in made:
        job.finish()
    for stream in streams:
        stream.finish()


def scatter_tokens(parts, spots, planes, number, jobs):
    total, width = parts[0].shape
    groups = planes
    rows = total // (groups * 2 * spots)
    slots = 2 if spots == 4 else spots - 1
    piece = (groups, rows, width)
    count = len(parts)
    return job_call(
        functools.partial(scatter_kernel, count), "scatter_tokens", number, spots, planes, jobs,
        [part.reshape(groups, 2, spots, rows, width) for part in parts], [pl.ANY] * count,
        [(jax.ShapeDtypeStruct(piece, F32), VM)] * count,
        [
            VM((spots,) + piece, BF), VM((spots,) + piece, BF),
            VM((2, groups // 2, rows, width), BF), VM((slots,) + piece, BF),
        ] * count,
        count * (spots + (6 if spots == 4 else spots - 1)), count * spots,
    )


def end_kernel(spots, planes, jobs, *refs):
    place = Place(spots, planes, None, None, None)
    ins, outs, scratch, _ = unpack(jobs, place, refs, 5, 5, 2)
    p, s, z, c = place.p, place.s, place.z, place.c
    crowd = [
        (k, e, ((p + k) % spots, s if e == 0 else place.near))
        for k in range(spots) for e in range(2) if k or e
    ]
    greet(place, [dest for _, _, dest in crowd], True)
    streams = list(zip(ins[:2], scratch, outs[:2]))
    moved = []
    for own, buf, out in streams:
        row = []
        for k in range(1, planes):
            to = (z + k) % planes
            copy = place.far(own.at[to], buf.at[z], place.take(), place.at_z(to))
            copy.start()
            row.append(copy)
        moved.append(row)
    mailed, kept = [], []
    for own, out in zip(ins[2:4], outs[2:4]):
        for k, e, dest in crowd:
            core = c if e == 0 else 1 - c
            copy = place.far(own.at[dest[0], core], out.at[p, c], place.take(), dest)
            copy.start()
            mailed.append(copy)
        kept.append(place.keep(own.at[p, c], out.at[p, c]))
    for k, e, dest in crowd:
        copy = place.far(ins[4], outs[4].at[p, c], place.take(), dest)
        copy.start()
        mailed.append(copy)
    kept.append(place.keep(ins[4], outs[4].at[p, c]))
    for copy in kept:
        copy.start()
    homes = []
    for (own, buf, out), row in zip(streams, moved):
        send_at, recv_at = place.take(planes), place.take(spots)
        place.kept += 1
        local = place.kept - 1
        for k in range(planes):
            j = (z + planes - k) % planes
            if k:
                row[k - 1].wait_recv()
            data = own.at[z] if k == 0 else buf.at[j]

            @pl.when(j != p)
            def _():
                place.far(data, out.at[p], send_at + k, (j, s), recv_at + p).start()

            @pl.when(j == p)
            def _():
                pltpu.make_async_copy(data, out.at[p], place.copy_sem.at[local]).start()

        homes.append((send_at, recv_at, local))
    for copy in mailed:
        copy.wait_recv()
    for (own, buf, out), (send_at, recv_at, local) in zip(streams, homes):
        for k in range(1, spots):
            q = (p + k) % spots
            place.far(out.at[q], out.at[q], send_at, (q, s), recv_at + q).wait_recv()
        pltpu.make_async_copy(own.at[0], out.at[p], place.copy_sem.at[local]).wait()
    for copy in kept:
        copy.wait()
    for row in moved:
        for copy in row:
            copy.wait_send()
    for copy in mailed:
        copy.wait_send()
    for (own, buf, out), (send_at, recv_at, local) in zip(streams, homes):
        for k in range(planes):
            j = (z + planes - k) % planes

            @pl.when(j != p)
            def _():
                place.far(own.at[0], out.at[p], send_at + k, (j, s)).wait_send()


def send_home(grad_tok, outputs, first_grad, next_grad, sums, spots, planes):
    _, rows, width = grad_tok.shape
    home = jax.ShapeDtypeStruct((spots, rows, width), BF)
    slot = jax.ShapeDtypeStruct(first_grad.shape, BF)
    return job_call(
        end_kernel, "send_home", 9, spots, planes, [],
        [grad_tok, outputs, first_grad, next_grad, sums], [VM] * 5,
        [
            (home, pl.ANY), (home, pl.ANY), (slot, pl.ANY), (slot, pl.ANY),
            (jax.ShapeDtypeStruct((spots, 2) + sums.shape, F32), pl.ANY),
        ],
        [VM((planes, rows, width), BF)] * 2,
        2 * (planes - 1) + 3 * (2 * spots - 1) + 2 * (spots + planes), 5,
    )


class Net:
    def __init__(self, mesh):
        self.planes = mesh.shape["seq"] // 2
        self.spots = mesh.shape["dp"]
        self.p = lax.axis_index("dp")
        self.z = lax.axis_index("seq") // 2
        self.c = lax.axis_index("seq") % 2

    def permute(self, x, to):
        pairs = []
        for p in range(self.spots):
            for z in range(self.planes):
                for c in range(2):
                    tp, tz, tc = to(p, z, c)
                    source = (p * self.planes + z) * 2 + c
                    pairs.append((source, (tp * self.planes + tz) * 2 + tc))
        return lax.ppermute(x, AXES, pairs)

    def turned(self, x):
        return self.permute(x, lambda p, z, c: (z, p, c))


def normalize(resid):
    mean = jnp.mean(resid, axis=-1, keepdims=True)
    center = resid - mean
    spread = jnp.mean(center * center, axis=-1, keepdims=True)
    inv = lax.rsqrt(spread + norm_eps)
    return center * inv, inv


def gelu_parts(pre):
    cdf = 0.5 * (1.0 + lax.erf(pre * (2.0**-0.5)))
    return cdf


def on_device(
    mesh, tokens, cotangent, segments, qkv_weight, out_weight, fc_weight, proj_weight,
    biases, ln_gain, ln_shift,
):
    net = Net(mesh)
    spots, planes = net.spots, net.planes
    team = spots * 2
    layers, rows, _ = qkv_weight.shape
    width = out_weight.shape[2]
    local = tokens.shape[1]
    head_cols = width // team
    hidden_all = fc_weight.shape[2]
    fc_piece = proj_weight.shape[1]
    owner = (net.p * planes + net.z) * 2 + net.c
    assert spots == planes

    seg_row = net.turned(segments)
    full_len = seg_row.shape[1]
    index = lax.broadcasted_iota(jnp.int32, (1, full_len), 1)
    starts = jnp.zeros((1, full_len), jnp.int32)
    for doc in range(3):
        count = jnp.sum((seg_row == doc).astype(jnp.int32))
        starts = starts + jnp.where(seg_row > doc, count, 0)
    position = (index - starts).astype(F32)
    first_block = starts[0, ::BLOCK] // BLOCK
    half = ROT // 2
    entry = jnp.arange(head_cols, dtype=jnp.int32) % HEAD_DIM
    inverse = 10000.0 ** (-2.0 * (entry % half).astype(F32) / ROT)
    inverse = jnp.where(entry < ROT, inverse, 0.0)
    angle = position.reshape(full_len, 1) * inverse[None, :]
    cosine, sine = jnp.cos(angle), jnp.sin(angle)

    gain_own = ln_gain.astype(F32)
    shift_own = ln_shift.astype(F32)
    t_at = net.p * 2 + net.c
    qkv_cols, fc_cols = 3 * head_cols, planes * fc_piece
    in_cols = qkv_cols + fc_cols
    bias_rows = biases.shape[1]

    def in_weight(layer):
        qkv = qkv_weight[layer].astype(F32) * gain_own[layer, 0][:, None]
        qkv = qkv.astype(BF).reshape(rows, 3, spots, 2, head_cols)
        qkv = jnp.transpose(qkv, (2, 3, 0, 1, 4)).reshape(spots, 2, rows, qkv_cols)
        fc = fc_weight[layer].astype(F32) * gain_own[layer, 1][:, None]
        fc = fc.astype(BF).reshape(rows, spots, planes, 2, fc_piece)
        fc = jnp.transpose(fc, (1, 3, 0, 2, 4)).reshape(spots, 2, rows, fc_cols)
        return [qkv, fc]

    small = jnp.concatenate([biases, ln_gain, ln_shift], axis=1).reshape(-1, rows).T
    small_cols = small.shape[1]
    small = jnp.pad(small, ((0, 0), (0, 128 - small_cols)))
    small = jnp.broadcast_to(small, (spots, 2, rows, 128))
    first_in = jnp.concatenate(in_weight(0) + [small], axis=-1)
    next_in = jnp.concatenate(in_weight(1), axis=-1)

    per_spot = (spots, local // spots, width)
    tok_all, cot_all, first_all, next_slot, heads_w0, proj_w0 = bring_all(
        tokens.reshape(per_spot), cotangent.reshape(per_spot), first_in, next_in,
        out_weight[0], proj_weight[0], spots, planes,
    )
    first_all = first_all.reshape(width, -1)
    small = first_all[:, in_cols : in_cols + small_cols].T.astype(F32).reshape(layers, -1, width)
    bias_all, gain_all, shift_all = (
        small[:, :bias_rows], small[:, bias_rows : bias_rows + 2], small[:, bias_rows + 2 :],
    )
    weights_in = [(first_all[:, :qkv_cols], first_all[:, qkv_cols:in_cols]), None]
    whole_in = [first_all, None]
    weights_out = [(heads_w0.reshape(head_cols, width), proj_w0.reshape(fc_cols, width)), None]

    def bias_in(layer):
        qkv_b = bias_all[layer, :3].reshape(3, team, head_cols)
        qkv_b = lax.dynamic_index_in_dim(qkv_b, t_at, 1, keepdims=False).reshape(1, -1)
        fc_b = bias_all[layer, 4 : bias_rows - 1].reshape(spots, planes, 2, fc_piece)
        fc_b = lax.dynamic_index_in_dim(fc_b, net.p, 0, keepdims=False)
        fc_b = lax.dynamic_index_in_dim(fc_b, net.c, 1, keepdims=False).reshape(1, -1)
        ratio = shift_all[layer] / gain_all[layer]
        high = ratio.astype(BF)
        low = (ratio - high.astype(F32)).astype(BF)
        qkv_w, fc_w = weights_in[layer]
        qkv_b = qkv_b + nn(high[:1], qkv_w) + nn(low[:1], qkv_w)
        fc_b = fc_b + nn(high[1:], fc_w) + nn(low[1:], fc_w)
        return qkv_b, fc_b

    def own_part(whole):
        part = lax.dynamic_index_in_dim(whole, net.c, 1, keepdims=False)
        return lax.dynamic_index_in_dim(part, net.p, 1, keepdims=False)

    cot_own = own_part(cot_all)
    cot_all = cot_all.reshape(full_len, width)

    resid = own_part(tok_all).astype(F32)
    saved = []
    for layer in range(layers):
        normed, inv = normalize(resid)
        if layer == 0:
            normed_all = normalize(tok_all.reshape(full_len, width).astype(F32))[0].astype(BF)
        else:
            normed_all, heads_w, proj_w = gather_tokens(
                normed.astype(BF), spots, planes, 4,
                [out_weight_gather(out_weight[layer], proj_weight[layer], spots, planes)],
            )
            weights_out[layer] = (
                heads_w.reshape(head_cols, width), proj_w.reshape(fc_cols, width)
            )
        qkv_w, fc_w = weights_in[layer]
        head_w, proj_w = weights_out[layer]
        qkv_b, fc_b = bias_in(layer)
        mixed = nn(normed_all, qkv_w) + qkv_b
        hidden_pre = nn(normed_all, fc_w) + fc_b
        query, key, value, ctx, ctx_low, lse = attn_forward(
            mixed, cosine, sine, starts, first_block
        )
        hidden = (hidden_pre * gelu_parts(hidden_pre)).astype(BF)
        part = pair_product(hidden, ctx_low, [proj_w, head_w], False)
        saved.append((normed, inv, normed_all, query, key, value, ctx, ctx_low, lse, hidden_pre, hidden))
        end_bias = bias_all[layer, 3] + bias_all[layer, bias_rows - 1]
        if layer < layers - 1:
            summed, next_all = scatter_tokens(
                [part], spots, planes, 5, [in_weight_gather(next_slot, spots, planes)]
            )
            next_all = next_all.reshape(width, -1)
            whole_in[1] = next_all
            weights_in[1] = (next_all[:, :qkv_cols], next_all[:, qkv_cols:])
            resid = resid + summed + end_bias
    last_part, last_bias = part, end_bias

    grad_own = cot_own
    sums_rows = -(-(in_cols + width) // 1024) * 8

    def out_grads(ctx_low, hidden, grad_all):
        heads = tn(ctx_low, grad_all).astype(BF).reshape(planes // 2, 2, rows, width)
        proj = tn(hidden, grad_all).astype(BF).reshape(planes, fc_piece, width)
        return out_grad_sum(heads, proj, spots, planes)

    in_slots, in_sums, out_parts = [None] * layers, [None] * layers, [None] * layers
    waiting = None
    for layer in reversed(range(layers)):
        normed, inv, normed_all, query, key, value, ctx, ctx_low, lse, hidden_pre, hidden = saved[layer]
        qkv_w, fc_w = weights_in[layer]
        head_w, proj_w = weights_out[layer]
        if layer == layers - 1:
            grad_all = cot_all
        else:
            grad_all, *out_parts[layer + 1] = gather_tokens(grad_own, spots, planes, 6, [waiting])
        grad_ctx = nt(grad_all, head_w).astype(BF)
        grad_mixed = attn_backward(
            query, key, value, ctx, lse, grad_ctx, cosine, sine, starts, first_block
        )
        cdf = gelu_parts(hidden_pre)
        density = jnp.exp(-0.5 * hidden_pre * hidden_pre) * ((2.0 * jnp.pi) ** -0.5)
        grad_pre = (nt(grad_all, proj_w) * (cdf + hidden_pre * density)).astype(BF)
        part = pair_product(grad_mixed, grad_pre, [whole_in[layer]], True)

        owners = (spots, planes, 2, rows)
        grad_qkv = tn(normed_all, grad_mixed).astype(BF).reshape(owners + (qkv_cols,))
        grad_fc = tn(normed_all, grad_pre).astype(BF).reshape(owners + (fc_cols,))
        sums = jnp.concatenate(
            [
                jnp.sum(grad_mixed.astype(F32), axis=0),
                jnp.sum(grad_pre.astype(F32), axis=0),
                jnp.sum(grad_own.astype(F32), axis=(0, 1)),
            ]
        )
        sums = jnp.pad(sums, (0, sums_rows * 128 - sums.shape[0])).reshape(sums_rows, 128)
        jobs = [in_grad_sum(grad_qkv, grad_fc, sums, spots, planes)]
        waiting = out_grads(ctx_low, hidden, grad_all)
        if layer == 0:
            jobs.append(waiting)
        if layer:
            norm_grad, in_slots[layer], in_sums[layer] = scatter_tokens(
                [part], spots, planes, 7, jobs
            )
        else:
            norm_grad, summed, in_slots[layer], in_sums[layer], *out_parts[layer] = scatter_tokens(
                [part, last_part], spots, planes, 8, jobs
            )
            outputs_own = (resid + summed + last_bias).astype(BF)
        mean_grad = jnp.mean(norm_grad, axis=-1, keepdims=True)
        mean_dot = jnp.mean(norm_grad * normed, axis=-1, keepdims=True)
        grad_next = grad_own.astype(F32) + inv * (norm_grad - mean_grad - normed * mean_dot)
        grad_own = lax.optimization_barrier(grad_next.astype(BF))

    grad_tokens, outputs, *in_grads, sums_all = send_home(
        grad_own, outputs_own, in_slots[0], in_slots[1], jnp.concatenate(in_sums, axis=0), spots, planes
    )
    sums_all = sums_all.reshape(team, layers, -1)
    scale = jnp.concatenate([gain_own, shift_own], axis=1).reshape(4 * layers, rows).T
    grad_qkv, grad_fc, stats = owner_grads(
        in_grads[0], in_grads[1], sums_all, qkv_weight, fc_weight, scale, head_cols, fc_piece, planes
    )
    stats = jnp.transpose(stats.reshape(rows, layers, 2, 2), (3, 1, 2, 0))
    end_sum = jnp.sum(sums_all[:, :, in_cols : in_cols + width], axis=0)[:, None]
    qkv_sum = sums_all[:, :, :qkv_cols].reshape(team, layers, 3, head_cols)
    qkv_sum = jnp.transpose(qkv_sum, (1, 2, 0, 3)).reshape(layers, 3, width)
    fc_sum = sums_all[:, :, qkv_cols:in_cols].reshape(spots, 2, layers, planes, fc_piece)
    fc_sum = jnp.transpose(fc_sum, (2, 0, 3, 1, 4)).reshape(layers, -1, width)
    bias_grad = jnp.concatenate([qkv_sum, end_sum, fc_sum, end_sum], axis=1)
    bias_grad = lax.dynamic_slice_in_dim(bias_grad, owner * rows, rows, 2)
    whole = (1, local, width)
    return (
        outputs.reshape(whole),
        grad_tokens.reshape(whole),
        grad_qkv,
        jnp.stack([part[0] for part in out_parts]),
        grad_fc,
        jnp.stack([part[1] for part in out_parts]),
        bias_grad,
        stats[0],
        stats[1],
    )


def solution(mesh):
    return jax.shard_map(
        functools.partial(on_device, mesh),
        mesh=mesh,
        in_specs=(
            P("dp", "seq", None),
            P("dp", "seq", None),
            P("dp", None),
            P(None, ("dp", "seq"), None),
            P(None, ("dp", "seq"), None),
            P(None, ("dp", "seq"), None),
            P(None, ("dp", "seq"), None),
            P(None, None, ("dp", "seq")),
            P(None, None, ("dp", "seq")),
            P(None, None, ("dp", "seq")),
        ),
        out_specs=(
            P("dp", "seq", None),
            P("dp", "seq", None),
            P(None, ("dp", "seq"), None),
            P(None, ("dp", "seq"), None),
            P(None, ("dp", "seq"), None),
            P(None, ("dp", "seq"), None),
            P(None, None, ("dp", "seq")),
            P(None, None, ("dp", "seq")),
            P(None, None, ("dp", "seq")),
        ),
        check_vma=False,
    )
```

```python
import functools

import jax
import jax.numpy as jnp
from jax import lax
from jax.experimental import pallas as pl
from jax.experimental.pallas import tpu as pltpu
from jax.sharding import PartitionSpec as P

HEAD_DIM = 64
ROT = 16
norm_eps = 1e-05
mask_fill = -1e30
BF = jnp.bfloat16
F32 = jnp.float32
AXES = ("dp", "seq")
BLOCK = 256


def nt(left, right):
    return lax.dot_general(left, right, (((1,), (1,)), ((), ())), preferred_element_type=F32)


def nn(left, right):
    return lax.dot_general(left, right, (((1,), (0,)), ((), ())), preferred_element_type=F32)


def tn(left, right):
    return lax.dot_general(left, right, (((0,), (0,)), ((), ())), preferred_element_type=F32)


def lane_in_head(shape):
    lane = lax.broadcasted_iota(jnp.int32, shape, len(shape) - 1)
    return lane, lane % HEAD_DIM


def rope(vals, cosine, sine):
    width = vals.shape[-1]
    half = ROT // 2
    _, entry = lane_in_head(vals.shape)
    up = pltpu.roll(vals, width - half, 1)
    down = pltpu.roll(vals, half, 1)
    swapped = jnp.where(entry < half, -up, down)
    return vals * cosine + swapped * sine


def rope_back(grads, cosine, sine):
    width = grads.shape[-1]
    half = ROT // 2
    _, entry = lane_in_head(grads.shape)
    scaled = grads * sine
    up = pltpu.roll(scaled, width - half, 1)
    down = pltpu.roll(scaled, half, 1)
    swapped = jnp.where(entry < half, up, jnp.where(entry < ROT, -down, 0.0))
    return grads * cosine + swapped


def head_only(vals, head):
    lane, _ = lane_in_head(vals.shape)
    keep = (lane >= head * HEAD_DIM) & (lane < (head + 1) * HEAD_DIM)
    return jnp.where(keep, vals, jnp.zeros_like(vals))


def attn_fwd_kernel(
    first_ref, mixed_ref, cos_ref, sin_ref, start_ref,
    query_ref, key_ref, value_ref, ctx_ref, ctx_low_ref, lse_ref,
    value_t_ref,
):
    at = pl.program_id(0)
    total, width = key_ref.shape
    heads = width // HEAD_DIM

    @pl.when(at == 0)
    def _():
        def one(i, carry):
            rows = pl.ds(pl.multiple_of(i * BLOCK, BLOCK), BLOCK)
            keys = mixed_ref[rows, width : 2 * width]
            key_ref[rows, :] = rope(keys, cos_ref[rows, :], sin_ref[rows, :]).astype(BF)
            vals = mixed_ref[rows, 2 * width : 3 * width]
            value_ref[rows, :] = vals.astype(BF)
            value_t_ref[:, rows] = vals.T.astype(BF)
            return carry

        lax.fori_loop(0, total // BLOCK, one, 0)

    rows = pl.ds(pl.multiple_of(at * BLOCK, BLOCK), BLOCK)
    quer = rope(mixed_ref[rows, 0:width], cos_ref[rows, :], sin_ref[rows, :]).astype(BF)
    quer = quer * jnp.asarray(HEAD_DIM**-0.5, BF)
    query_ref[...] = quer
    by_head = [head_only(quer, h) for h in range(heads)]
    key_iota = lax.broadcasted_iota(jnp.int32, (BLOCK, BLOCK), 0)
    query_pos = at * BLOCK + lax.broadcasted_iota(jnp.int32, (1, BLOCK), 1)
    starts = start_ref[...]

    def step(turn, carry):
        block = at - turn
        keys_at = pl.ds(pl.multiple_of(block * BLOCK, BLOCK), BLOCK)
        keys = key_ref[keys_at, :]
        vals_t = value_t_ref[:, keys_at]
        keep = (key_iota >= starts - block * BLOCK) & (key_iota <= query_pos - block * BLOCK)
        out = []
        for h in range(heads):
            top, total_h, acc = carry[h]
            scores = jnp.where(keep, nt(keys, by_head[h]), mask_fill)
            new_top = jnp.maximum(top, jnp.max(scores, axis=0, keepdims=True))
            fade = jnp.exp(top - new_top)
            probs = jnp.exp(scores - new_top)
            total_h = total_h * fade + jnp.sum(probs, axis=0, keepdims=True)
            acc = acc * fade + nn(vals_t, probs.astype(BF))
            out.append((new_top, total_h, acc))
        return tuple(out)

    init = tuple(
        (
            jnp.full((1, BLOCK), mask_fill, F32),
            jnp.zeros((1, BLOCK), F32),
            jnp.zeros((width, BLOCK), F32),
        )
        for h in range(heads)
    )
    done = lax.fori_loop(0, at - first_ref[at] + 1, step, init)
    parts = []
    for h in range(heads):
        top, total_h, acc = done[h]
        lse_ref[h : h + 1, :] = top + jnp.log(total_h)
        parts.append(acc[h * HEAD_DIM : (h + 1) * HEAD_DIM, :] / total_h)
    ctx = jnp.concatenate(parts, axis=0).T
    ctx_ref[...] = ctx
    ctx_low_ref[...] = ctx.astype(BF)


def attn_forward(mixed, cosine, sine, starts, first_block):
    total, width = cosine.shape
    heads = width // HEAD_DIM
    blocks = total // BLOCK
    full = lambda cols: pl.BlockSpec((total, cols), lambda i, f: (0, 0))
    rows = pl.BlockSpec((BLOCK, width), lambda i, f: (i, 0))
    lanes = lambda n: pl.BlockSpec((n, BLOCK), lambda i, f: (0, i))
    wide = jax.ShapeDtypeStruct((total, width), BF)
    return pl.pallas_call(
        attn_fwd_kernel,
        grid_spec=pltpu.PrefetchScalarGridSpec(
            num_scalar_prefetch=1,
            grid=(blocks,),
            in_specs=[full(3 * width), full(width), full(width), lanes(1)],
            out_specs=[rows, full(width), full(width), rows, rows, lanes(heads)],
            scratch_shapes=[pltpu.VMEM((width, total), BF)],
        ),
        out_shape=[
            wide, wide, wide,
            jax.ShapeDtypeStruct((total, width), F32),
            wide,
            jax.ShapeDtypeStruct((heads, total), F32),
        ],
        compiler_params=pltpu.CompilerParams(
            dimension_semantics=("arbitrary",), vmem_limit_bytes=24 << 20
        ),
        cost_estimate=pl.CostEstimate(
            flops=20 * 4 * BLOCK * BLOCK * width * heads,
            bytes_accessed=total * width * 40,
            transcendentals=20 * BLOCK * BLOCK * heads,
        ),
        name="attn_fwd",
    )(first_block, mixed, cosine, sine, starts)


def attn_bwd_kernel(
    first_ref, query_ref, key_ref, value_ref, ctx_ref, lse_ref, grad_ref, cos_ref, sin_ref, start_ref,
    out_ref,
    key_t_ref, grad_key_ref, grad_value_ref,
):
    at = pl.program_id(0)
    total, width = key_ref.shape
    heads = width // HEAD_DIM

    @pl.when(at == 0)
    def _():
        def one(i, carry):
            rows = pl.ds(pl.multiple_of(i * BLOCK, BLOCK), BLOCK)
            key_t_ref[:, rows] = key_ref[rows, :].T
            grad_key_ref[rows, :] = jnp.zeros((BLOCK, width), F32)
            grad_value_ref[rows, :] = jnp.zeros((BLOCK, width), F32)
            return carry

        lax.fori_loop(0, total // BLOCK, one, 0)

    quer = query_ref[...]
    grad = grad_ref[...]
    by_head = [head_only(quer, h) for h in range(heads)]
    grad_head = [head_only(grad, h) for h in range(heads)]
    inner_t = (grad.astype(F32) * ctx_ref[...]).T
    inner = [
        jnp.sum(inner_t[h * HEAD_DIM : (h + 1) * HEAD_DIM, :], axis=0, keepdims=True)
        for h in range(heads)
    ]
    logs = [lse_ref[h : h + 1, :] for h in range(heads)]
    key_iota = lax.broadcasted_iota(jnp.int32, (BLOCK, BLOCK), 0)
    query_pos = at * BLOCK + lax.broadcasted_iota(jnp.int32, (1, BLOCK), 1)
    starts = start_ref[...]

    def step(turn, carry):
        block = at - turn
        keys_at = pl.ds(pl.multiple_of(block * BLOCK, BLOCK), BLOCK)
        keys = key_ref[keys_at, :]
        vals = value_ref[keys_at, :]
        keys_t = key_t_ref[:, keys_at]
        keep = (key_iota >= starts - block * BLOCK) & (key_iota <= query_pos - block * BLOCK)
        out = []
        grad_key = jnp.zeros((BLOCK, width), F32)
        grad_value = jnp.zeros((BLOCK, width), F32)
        for h in range(heads):
            scores = nt(keys, by_head[h])
            probs = jnp.where(keep, jnp.exp(jnp.where(keep, scores, mask_fill) - logs[h]), 0.0)
            grad_probs = nt(vals, grad_head[h])
            grad_scores = (probs * (grad_probs - inner[h])).astype(BF)
            grad_value = grad_value + nn(probs.astype(BF), grad_head[h])
            grad_key = grad_key + nn(grad_scores, by_head[h])
            out.append(carry[h] + nn(keys_t, grad_scores))
        grad_key_ref[keys_at, :] += grad_key
        grad_value_ref[keys_at, :] += grad_value
        return tuple(out)

    init = tuple(jnp.zeros((width, BLOCK), F32) for h in range(heads))
    done = lax.fori_loop(0, at - first_ref[at] + 1, step, init)
    parts = [done[h][h * HEAD_DIM : (h + 1) * HEAD_DIM, :] for h in range(heads)]
    grad_query = jnp.concatenate(parts, axis=0).T * (HEAD_DIM**-0.5)
    rows = pl.ds(pl.multiple_of(at * BLOCK, BLOCK), BLOCK)
    out_ref[rows, 0:width] = rope_back(grad_query, cos_ref[rows, :], sin_ref[rows, :]).astype(BF)

    @pl.when(at == pl.num_programs(0) - 1)
    def _():
        def one(i, carry):
            rows = pl.ds(pl.multiple_of(i * BLOCK, BLOCK), BLOCK)
            grad_key = rope_back(grad_key_ref[rows, :], cos_ref[rows, :], sin_ref[rows, :])
            out_ref[rows, width : 2 * width] = grad_key.astype(BF)
            out_ref[rows, 2 * width : 3 * width] = grad_value_ref[rows, :].astype(BF)
            return carry

        lax.fori_loop(0, total // BLOCK, one, 0)


def attn_backward(query, key, value, ctx, lse, grad_ctx, cosine, sine, starts, first_block):
    total, width = cosine.shape
    heads = width // HEAD_DIM
    blocks = total // BLOCK
    full = lambda cols: pl.BlockSpec((total, cols), lambda i, f: (0, 0))
    rows = pl.BlockSpec((BLOCK, width), lambda i, f: (i, 0))
    lanes = lambda n: pl.BlockSpec((n, BLOCK), lambda i, f: (0, i))
    return pl.pallas_call(
        attn_bwd_kernel,
        grid_spec=pltpu.PrefetchScalarGridSpec(
            num_scalar_prefetch=1,
            grid=(blocks,),
            in_specs=[
                rows, full(width), full(width), rows, lanes(heads), rows,
                full(width), full(width), lanes(1),
            ],
            out_specs=full(3 * width),
            scratch_shapes=[
                pltpu.VMEM((width, total), BF),
                pltpu.VMEM((total, width), F32),
                pltpu.VMEM((total, width), F32),
            ],
        ),
        out_shape=jax.ShapeDtypeStruct((total, 3 * width), BF),
        compiler_params=pltpu.CompilerParams(
            dimension_semantics=("arbitrary",), vmem_limit_bytes=24 << 20
        ),
        cost_estimate=pl.CostEstimate(
            flops=20 * 10 * BLOCK * BLOCK * width * heads,
            bytes_accessed=total * width * 40,
            transcendentals=20 * BLOCK * BLOCK * heads,
        ),
        name="attn_bwd",
    )(first_block, query, key, value, ctx, lse, grad_ctx, cosine, sine, starts)


def in_kernel(raw, qkv_cols, in_cols, rows_ref, weight_ref, bias_ref, mixed_ref, pre_ref, hidden_ref, *more):
    rows = rows_ref[...]
    if raw:
        rows = normalize(rows.astype(F32))[0].astype(BF)
        more[0][...] = rows
    mixed_ref[...] = nn(rows, weight_ref[:, 0:qkv_cols]) + bias_ref[:, 0:qkv_cols]
    pre = nn(rows, weight_ref[:, qkv_cols:in_cols]) + bias_ref[:, qkv_cols:in_cols]
    pre_ref[...] = pre
    hidden_ref[...] = (pre * gelu_parts(pre)).astype(BF)


def in_product(rows, weight, bias, qkv_cols, raw):
    total, width = rows.shape
    in_cols = bias.shape[1]
    fc_cols = in_cols - qkv_cols
    tall = lambda cols: pl.BlockSpec((BLOCK, cols), lambda i: (i, 0))
    full = lambda x: pl.BlockSpec(x.shape, lambda i: (0, 0))
    outs = [(qkv_cols, F32), (fc_cols, F32), (fc_cols, BF)] + ([(width, BF)] if raw else [])
    return pl.pallas_call(
        functools.partial(in_kernel, raw, qkv_cols, in_cols),
        grid=(total // BLOCK,),
        out_shape=[jax.ShapeDtypeStruct((total, cols), kind) for cols, kind in outs],
        in_specs=[tall(width), full(weight), full(bias)],
        out_specs=[tall(cols) for cols, _ in outs],
        compiler_params=pltpu.CompilerParams(
            dimension_semantics=("arbitrary",), vmem_limit_bytes=16 << 20
        ),
        cost_estimate=pl.CostEstimate(
            flops=2 * total * width * in_cols, bytes_accessed=6 * total * (width + in_cols),
            transcendentals=total * fc_cols,
        ),
        name="in_product",
    )(rows, weight, bias)


def pair_kernel(turned, cols, left_ref, right_ref, *refs):
    *weights, out_ref = refs
    if turned:
        whole = weights[0]
        split = left_ref.shape[1]
        total = nt(left_ref[...], whole[:, 0:split]) + nt(right_ref[...], whole[:, split:cols])
    else:
        total = nn(left_ref[...], weights[0][...]) + nn(right_ref[...], weights[1][...])
    out_ref[...] = total.astype(BF)


def pair_product(left, right, weights, turned):
    total = left.shape[0]
    cols = left.shape[1] + right.shape[1]
    width = weights[0].shape[0] if turned else weights[0].shape[1]
    rows = lambda x: pl.BlockSpec((BLOCK, x.shape[1]), lambda i: (i, 0))
    full = lambda x: pl.BlockSpec(x.shape, lambda i: (0, 0))
    return pl.pallas_call(
        functools.partial(pair_kernel, turned, cols),
        grid=(total // BLOCK,),
        out_shape=jax.ShapeDtypeStruct((total, width), BF),
        in_specs=[rows(left), rows(right)] + [full(w) for w in weights],
        out_specs=pl.BlockSpec((BLOCK, width), lambda i: (i, 0)),
        compiler_params=pltpu.CompilerParams(
            dimension_semantics=("arbitrary",), vmem_limit_bytes=14 << 20
        ),
        cost_estimate=pl.CostEstimate(
            flops=2 * total * cols * width, bytes_accessed=2 * total * (cols + width),
            transcendentals=0,
        ),
        name="pair_product",
    )(left, right, *weights)


def owner_kernel(
    spots, planes, head_cols, fc_piece,
    first_ref, next_ref, sums_ref, qkv_ref, fc_ref, scale_ref, qkv_out, fc_out, stat_out,
):
    layers, rows, wide = qkv_ref.shape
    width = wide // 3
    stats = []
    for layer, grad_ref in enumerate((first_ref, next_ref)):
        groups = [[], []]
        for p in range(spots):
            for core in range(2):
                t = p * 2 + core
                for j in range(3):
                    groups[0].append((p, core, j * head_cols, head_cols, j * width + t * head_cols))
                for z in range(planes):
                    groups[1].append(
                        (p, core, 3 * head_cols + z * fc_piece, fc_piece,
                         ((p * planes + z) * 2 + core) * fc_piece)
                    )
        for norm, (weight_ref, out_ref) in enumerate(((qkv_ref, qkv_out), (fc_ref, fc_out))):
            at = 4 * layer + norm
            gain, shift = scale_ref[:, at : at + 1], scale_ref[:, at + 2 : at + 3]
            gain_sum = shift_sum = 0.0
            for p, core, source, count, target in groups[norm]:
                grad = grad_ref[p, core, :, source : source + count].astype(F32)
                sums = sums_ref[p * 2 + core, layer : layer + 1, source : source + count]
                weight = weight_ref[layer, :, target : target + count].astype(F32)
                out_ref[layer, :, target : target + count] = gain * grad + shift * sums
                gain_sum = gain_sum + weight * grad
                shift_sum = shift_sum + weight * sums
            stats.append(jnp.sum(gain_sum, axis=1, keepdims=True))
            stats.append(jnp.sum(shift_sum, axis=1, keepdims=True))
    for i, stat in enumerate(stats):
        stat_out[:, i : i + 1] = stat


def owner_grads(first, following, sums, qkv_weight, fc_weight, scale, head_cols, fc_piece, planes):
    layers, rows, _ = qkv_weight.shape
    vmem = pl.BlockSpec(memory_space=pltpu.VMEM)
    return pl.pallas_call(
        functools.partial(owner_kernel, first.shape[0], planes, head_cols, fc_piece),
        out_shape=[
            jax.ShapeDtypeStruct(qkv_weight.shape, F32),
            jax.ShapeDtypeStruct(fc_weight.shape, F32),
            jax.ShapeDtypeStruct((rows, 4 * layers), F32),
        ],
        in_specs=[vmem] * 6,
        out_specs=[vmem] * 3,
        compiler_params=pltpu.CompilerParams(vmem_limit_bytes=32 << 20),
        name="owner_grads",
    )(first, following, sums, qkv_weight, fc_weight, scale)


MESH = pl.DeviceIdType.MESH


class Place:
    def __init__(self, spots, planes, send_sem, recv_sem, copy_sem):
        self.spots, self.planes = spots, planes
        self.p, self.s = lax.axis_index("dp"), lax.axis_index("seq")
        self.z, self.c = self.s // 2, self.s % 2
        self.near = self.s + 1 - 2 * self.c
        self.send_sem, self.recv_sem, self.copy_sem = send_sem, recv_sem, copy_sem
        self.used, self.kept = 0, 0

    def take(self, count=1):
        self.used += count
        return self.used - count

    def far(self, src, dst, at, dest, recv_at=None):
        return pltpu.make_async_remote_copy(
            src_ref=src, dst_ref=dst,
            send_sem=self.send_sem.at[at],
            recv_sem=self.recv_sem.at[at if recv_at is None else recv_at],
            device_id=dest, device_id_type=MESH,
        )

    def keep(self, src, dst):
        self.kept += 1
        return pltpu.make_async_copy(src, dst, self.copy_sem.at[self.kept - 1])

    def at_z(self, z):
        return (self.p, z * 2 + self.c)

    def plane_partners(self):
        p = self.p
        if self.spots == 4:
            return [p + 1 - 2 * (p % 2), p + 2 - 4 * (p // 2)]
        return [(p + k) % self.spots for k in range(1, self.spots)]


def cut(ref, splits, h, *lead):
    size = ref.shape[len(lead)] // splits
    return ref.at[(*lead, pl.ds(h * size, size))]


class Relay:
    def __init__(self, place, own, slot, splits):
        self.place, self.own, self.slot, self.splits = place, own, slot, splits
        self.up = place.take(place.planes * splits)
        self.down = place.take(place.planes * splits)

    def copy(self, src, z, h, k, step):
        place = self.place
        at = (self.up if step > 0 else self.down) + k * self.splits + h
        return place.far(src, self.slot(z, h), at, place.at_z(place.z + step))

    def start(self):
        z, last = self.place.z, self.place.planes - 1
        for h in range(self.splits):

            @pl.when(z < last)
            def _():
                self.copy(self.own(h), z, h, 0, 1).start()

            @pl.when(z > 0)
            def _():
                self.copy(self.own(h), z, h, 0, -1).start()

    def stage(self, k):
        z, last = self.place.z, self.place.planes - 1
        for h in range(self.splits):

            @pl.when(z >= k)
            def _():
                got = self.slot(z - k, h)
                self.copy(got, z - k, h, k - 1, 1).wait_recv()

                @pl.when(z < last)
                def _():
                    self.copy(got, z - k, h, k, 1).start()

            @pl.when(z + k <= last)
            def _():
                got = self.slot(z + k, h)
                self.copy(got, z + k, h, k - 1, -1).wait_recv()

                @pl.when(z > 0)
                def _():
                    self.copy(got, z + k, h, k, -1).start()

    def finish(self):
        z, last = self.place.z, self.place.planes - 1
        for k in range(last):
            for h in range(self.splits):

                @pl.when((z < last) & (z >= k))
                def _():
                    self.copy(self.slot(z, h), z, h, k, 1).wait_send()

                @pl.when((z > 0) & (z + k <= last))
                def _():
                    self.copy(self.slot(z, h), z, h, k, -1).wait_send()


class PlaneGather:
    def __init__(self, place, all_ref, parts):
        self.place, self.all_ref = place, all_ref
        self.parts = parts
        self.sent, self.passed = [], []
        relayed = place.spots == 4
        self.others = place.plane_partners()
        self.ways = len(self.others)
        count = len(parts)
        self.base = [place.take(self.ways) for _ in parts]
        self.relay = [place.take() if relayed else None for _ in parts]
        self.close = [place.take(place.spots) for _ in parts]

    def view(self, part, spot):
        return self.all_ref.at[part, self.place.c, spot]

    def near(self, i, src, spot, m):
        place = self.place
        copy = place.far(src, self.view(self.parts[i], spot), self.close[i] + m, (place.p, place.near))
        copy.start()
        self.passed.append(copy)

    def start(self, i, src=None):
        place = self.place
        src = self.view(self.parts[i], place.p) if src is None else src
        for w, q in enumerate(self.others):
            copy = place.far(
                src, self.view(self.parts[i], place.p), self.base[i] + w, (q, place.s)
            )
            copy.start()
            self.sent.append(copy)
        self.near(i, src, place.p, 0)

    def arrive(self, i):
        place = self.place
        relayed = place.spots == 4
        for w, q in enumerate(self.others):
            spot = q if relayed else (place.p + place.spots - 1 - w) % place.spots
            got = self.view(self.parts[i], spot)
            place.far(got, got, self.base[i] + w, (q, place.s)).wait_recv()
            if relayed and w == (0 if i < len(self.parts) // 2 else 1):
                copy = place.far(got, got, self.relay[i], (self.others[1 - w], place.s))
                copy.start()
                self.sent.append(copy)
            self.near(i, got, spot, 1 + w)

    def arrive_diagonal(self, i):
        place = self.place
        if place.spots == 4:
            got = self.view(self.parts[i], 3 - place.p)
            place.far(got, got, self.relay[i], (self.others[0], place.s)).wait_recv()
            self.near(i, got, 3 - place.p, 3)

    def finish(self):
        for copy in self.passed:
            copy.wait_recv()
        for copy in self.sent + self.passed:
            copy.wait_send()


def greet(place, plane, column):
    barrier = pltpu.get_barrier_semaphore()
    dests = list(plane)
    if column:
        dests += [place.at_z((place.z + k) % place.planes) for k in range(1, place.planes)]
    for dest in dests:
        pl.semaphore_signal(barrier, inc=1, device_id=dest, device_id_type=MESH)
    pl.semaphore_wait(barrier, len(dests))


def heads_home(place, col, heads_ref, half):
    c = place.c
    at = place.take()
    keep = place.keep(col.at[pl.ds(c * half, half)], heads_ref.at[pl.ds(0, half), c])
    keep.start()
    over = place.far(
        col.at[pl.ds((1 - c) * half, half)], heads_ref.at[pl.ds(0, half), c], at, (place.p, place.near)
    )
    over.start()
    return keep, over


class LineSum:
    def __init__(self, place, below, above, own_value, piece, count, splits):
        self.place, self.below, self.above = place, below, above
        self.own_value, self.piece, self.count, self.splits = own_value, piece, count, splits
        self.up = place.take(place.planes * splits)
        self.down = place.take(place.planes * splits)

    def copy(self, d, h, step):
        place = self.place
        at = (self.up if step > 0 else self.down) + d * self.splits + h
        part = cut(self.below if step > 0 else self.above, self.splits, h, d)
        return place.far(part, part, at, place.at_z(place.z + step))

    def fill(self, d, h, step, add):
        into = self.below if step > 0 else self.above
        per = self.count // self.splits

        def one(i, carry):
            at = self.piece(into, d, i)
            total = self.own_value(d, i)
            if add:
                total = (at[...].astype(F32) + total.astype(F32)).astype(BF)
            at[...] = total
            return carry

        lax.fori_loop(h * per, (h + 1) * per, one, 0)

    def start(self):
        z, last = self.place.z, self.place.planes - 1

        def send(slots, step):
            for d in slots:
                for h in range(self.splits):
                    self.fill(d, h, step, False)
                    self.copy(d, h, step).start()

        pl.when(z == 0)(lambda: send(range(last, 0, -1), 1))
        pl.when(z == last)(lambda: send(range(last), -1))

    def forward(self, d, step):
        z, last = self.place.z, self.place.planes - 1

        @pl.when((z > 0) & (z < d) if step > 0 else (z < last) & (z > d))
        def _():
            for h in range(self.splits):
                self.copy(d, h, step).wait_recv()
                self.fill(d, h, step, True)
                self.copy(d, h, step).start()

    def stage(self, i):
        z, planes = self.place.z, self.place.planes

        @pl.when(2 * z < planes)
        def _():
            self.forward(planes - 1 - i, 1)
            self.forward(i, -1)

        @pl.when(2 * z >= planes)
        def _():
            self.forward(i, -1)
            self.forward(planes - 1 - i, 1)

    def finish(self, out_piece):
        z, last = self.place.z, self.place.planes - 1

        @pl.when(z > 0)
        def _():
            for h in range(self.splits):
                self.copy(z, h, 1).wait_recv()

        @pl.when(z < last)
        def _():
            for h in range(self.splits):
                self.copy(z, h, -1).wait_recv()

        def store(sources):
            def one(i, carry):
                total = self.own_value(z, i).astype(F32)
                for source in sources:
                    total = total + self.piece(source, z, i)[...].astype(F32)
                at = out_piece(i)
                at[...] = total.astype(at.dtype)
                return carry

            lax.fori_loop(0, self.count, one, 0)

        pl.when(z == 0)(lambda: store([self.above]))
        pl.when(z == last)(lambda: store([self.below]))
        pl.when((z > 0) & (z < last))(lambda: store([self.below, self.above]))
        for d in range(last + 1):
            for h in range(self.splits):
                if d > 0:

                    @pl.when(z < d)
                    def _():
                        self.copy(d, h, 1).wait_send()

                if d < last:

                    @pl.when(z > d)
                    def _():
                        self.copy(d, h, -1).wait_send()


class InWeightGather:
    def __init__(self, place, ins, outs, scratch):
        (slot_ref,), (in_all,) = ins, outs
        every = pl.ds(0, place.spots)
        some = place.spots // 2
        self.line = Relay(
            place, lambda h: cut(slot_ref, 2, h),
            lambda at, h: in_all.at[pl.ds(h * some, some), at], 2,
        )
        self.kept = place.keep(slot_ref, in_all.at[every, place.z])

    def start(self):
        self.line.start()
        self.kept.start()

    def stage(self, i):
        self.line.stage(i + 1)

    def finish(self):
        self.kept.wait()
        self.line.finish()


class OutWeightGather:
    def __init__(self, place, ins, outs, scratch):
        (out_ref, proj_ref), (self.heads, proj_all), (self.col,) = ins, outs, scratch
        col = self.col
        self.place = place
        self.lines = [
            Relay(place, lambda h: out_ref, lambda at, h: col.at[at], 1),
            Relay(place, lambda h: cut(proj_ref, 2, h), lambda at, h: cut(proj_all, 2, h, at), 2),
        ]
        self.kept = [
            place.keep(out_ref, col.at[place.z]), place.keep(proj_ref, proj_all.at[place.z]),
        ]

    def start(self):
        for line in self.lines:
            line.start()
        for copy in self.kept:
            copy.start()

    def stage(self, i):
        for line in self.lines:
            line.stage(i + 1)

    def finish(self):
        for copy in self.kept:
            copy.wait()
        keep, over = heads_home(self.place, self.col, self.heads, self.place.planes // 2)
        keep.wait()
        over.wait()
        for line in self.lines:
            line.finish()


class InGradSum:
    def __init__(self, place, ins, outs, scratch):
        (qkv_ref, fc_ref, self.sums), (self.out, self.sums_out) = ins, outs
        below, above, self.sums_buf = scratch
        self.place = place
        self.line = LineSum(
            place, below, above,
            lambda d, i: jnp.concatenate(
                [qkv_ref[i // 2, d, i % 2], fc_ref[i // 2, d, i % 2]], axis=-1
            ),
            lambda ref, d, i: ref.at[d, i // 2, i % 2],
            2 * place.spots, 2,
        )
        self.at = place.take(place.planes)
        self.sent = []

    def start(self):
        place = self.place
        self.line.start()
        for k in range(1, place.planes):
            copy = place.far(
                self.sums, self.sums_buf.at[k], self.at + k,
                place.at_z((place.z + k) % place.planes),
            )
            copy.start()
            self.sent.append(copy)

    def stage(self, i):
        self.line.stage(i)

    def finish(self):
        total = self.sums[...]
        for k, copy in enumerate(self.sent):
            copy.wait_recv()
            total = total + self.sums_buf[k + 1]
        self.sums_out[...] = total
        self.line.finish(lambda i: self.out.at[i // 2, i % 2])
        for copy in self.sent:
            copy.wait_send()


class OutGradSum:
    def __init__(self, place, ins, outs, scratch):
        heads_ref, proj_ref = ins
        self.heads_out, self.proj_out = outs
        col, col_below, col_above, below, above = scratch
        c, half = place.c, place.planes // 2
        few = pl.ds(0, half)
        self.place = place
        mine = pl.ds(c * half, half)
        self.keep = place.keep(heads_ref.at[few, c], col.at[mine])
        self.over = place.far(heads_ref.at[few, 1 - c], col.at[mine], place.take(), (place.p, place.near))
        rows = col.shape[1]

        def line(own, below, above, count, splits):
            step = own.shape[1] // count
            some = lambda i: pl.ds(pl.multiple_of(i * step, step), step)
            return LineSum(
                place, below, above,
                lambda d, i: own[d, some(i)], lambda ref, d, i: ref.at[d, some(i)], count, splits,
            )

        self.count = proj_ref.shape[1] // rows
        self.rows = rows
        self.head_line = line(col, col_below, col_above, 1, 1)
        self.proj_line = line(proj_ref, below, above, self.count, 2)

    def start(self):
        self.keep.start()
        self.over.start()
        self.proj_line.start()
        self.keep.wait()
        self.over.wait_recv()
        self.head_line.start()

    def stage(self, i):
        self.proj_line.stage(i)

    def finish(self):
        rows = self.rows
        for i in range(self.place.planes - 1):
            self.head_line.stage(i)
        self.head_line.finish(lambda i: self.heads_out.at[pl.ds(0, rows)])
        self.proj_line.finish(
            lambda i: self.proj_out.at[pl.ds(pl.multiple_of(i * rows, rows), rows)]
        )
        self.over.wait_send()


VM = pltpu.VMEM


def in_weight_gather(slot, spots, planes):
    owned, cols = slot.shape[2:]
    shape = jax.ShapeDtypeStruct((spots, planes, 2, owned, cols), BF)
    return (InWeightGather, [slot], [(shape, pl.ANY)], [], 4 * planes, 1)


def out_weight_gather(out_w, proj_w, spots, planes):
    heads = jax.ShapeDtypeStruct((planes // 2, 2) + out_w.shape, BF)
    proj = jax.ShapeDtypeStruct((planes,) + proj_w.shape, BF)
    return (
        OutWeightGather, [out_w, proj_w], [(heads, pl.ANY), (proj, pl.ANY)],
        [VM((planes,) + out_w.shape, BF)], 6 * planes + 1, 3,
    )


def in_grad_sum(grad_qkv, grad_fc, sums, spots, planes):
    owned = grad_qkv.shape[3]
    slot = (spots, 2, owned, grad_qkv.shape[4] + grad_fc.shape[4])
    return (
        InGradSum, [grad_qkv, grad_fc, sums],
        [(jax.ShapeDtypeStruct(slot, BF), VM), (jax.ShapeDtypeStruct(sums.shape, F32), VM)],
        [VM((planes,) + slot, BF), VM((planes,) + slot, BF), VM((planes,) + sums.shape, F32)],
        5 * planes, 0,
    )


def out_grad_sum(heads, proj, spots, planes):
    _, _, owned, width = heads.shape
    wide = proj.shape[1]
    return (
        OutGradSum, [heads, proj],
        [
            (jax.ShapeDtypeStruct((owned, width), F32), VM),
            (jax.ShapeDtypeStruct((wide, width), F32), VM),
        ],
        [VM((planes, owned, width), BF)] * 3 + [VM((planes, wide, width), BF)] * 2,
        6 * planes + 1, 1,
    )


def unpack(jobs, place, refs, lead_in, lead_out, lead_scratch):
    refs = list(refs)
    ins = [refs.pop(0) for _ in range(lead_in)]
    job_ins = [[refs.pop(0) for _ in job[1]] for job in jobs]
    outs = [refs.pop(0) for _ in range(lead_out)]
    job_outs = [[refs.pop(0) for _ in job[2]] for job in jobs]
    scratch = [refs.pop(0) for _ in range(lead_scratch)]
    job_scratch = [[refs.pop(0) for _ in job[3]] for job in jobs]
    place.send_sem, place.recv_sem, place.copy_sem = refs
    made = [
        job[0](place, *three) for job, three in zip(jobs, zip(job_ins, job_outs, job_scratch))
    ]
    return ins, outs, scratch, made


def job_call(kernel, name, number, spots, planes, jobs, args, in_spaces, outs, scratch, remote, local):
    spec = lambda space: pl.BlockSpec(memory_space=space)
    count = 0
    for job in jobs:
        args = args + job[1]
        in_spaces = in_spaces + [VM] * len(job[1])
        outs = outs + job[2]
        scratch = scratch + job[3]
        remote, local = remote + job[4], local + job[5]
    held = sum(x.inner_aval.size * x.inner_aval.dtype.itemsize for x in scratch)
    held += sum(x.size * x.dtype.itemsize for x, space in zip(args, in_spaces) if space is VM)
    held += sum(x.size * x.dtype.itemsize for x, space in outs if space is VM)
    plain = [(job[0], [0] * len(job[1]), [0] * len(job[2]), [0] * len(job[3])) for job in jobs]
    return pl.pallas_call(
        functools.partial(kernel, spots, planes, plain),
        out_shape=[shape for shape, _ in outs],
        in_specs=[spec(space) for space in in_spaces],
        out_specs=[spec(space) for _, space in outs],
        scratch_shapes=scratch + sems(remote, local),
        compiler_params=pltpu.CompilerParams(
            collective_id=number, has_side_effects=True, vmem_limit_bytes=held + (2 << 20)
        ),
        name=name,
    )(*args)


def sems(remote, local):
    return [
        pltpu.SemaphoreType.DMA((remote,)),
        pltpu.SemaphoreType.DMA((remote,)),
        pltpu.SemaphoreType.DMA((local,)),
    ]


def gather_sems(spots, pieces):
    ways = 2 if spots == 4 else spots - 1
    return pieces * (ways + spots + (1 if spots == 4 else 0))


def start_kernel(
    spots, planes,
    tok_ref, cot_ref, first_in_ref, next_in_ref, out_ref, proj_ref,
    tok_all, cot_all, first_all, next_slot, heads_all, proj_all,
    tok_buf, cot_buf, col, send_sem, recv_sem, copy_sem,
):
    place = Place(spots, planes, send_sem, recv_sem, copy_sem)
    p, s, z, c = place.p, place.s, place.z, place.c
    half = planes // 2
    crowd = [
        ((p + k) % spots, s if e == 0 else place.near)
        for k in range(spots) for e in range(2) if k or e
    ]
    greet(place, crowd, True)

    streams = [(tok_ref, tok_buf, tok_all), (cot_ref, cot_buf, cot_all)]
    spread = []
    for own, buf, _ in streams:
        row = []
        for k in range(1, spots):
            q = (p + k) % spots
            copy = place.far(own.at[q], buf.at[p], place.take(), (q, s))
            copy.start()
            row.append(copy)
        spread.append(row)
    proj_line = Relay(
        place, lambda h: cut(proj_ref, 2, h), lambda at, h: cut(proj_all, 2, h, at), 2
    )
    head_line = Relay(place, lambda h: out_ref, lambda at, h: col.at[at], 1)
    proj_line.start()
    head_line.start()
    kept = [place.keep(proj_ref, proj_all.at[z]), place.keep(out_ref, col.at[z])]
    mailed = []
    for own, slot in (
        (first_in_ref, lambda q, core: first_all.at[q, z, core]),
        (next_in_ref, lambda q, core: next_slot.at[q, core]),
    ):
        for k in range(spots):
            for e in range(2):
                q = (p + k) % spots
                core = c if e == 0 else 1 - c
                if k or e:
                    copy = place.far(
                        own.at[q, core], slot(p, c), place.take(),
                        (q, s if e == 0 else place.near),
                    )
                    copy.start()
                    mailed.append(copy)
        kept.append(place.keep(own.at[p, c], slot(p, c)))
    for copy in kept:
        copy.start()
    moved = []
    for (own, buf, whole), row in zip(streams, spread):
        send_at, recv_at = place.take(spots), place.take(planes)
        place.kept += 1
        local = place.kept - 1
        for k in range(spots):
            j = (p + spots - k) % spots
            if k:
                row[k - 1].wait_recv()
            data = own.at[p] if k == 0 else buf.at[j]

            @pl.when(j != z)
            def _():
                place.far(data, whole.at[z, c, p], send_at + k, place.at_z(j), recv_at + z).start()

            @pl.when(j == z)
            def _():
                pltpu.make_async_copy(data, whole.at[z, c, p], copy_sem.at[local]).start()

        moved.append((send_at, recv_at, local))
    for copy in kept:
        copy.wait()
    count = len(mailed) // 2
    for copy in mailed[:count]:
        copy.wait_recv()
    in_slot = lambda at, h: first_all.at[pl.ds(h * (spots // 2), spots // 2), at]
    in_line = Relay(place, lambda h: in_slot(z, h), in_slot, 2)
    in_line.start()
    head_line.stage(1)
    proj_line.stage(1)
    gathers = []
    for (own, buf, whole), (send_at, recv_at, local) in zip(streams, moved):
        gather = PlaneGather(place, whole, [(z + i) % planes for i in range(planes)])
        for i in range(planes):
            at = (z + i) % planes
            piece = whole.at[at, c, p]
            if i == 0:
                pltpu.make_async_copy(tok_ref.at[0], piece, copy_sem.at[local]).wait()
            else:
                place.far(piece, piece, send_at, place.at_z(at), recv_at + at).wait_recv()
            gather.start(i)
        gathers.append(gather)
        if len(gathers) == 1:
            in_line.stage(1)
            head_line.stage(2)
            proj_line.stage(2)
    for i in range(planes):
        gathers[0].arrive(i)
    for k in range(2, planes):
        in_line.stage(k)
        if k + 1 < planes:
            head_line.stage(k + 1)
            proj_line.stage(k + 1)
        if k == 2:
            for i in range(planes):
                gathers[0].arrive_diagonal(i)
            for i in range(planes):
                gathers[1].arrive(i)
            for i in range(planes):
                gathers[1].arrive_diagonal(i)
    keep, over = heads_home(place, col, heads_all, half)
    for copy in mailed[count:]:
        copy.wait_recv()
    for gather in gathers:
        gather.finish()
    keep.wait()
    over.wait()
    for line in (in_line, head_line, proj_line):
        line.finish()
    for row in spread:
        for copy in row:
            copy.wait_send()
    for copy in mailed:
        copy.wait_send()
    for (own, buf, whole), (send_at, recv_at, local) in zip(streams, moved):
        for k in range(spots):
            j = (p + spots - k) % spots

            @pl.when(j != z)
            def _():
                place.far(own.at[p], whole.at[z, c, p], send_at + k, place.at_z(j)).wait_send()


def bring_all(tok, cot, first_in, next_in, out_w, proj_w, spots, planes):
    _, rows, width = tok.shape
    vmem = pl.BlockSpec(memory_space=pltpu.VMEM)
    hbm = pl.BlockSpec(memory_space=pl.ANY)
    whole = jax.ShapeDtypeStruct((planes, 2, spots, rows, width), BF)
    owned, cols = first_in.shape[2:]
    return pl.pallas_call(
        functools.partial(start_kernel, spots, planes),
        out_shape=[
            whole, whole,
            jax.ShapeDtypeStruct((spots, planes, 2, owned, cols), BF),
            jax.ShapeDtypeStruct(next_in.shape, BF),
            jax.ShapeDtypeStruct((planes // 2, 2) + out_w.shape, BF),
            jax.ShapeDtypeStruct((planes,) + proj_w.shape, BF),
        ],
        in_specs=[vmem] * 6,
        out_specs=[hbm] * 6,
        scratch_shapes=[
            pltpu.VMEM((spots, rows, width), BF),
            pltpu.VMEM((spots, rows, width), BF),
            pltpu.VMEM((planes,) + out_w.shape, BF),
        ] + sems(
            2 * (spots - 1) + 2 * (2 * spots - 1) + 10 * planes + 2 * (spots + planes)
            + 2 * gather_sems(spots, planes) + 1,
            7,
        ),
        compiler_params=pltpu.CompilerParams(
            collective_id=3, has_side_effects=True, vmem_limit_bytes=12 << 20
        ),
        name="bring_all",
    )(tok, cot, first_in, next_in, out_w, proj_w)


def gather_kernel(spots, planes, jobs, *refs):
    place = Place(spots, planes, None, None, None)
    (own_ref,), (all_ref,), _, made = unpack(jobs, place, refs, 1, 1, 0)
    groups = own_ref.shape[0]
    half = groups // 2
    parts = [pl.ds(0, half), pl.ds(half, half)]
    plane = [(q, place.s) for q in place.plane_partners()] + [(place.p, place.near)]
    greet(place, plane, bool(made))
    gather = PlaneGather(place, all_ref, parts)
    for i in range(2):
        gather.start(i, own_ref.at[parts[i]])
    keep = place.keep(own_ref, all_ref.at[pl.ds(0, groups), place.c, place.p])
    keep.start()
    for job in made:
        job.start()
    gather.arrive(0)
    for job in made:
        job.stage(0)
    gather.arrive(1)
    for job in made:
        job.stage(1)
    for i in range(2):
        gather.arrive_diagonal(i)
    for i in range(2, planes - 1):
        for job in made:
            job.stage(i)
    for job in made:
        job.finish()
    keep.wait()
    gather.finish()


def gather_tokens(own, spots, planes, number, jobs):
    groups, rows, width = own.shape
    whole = jax.ShapeDtypeStruct((groups, 2, spots, rows, width), own.dtype)
    out = job_call(
        gather_kernel, "gather_tokens", number, spots, planes, jobs, [own], [VM],
        [(whole, pl.ANY)], [], gather_sems(spots, 2), 1,
    )
    return [out[0].reshape(-1, width)] + list(out[1:])


class PlaneScatter:
    def __init__(self, place, part_ref, out_ref, near_buf, mine, relay, inbox):
        self.place, self.out = place, out_ref
        self.near_buf, self.mine, self.relay, self.inbox = near_buf, mine, relay, inbox
        spots, p, c = place.spots, place.p, place.c
        self.others = place.plane_partners()
        _, self.groups, self.rows, _ = mine.shape
        half = self.groups // 2
        self.halves = [pl.ds(0, half), pl.ds(half, half)]
        self.whole = pl.ds(0, self.groups)
        if spots == 4:
            spot_of = [p] + self.others + [3 - p]
            self.order = [3, 1, 2, 0]
        else:
            spot_of = [p] + self.others
            self.order = list(range(1, spots)) + [0]
        self.handed, self.kept, self.sent = {}, {}, {}
        for m in self.order:
            self.handed[m] = place.far(
                part_ref.at[self.whole, 1 - c, spot_of[m]], near_buf.at[m],
                place.take(), (p, place.near),
            )
            self.kept[m] = place.keep(part_ref.at[self.whole, c, spot_of[m]], mine.at[m])

    def start(self):
        for m in self.order:
            self.handed[m].start()
            self.kept[m].start()

    def add(self, first, count, into, left, right):
        step = min(self.rows, 16)
        per = self.rows // step

        def one(i, carry):
            g = first + i // per
            at = pl.ds(pl.multiple_of((i % per) * step, step), step)
            into[g, at, :] = (left(g, at) + right(g, at)).astype(into.dtype)
            return carry

        lax.fori_loop(0, count * per, one, 0)

    def far(self, name, m, part, slot, dest):
        copy = self.place.far(self.mine.at[m, part], slot, self.place.take(), (dest, self.place.s))
        copy.start()
        self.sent[name] = copy

    def combine(self, m):
        mine, near_buf = self.mine, self.near_buf
        self.handed[m].wait_recv()
        self.kept[m].wait()
        self.add(
            0, self.groups, self.out if m == 0 else mine.at[m],
            lambda g, at: mine[m, g, at, :].astype(F32),
            lambda g, at: near_buf[m, g, at, :].astype(F32),
        )
        if self.place.spots == 4:
            x, y = self.others
            first, last = self.halves
            if m == 3:
                self.far(0, 3, first, self.relay.at[0], x)
                self.far(1, 3, last, self.relay.at[1], y)
            elif m == 1:
                self.far(2, 1, first, self.inbox.at[0, first], x)
            elif m == 2:
                self.far(3, 2, last, self.inbox.at[1, last], y)
        elif m > 0:
            self.far(m + 1, m, self.whole, self.inbox.at[m - 1], self.others[m - 1])

    def pass_on(self):
        if self.place.spots != 4:
            return
        mine, relay = self.mine, self.relay
        x, y = self.others
        first, last = self.halves
        half = self.groups // 2
        self.sent[0].wait_recv()
        self.add(
            0, half, mine.at[2],
            lambda g, at: mine[2, g, at, :].astype(F32),
            lambda g, at: relay[0, g, at, :].astype(F32),
        )
        self.far(4, 2, first, self.inbox.at[1, first], y)
        self.sent[1].wait_recv()
        self.add(
            half, half, mine.at[1],
            lambda g, at: mine[1, g, at, :].astype(F32),
            lambda g, at: relay[1, g - half, at, :].astype(F32),
        )
        self.far(5, 1, last, self.inbox.at[0, last], x)

    def total(self):
        for name in self.sent:
            if name >= 2:
                self.sent[name].wait_recv()
        out, inbox = self.out, self.inbox

        def received(g, at):
            total = inbox[0, g, at, :].astype(F32)
            for slot in range(1, inbox.shape[0]):
                total = total + inbox[slot, g, at, :].astype(F32)
            return total

        self.add(0, self.groups, out, lambda g, at: out[g, at, :], received)

    def finish(self):
        for m in self.order:
            self.handed[m].wait_send()
        for name in self.sent:
            self.sent[name].wait_send()


def scatter_kernel(count, spots, planes, jobs, *refs):
    place = Place(spots, planes, None, None, None)
    ins, outs, scratch, made = unpack(jobs, place, refs, count, count, 4 * count)
    streams = [
        PlaneScatter(place, ins[i], outs[i], *scratch[4 * i : 4 * i + 4]) for i in range(count)
    ]
    plane = [(q, place.s) for q in place.plane_partners()] + [(place.p, place.near)]
    greet(place, plane, bool(made))
    for stream in streams:
        stream.start()
    for job in made:
        job.start()
    for at, stream in enumerate(streams):
        job = made[at] if at < len(made) else None
        for m in stream.order:
            stream.combine(m)
        if job:
            job.stage(0)
        stream.pass_on()
        if job:
            job.stage(1)
        stream.total()
        if job:
            for i in range(2, planes - 1):
                job.stage(i)
    for job in made:
        job.finish()
    for stream in streams:
        stream.finish()


def scatter_tokens(parts, spots, planes, number, jobs):
    total, width = parts[0].shape
    groups = planes
    rows = total // (groups * 2 * spots)
    slots = 2 if spots == 4 else spots - 1
    piece = (groups, rows, width)
    count = len(parts)
    return job_call(
        functools.partial(scatter_kernel, count), "scatter_tokens", number, spots, planes, jobs,
        [part.reshape(groups, 2, spots, rows, width) for part in parts], [pl.ANY] * count,
        [(jax.ShapeDtypeStruct(piece, F32), VM)] * count,
        [
            VM((spots,) + piece, BF), VM((spots,) + piece, BF),
            VM((2, groups // 2, rows, width), BF), VM((slots,) + piece, BF),
        ] * count,
        count * (spots + (6 if spots == 4 else spots - 1)), count * spots,
    )


def end_kernel(spots, planes, jobs, *refs):
    place = Place(spots, planes, None, None, None)
    ins, outs, scratch, _ = unpack(jobs, place, refs, 5, 5, 2)
    p, s, z, c = place.p, place.s, place.z, place.c
    crowd = [
        (k, e, ((p + k) % spots, s if e == 0 else place.near))
        for k in range(spots) for e in range(2) if k or e
    ]
    greet(place, [dest for _, _, dest in crowd], True)
    streams = list(zip(ins[:2], scratch, outs[:2]))
    moved = []
    for own, buf, out in streams:
        row = []
        for k in range(1, planes):
            to = (z + k) % planes
            copy = place.far(own.at[to], buf.at[z], place.take(), place.at_z(to))
            copy.start()
            row.append(copy)
        moved.append(row)
    mailed, kept = [], []
    for own, out in zip(ins[2:4], outs[2:4]):
        for k, e, dest in crowd:
            core = c if e == 0 else 1 - c
            copy = place.far(own.at[dest[0], core], out.at[p, c], place.take(), dest)
            copy.start()
            mailed.append(copy)
        kept.append(place.keep(own.at[p, c], out.at[p, c]))
    for k, e, dest in crowd:
        copy = place.far(ins[4], outs[4].at[p, c], place.take(), dest)
        copy.start()
        mailed.append(copy)
    kept.append(place.keep(ins[4], outs[4].at[p, c]))
    for copy in kept:
        copy.start()
    homes = []
    for (own, buf, out), row in zip(streams, moved):
        send_at, recv_at = place.take(planes), place.take(spots)
        place.kept += 1
        local = place.kept - 1
        for k in range(planes):
            j = (z + planes - k) % planes
            if k:
                row[k - 1].wait_recv()
            data = own.at[z] if k == 0 else buf.at[j]

            @pl.when(j != p)
            def _():
                place.far(data, out.at[p], send_at + k, (j, s), recv_at + p).start()

            @pl.when(j == p)
            def _():
                pltpu.make_async_copy(data, out.at[p], place.copy_sem.at[local]).start()

        homes.append((send_at, recv_at, local))
    for copy in mailed:
        copy.wait_recv()
    for (own, buf, out), (send_at, recv_at, local) in zip(streams, homes):
        for k in range(1, spots):
            q = (p + k) % spots
            place.far(out.at[q], out.at[q], send_at, (q, s), recv_at + q).wait_recv()
        pltpu.make_async_copy(own.at[0], out.at[p], place.copy_sem.at[local]).wait()
    for copy in kept:
        copy.wait()
    for row in moved:
        for copy in row:
            copy.wait_send()
    for copy in mailed:
        copy.wait_send()
    for (own, buf, out), (send_at, recv_at, local) in zip(streams, homes):
        for k in range(planes):
            j = (z + planes - k) % planes

            @pl.when(j != p)
            def _():
                place.far(own.at[0], out.at[p], send_at + k, (j, s)).wait_send()


def send_home(grad_tok, outputs, first_grad, next_grad, sums, spots, planes):
    _, rows, width = grad_tok.shape
    home = jax.ShapeDtypeStruct((spots, rows, width), BF)
    slot = jax.ShapeDtypeStruct(first_grad.shape, BF)
    return job_call(
        end_kernel, "send_home", 9, spots, planes, [],
        [grad_tok, outputs, first_grad, next_grad, sums], [VM] * 5,
        [
            (home, pl.ANY), (home, pl.ANY), (slot, pl.ANY), (slot, pl.ANY),
            (jax.ShapeDtypeStruct((spots, 2) + sums.shape, F32), pl.ANY),
        ],
        [VM((planes, rows, width), BF)] * 2,
        2 * (planes - 1) + 3 * (2 * spots - 1) + 2 * (spots + planes), 5,
    )


class Net:
    def __init__(self, mesh):
        self.planes = mesh.shape["seq"] // 2
        self.spots = mesh.shape["dp"]
        self.p = lax.axis_index("dp")
        self.z = lax.axis_index("seq") // 2
        self.c = lax.axis_index("seq") % 2

    def permute(self, x, to):
        pairs = []
        for p in range(self.spots):
            for z in range(self.planes):
                for c in range(2):
                    tp, tz, tc = to(p, z, c)
                    source = (p * self.planes + z) * 2 + c
                    pairs.append((source, (tp * self.planes + tz) * 2 + tc))
        return lax.ppermute(x, AXES, pairs)

    def turned(self, x):
        return self.permute(x, lambda p, z, c: (z, p, c))


def normalize(resid):
    mean = jnp.mean(resid, axis=-1, keepdims=True)
    center = resid - mean
    spread = jnp.mean(center * center, axis=-1, keepdims=True)
    inv = lax.rsqrt(spread + norm_eps)
    return center * inv, inv


def gelu_parts(pre):
    cdf = 0.5 * (1.0 + lax.erf(pre * (2.0**-0.5)))
    return cdf


def on_device(
    mesh, tokens, cotangent, segments, qkv_weight, out_weight, fc_weight, proj_weight,
    biases, ln_gain, ln_shift,
):
    net = Net(mesh)
    spots, planes = net.spots, net.planes
    team = spots * 2
    layers, rows, _ = qkv_weight.shape
    width = out_weight.shape[2]
    local = tokens.shape[1]
    head_cols = width // team
    hidden_all = fc_weight.shape[2]
    fc_piece = proj_weight.shape[1]
    owner = (net.p * planes + net.z) * 2 + net.c
    assert spots == planes

    seg_row = net.turned(segments)
    full_len = seg_row.shape[1]
    index = lax.broadcasted_iota(jnp.int32, (1, full_len), 1)
    starts = jnp.zeros((1, full_len), jnp.int32)
    for doc in range(3):
        count = jnp.sum((seg_row == doc).astype(jnp.int32))
        starts = starts + jnp.where(seg_row > doc, count, 0)
    position = (index - starts).astype(F32)
    first_block = starts[0, ::BLOCK] // BLOCK
    half = ROT // 2
    entry = jnp.arange(head_cols, dtype=jnp.int32) % HEAD_DIM
    inverse = 10000.0 ** (-2.0 * jnp.arange(half, dtype=F32) / ROT)
    angle = inverse[:, None] * position
    spread = ((entry % half)[None, :] == jnp.arange(half)[:, None]) & (entry < ROT)[None, :]
    spread = lambda rows, hot=spread.astype(F32): lax.dot_general(
        rows, hot, (((0,), (0,)), ((), ())), precision=lax.Precision.HIGHEST,
        preferred_element_type=F32,
    )
    cosine = spread(jnp.cos(angle)) + (entry >= ROT).astype(F32)[None, :]
    sine = spread(jnp.sin(angle))

    gain_own = ln_gain.astype(F32)
    shift_own = ln_shift.astype(F32)
    t_at = net.p * 2 + net.c
    qkv_cols, fc_cols = 3 * head_cols, planes * fc_piece
    in_cols = qkv_cols + fc_cols
    bias_rows = biases.shape[1]

    def in_weight(layer):
        qkv = qkv_weight[layer].astype(F32) * gain_own[layer, 0][:, None]
        qkv = qkv.astype(BF).reshape(rows, 3, spots, 2, head_cols)
        qkv = jnp.transpose(qkv, (2, 3, 0, 1, 4)).reshape(spots, 2, rows, qkv_cols)
        fc = fc_weight[layer].astype(F32) * gain_own[layer, 1][:, None]
        fc = fc.astype(BF).reshape(rows, spots, planes, 2, fc_piece)
        fc = jnp.transpose(fc, (1, 3, 0, 2, 4)).reshape(spots, 2, rows, fc_cols)
        return [qkv, fc]

    small = jnp.concatenate([biases, ln_gain, ln_shift], axis=1).reshape(-1, rows).T
    small_cols = small.shape[1]
    small = jnp.pad(small, ((0, 0), (0, 128 - small_cols)))
    small = jnp.broadcast_to(small, (spots, 2, rows, 128))
    first_in = jnp.concatenate(in_weight(0) + [small], axis=-1)
    next_in = jnp.concatenate(in_weight(1), axis=-1)

    per_spot = (spots, local // spots, width)
    tok_all, cot_all, first_all, next_slot, heads_w0, proj_w0 = bring_all(
        tokens.reshape(per_spot), cotangent.reshape(per_spot), first_in, next_in,
        out_weight[0], proj_weight[0], spots, planes,
    )
    first_all = first_all.reshape(width, -1)
    small = first_all[:, in_cols : in_cols + small_cols].T.astype(F32).reshape(layers, -1, width)
    bias_all, gain_all, shift_all = (
        small[:, :bias_rows], small[:, bias_rows : bias_rows + 2], small[:, bias_rows + 2 :],
    )
    whole_in = [first_all, None]
    weights_out = [(heads_w0.reshape(head_cols, width), proj_w0.reshape(fc_cols, width)), None]

    def bias_in(layer):
        qkv_b = bias_all[layer, :3].reshape(3, team, head_cols)
        qkv_b = lax.dynamic_index_in_dim(qkv_b, t_at, 1, keepdims=False).reshape(1, -1)
        fc_b = bias_all[layer, 4 : bias_rows - 1].reshape(spots, planes, 2, fc_piece)
        fc_b = lax.dynamic_index_in_dim(fc_b, net.p, 0, keepdims=False)
        fc_b = lax.dynamic_index_in_dim(fc_b, net.c, 1, keepdims=False).reshape(1, -1)
        ratio = shift_all[layer] / gain_all[layer]
        high = ratio.astype(BF)
        low = (ratio - high.astype(F32)).astype(BF)
        whole = whole_in[layer]
        first, second = (
            nn(high[k : k + 1], whole) + nn(low[k : k + 1], whole) for k in range(2)
        )
        qkv_b = qkv_b + first[:, :qkv_cols]
        fc_b = fc_b + second[:, qkv_cols:in_cols]
        return jnp.concatenate([qkv_b, fc_b], axis=1)

    def own_part(whole):
        part = lax.dynamic_index_in_dim(whole, net.c, 1, keepdims=False)
        return lax.dynamic_index_in_dim(part, net.p, 1, keepdims=False)

    cot_own = own_part(cot_all)
    cot_all = cot_all.reshape(full_len, width)

    resid = own_part(tok_all).astype(F32)
    saved = []
    for layer in range(layers):
        normed, inv = normalize(resid)
        if layer:
            normed_all, heads_w, proj_w = gather_tokens(
                normed.astype(BF), spots, planes, 4,
                [out_weight_gather(out_weight[layer], proj_weight[layer], spots, planes)],
            )
            weights_out[layer] = (
                heads_w.reshape(head_cols, width), proj_w.reshape(fc_cols, width)
            )
        head_w, proj_w = weights_out[layer]
        rows_in = normed_all if layer else tok_all.reshape(full_len, width)
        mixed, hidden_pre, hidden, *more = in_product(
            rows_in, whole_in[layer], bias_in(layer), qkv_cols, layer == 0
        )
        if more:
            normed_all = more[0]
        query, key, value, ctx, ctx_low, lse = attn_forward(
            mixed, cosine, sine, starts, first_block
        )
        part = pair_product(hidden, ctx_low, [proj_w, head_w], False)
        saved.append((normed, inv, normed_all, query, key, value, ctx, ctx_low, lse, hidden_pre, hidden))
        end_bias = bias_all[layer, 3] + bias_all[layer, bias_rows - 1]
        if layer < layers - 1:
            summed, next_all = scatter_tokens(
                [part], spots, planes, 5, [in_weight_gather(next_slot, spots, planes)]
            )
            next_all = next_all.reshape(width, -1)
            whole_in[1] = next_all
            resid = resid + summed + end_bias
    last_part, last_bias = part, end_bias

    grad_own = cot_own
    sums_rows = -(-(in_cols + width) // 1024) * 8

    def out_grads(ctx_low, hidden, grad_all):
        heads = tn(ctx_low, grad_all).astype(BF).reshape(planes // 2, 2, rows, width)
        proj = tn(hidden, grad_all).astype(BF).reshape(planes, fc_piece, width)
        return out_grad_sum(heads, proj, spots, planes)

    in_slots, in_sums, out_parts = [None] * layers, [None] * layers, [None] * layers
    waiting = None
    for layer in reversed(range(layers)):
        normed, inv, normed_all, query, key, value, ctx, ctx_low, lse, hidden_pre, hidden = saved[layer]
        head_w, proj_w = weights_out[layer]
        if layer == layers - 1:
            grad_all = cot_all
        else:
            grad_all, *out_parts[layer + 1] = gather_tokens(grad_own, spots, planes, 6, [waiting])
        grad_ctx = nt(grad_all, head_w).astype(BF)
        grad_mixed = attn_backward(
            query, key, value, ctx, lse, grad_ctx, cosine, sine, starts, first_block
        )
        cdf = gelu_parts(hidden_pre)
        density = jnp.exp(-0.5 * hidden_pre * hidden_pre) * ((2.0 * jnp.pi) ** -0.5)
        grad_pre = (nt(grad_all, proj_w) * (cdf + hidden_pre * density)).astype(BF)
        part = pair_product(grad_mixed, grad_pre, [whole_in[layer]], True)

        owners = (spots, planes, 2, rows)
        grad_qkv = tn(normed_all, grad_mixed).astype(BF).reshape(owners + (qkv_cols,))
        grad_fc = tn(normed_all, grad_pre).astype(BF).reshape(owners + (fc_cols,))
        sums = jnp.concatenate(
            [
                jnp.sum(grad_mixed.astype(F32), axis=0),
                jnp.sum(grad_pre.astype(F32), axis=0),
                jnp.sum(grad_own.astype(F32), axis=(0, 1)),
            ]
        )
        sums = jnp.pad(sums, (0, sums_rows * 128 - sums.shape[0])).reshape(sums_rows, 128)
        jobs = [in_grad_sum(grad_qkv, grad_fc, sums, spots, planes)]
        waiting = out_grads(ctx_low, hidden, grad_all)
        if layer == 0:
            jobs.append(waiting)
        if layer:
            norm_grad, in_slots[layer], in_sums[layer] = scatter_tokens(
                [part], spots, planes, 7, jobs
            )
        else:
            norm_grad, summed, in_slots[layer], in_sums[layer], *out_parts[layer] = scatter_tokens(
                [part, last_part], spots, planes, 8, jobs
            )
            outputs_own = (resid + summed + last_bias).astype(BF)
        mean_grad = jnp.mean(norm_grad, axis=-1, keepdims=True)
        mean_dot = jnp.mean(norm_grad * normed, axis=-1, keepdims=True)
        grad_next = grad_own.astype(F32) + inv * (norm_grad - mean_grad - normed * mean_dot)
        grad_own = lax.optimization_barrier(grad_next.astype(BF))

    grad_tokens, outputs, *in_grads, sums_all = send_home(
        grad_own, outputs_own, in_slots[0], in_slots[1], jnp.concatenate(in_sums, axis=0), spots, planes
    )
    sums_all = sums_all.reshape(team, layers, -1)
    scale = jnp.concatenate([gain_own, shift_own], axis=1).reshape(4 * layers, rows).T
    grad_qkv, grad_fc, stats = owner_grads(
        in_grads[0], in_grads[1], sums_all, qkv_weight, fc_weight, scale, head_cols, fc_piece, planes
    )
    stats = jnp.transpose(stats.reshape(rows, layers, 2, 2), (3, 1, 2, 0))
    end_sum = jnp.sum(sums_all[:, :, in_cols : in_cols + width], axis=0)[:, None]
    qkv_sum = sums_all[:, :, :qkv_cols].reshape(team, layers, 3, head_cols)
    qkv_sum = jnp.transpose(qkv_sum, (1, 2, 0, 3)).reshape(layers, 3, width)
    fc_sum = sums_all[:, :, qkv_cols:in_cols].reshape(spots, 2, layers, planes, fc_piece)
    fc_sum = jnp.transpose(fc_sum, (2, 0, 3, 1, 4)).reshape(layers, -1, width)
    bias_grad = jnp.concatenate([qkv_sum, end_sum, fc_sum, end_sum], axis=1)
    bias_grad = lax.dynamic_slice_in_dim(bias_grad, owner * rows, rows, 2)
    whole = (1, local, width)
    return (
        outputs.reshape(whole),
        grad_tokens.reshape(whole),
        grad_qkv,
        jnp.stack([part[0] for part in out_parts]),
        grad_fc,
        jnp.stack([part[1] for part in out_parts]),
        bias_grad,
        stats[0],
        stats[1],
    )


def solution(mesh):
    return jax.shard_map(
        functools.partial(on_device, mesh),
        mesh=mesh,
        in_specs=(
            P("dp", "seq", None),
            P("dp", "seq", None),
            P("dp", None),
            P(None, ("dp", "seq"), None),
            P(None, ("dp", "seq"), None),
            P(None, ("dp", "seq"), None),
            P(None, ("dp", "seq"), None),
            P(None, None, ("dp", "seq")),
            P(None, None, ("dp", "seq")),
            P(None, None, ("dp", "seq")),
        ),
        out_specs=(
            P("dp", "seq", None),
            P("dp", "seq", None),
            P(None, ("dp", "seq"), None),
            P(None, ("dp", "seq"), None),
            P(None, ("dp", "seq"), None),
            P(None, ("dp", "seq"), None),
            P(None, None, ("dp", "seq")),
            P(None, None, ("dp", "seq")),
            P(None, None, ("dp", "seq")),
        ),
        check_vma=False,
    )
```
